32 devices in a mesh: dp: 4 (over y, x), row: 2 (over core), col: 4 (over z).
Axes of the slice: x: 2, y: 2, z: 4, core: 2. Of those that a mesh axis runs over, the one named last changes fastest.
Arguments:
- tokens: bfloat16 [4096, 2048], P('dp', ('row', 'col')), may hold values from -40 to 40
- gain_attn: float32 [2048], P(('row', 'col')), may hold values from 0.5 to 1.5
- gain_ffn: float32 [2048], P(('row', 'col')), may hold values from 0.5 to 1.5
- w_query: bfloat16 [2048, 2048], P('row', 'col'), may hold values from -0.125 to 0.125
- w_key: bfloat16 [2048, 2048], P('row', 'col'), may hold values from -0.125 to 0.125
- w_value: bfloat16 [2048, 2048], P('row', 'col'), may hold values from -0.125 to 0.125
- w_out: bfloat16 [2048, 2048], P('col', 'row'), may hold values from -1 to 1
- w_gate: bfloat16 [2048, 8192], P('row', 'col'), may hold values from -0.125 to 0.125
- w_up: bfloat16 [2048, 8192], P('row', 'col'), may hold values from -0.125 to 0.125
- w_down: bfloat16 [8192, 2048], P('col', 'row'), may hold values from -0.0625 to 0.0625
- grad_output: bfloat16 [4096, 2048], P('dp', ('row', 'col')), may hold values from -6 to 6
- segments: int32 [4, 1024], P('dp'), may hold values from 0 to 2, as said below
- positions: int32 [4, 1024], P('dp'), may hold values from 0 to 2047, as said below
Outputs:
- output: float32 [4096, 2048], P('dp', ('row', 'col'))
- grad_tokens: float32 [4096, 2048], P('dp', ('row', 'col'))
- grad_gain_attn: float32 [8, 4, 64], P(('row', 'col'), 'dp')
- grad_gain_ffn: float32 [8, 4, 64], P(('row', 'col'), 'dp')
- grad_w_query: float32 [2, 4, 256, 2048], P('row', 'dp', None, 'col')
- grad_w_key: float32 [2, 4, 256, 2048], P('row', 'dp', None, 'col')
- grad_w_value: float32 [2, 4, 256, 2048], P('row', 'dp', None, 'col')
- grad_w_out: float32 [4, 4, 128, 2048], P('col', 'dp', None, 'row')
- grad_w_gate: float32 [2, 4, 256, 8192], P('row', 'dp', None, 'col')
- grad_w_up: float32 [2, 4, 256, 8192], P('row', 'dp', None, 'col')
- grad_w_down: float32 [4, 4, 512, 2048], P('col', 'dp', None, 'row')
The draws below stay inside these ranges and needn't reach their ends.
Inputs may be any that keep to these rules, and one draw needn't show every extreme that they name: `segments`: within a sequence the numbers never fall; each sequence holds three documents. `positions`: positions count up by one inside a document; the first document of a sequence starts at a position no larger than 2048 minus its length, the others at 0.
All inputs are finite; a program needn't handle non-finite values.
Results may differ from the reference program's by a relative error of at most 0.015.
Values may be sent and summed in bfloat16 or wider, within the bound.
A program may use at most 256 MiB of HBM per device.

```python
import math
import jax
import jax.numpy as jnp
from jax import lax

D = 2048
HEADS = 32
HD = 64
FF = 8192
SEQ = 1024
TOKENS = 4096
NSEQ = 4
N_DP = 4
N_ROW = 2
N_COL = 4


def draw_tokens(key, part):
    base_key, row_key, col_key = jax.random.split(jax.random.fold_in(key, 11), 3)
    feature = jnp.arange(D, dtype=jnp.float32)[None, :] / D
    base = jnp.clip(jax.random.normal(base_key, (TOKENS, D), jnp.float32), -4.0, 4.0)
    trend = jnp.exp(math.log(10.0) * feature)
    rough = jax.random.uniform(col_key, (1, D), jnp.float32, 0.6, 1.5)
    row_scale = jnp.exp(jax.random.uniform(row_key, (TOKENS, 1), jnp.float32, 0.0, math.log(10.0)))
    return (base * trend * rough * row_scale / 20.0).astype(jnp.bfloat16)


def doc_layout(key):
    first_key, second_key, offset_key = jax.random.split(jax.random.fold_in(key, 7), 3)
    first_len = jax.random.randint(first_key, (NSEQ, 1), SEQ // 8, SEQ // 2)
    second_len = jax.random.randint(second_key, (NSEQ, 1), SEQ // 8, SEQ // 2)
    slot_index = jnp.arange(SEQ, dtype=jnp.int32)[None, :]
    third_start = first_len + second_len
    segment = (slot_index >= first_len).astype(jnp.int32) + (slot_index >= third_start).astype(jnp.int32)
    top_offset = 2 * SEQ - first_len
    drawn = jax.random.randint(offset_key, (NSEQ, 1), 0, top_offset + 1)
    seq_index = jnp.arange(NSEQ, dtype=jnp.int32)[:, None]
    offset = jnp.where(seq_index == 0, top_offset, drawn)
    doc_start = jnp.where(segment == 0, -offset, jnp.where(segment == 1, first_len, third_start))
    return (segment, (slot_index - doc_start).astype(jnp.int32))


def draw_segments(key, part):
    return doc_layout(key)[0]


def draw_positions(key, part):
    return doc_layout(key)[1]


def shard_levels(stream_key, extent, cuts, low, largest):
    def one(axis_at, shards_of):
        draws = jax.random.uniform(jax.random.fold_in(jax.random.fold_in(stream_key, 6), axis_at), (shards_of,), jnp.float32, low / len(cuts), largest / len(cuts))
        return jnp.repeat(jnp.exp(draws), extent[axis_at] // shards_of).reshape((-1,) + (1,) * (len(extent) - axis_at - 1))

    gain = one(*cuts[0])
    for cut in cuts[1:]:
        gain = gain * one(*cut)
    return gain


def normal_values(key, shape, width, bound, shards=(), held_as=jnp.bfloat16):
    values = width * jax.random.normal(key, shape, jnp.float32)
    if shards:
        values = values * shard_levels(key, shape, shards, -0.22, 0.18)
    return jnp.clip(values, -bound, bound).astype(held_as)


def setup_inputs(seed: int = 0) -> dict:
    splits = jax.random.split(jax.random.key(seed), 14)
    tokens = draw_tokens(jax.random.fold_in(splits[13], 71), 0)
    gain_attn = jnp.clip(1.0 + 0.1 * jax.random.normal(splits[1], (D,), jnp.float32), 0.5, 1.5)
    gain_ffn = jnp.clip(1.0 + 0.1 * jax.random.normal(splits[2], (D,), jnp.float32), 0.5, 1.5)
    w_query = normal_values(splits[3], (D, D), D ** -0.5, 0.125, ((0, 2), (1, 4)))
    w_key = normal_values(splits[4], (D, D), D ** -0.5, 0.125, ((0, 2), (1, 4)))
    w_value = normal_values(splits[5], (D, D), D ** -0.5, 0.125, ((0, 2), (1, 4)))
    w_out = normal_values(splits[6], (D, D), (D // 64) ** -0.5, 1.0, ((0, 4), (1, 2)))
    w_gate = normal_values(splits[7], (D, FF), D ** -0.5, 0.125, ((0, 2), (1, 4)))
    w_up = normal_values(splits[8], (D, FF), D ** -0.5, 0.125, ((0, 2), (1, 4)))
    w_down = normal_values(splits[9], (FF, D), FF ** -0.5, 0.0625, ((0, 4), (1, 2)))
    grad_output = normal_values(splits[10], (TOKENS, D), 1.0, 6.0, ((0, 4), (1, 8)))
    segments = draw_segments(jax.random.fold_in(splits[13], 71), 0)
    positions = draw_positions(jax.random.fold_in(splits[13], 71), 0)
    return dict(tokens=tokens, gain_attn=gain_attn, gain_ffn=gain_ffn, w_query=w_query, w_key=w_key, w_value=w_value, w_out=w_out, w_gate=w_gate, w_up=w_up, w_down=w_down, grad_output=grad_output, segments=segments, positions=positions)


@jax.custom_vjp
def low(v):
    return lax.optimization_barrier(v.astype(jnp.bfloat16)).astype(jnp.float32)

@jax.custom_vjp
def low_back(v):
    return v

def low_keep(v):
    return (low(v), None)

def low_pass(kept, grad):
    return (grad,)

def back_keep(v):
    return (v, None)

def back_low(kept, grad):
    return (low(grad),)
low.defvjp(low_keep, low_pass)
low_back.defvjp(back_keep, back_low)
norm_eps = 1e-05
rope_base = 130000.0
masked_score = -1e+30

def matmul(left, right):
    return jnp.dot(left, right, precision=lax.Precision.HIGHEST, preferred_element_type=jnp.float32)

def rms_norm(values, gain_vec):
    scale_inv = lax.rsqrt(lax.optimization_barrier(jnp.mean(values * values, axis=-1, keepdims=True)) + norm_eps)
    return low(values * scale_inv * gain_vec)

def rope_tables(positions):
    half_steps = jnp.arange(HD // 2, dtype=jnp.float32)
    inv_freq = rope_base ** (-2.0 * half_steps / HD)
    angles = positions.astype(jnp.float32)[:, None] * inv_freq[None, :]
    return (jnp.cos(angles)[:, None, :], jnp.sin(angles)[:, None, :])

def rotate(values, cos_table, sin_table):
    half_dim = values.shape[-1] // 2
    first_half = values[..., :half_dim]
    second_half = values[..., half_dim:]
    return jnp.concatenate([first_half * cos_table - second_half * sin_table, second_half * cos_table + first_half * sin_table], axis=-1)

def attend_sequence(inputs):
    queries, key_rows, value_rows, segment = inputs
    raw_scores = low_back(jnp.einsum('qhd,khd->hqk', queries, key_rows, precision=lax.Precision.HIGHEST))
    slot_index = jnp.arange(SEQ)
    allowed = (slot_index[None, :] <= slot_index[:, None]) & (segment[:, None] == segment[None, :])
    scores = jnp.where(allowed[None], raw_scores * HD ** (-0.5), masked_score)
    log_total = jnp.log(lax.optimization_barrier(jnp.sum(jnp.exp(scores), axis=-1, keepdims=True)))
    attn_probs = low(jnp.exp(scores - log_total))
    return jnp.einsum('hqk,khd->qhd', attn_probs, value_rows, precision=lax.Precision.HIGHEST)

def layer_forward(residual, gain_attn, gain_ffn, w_query, w_key, w_value, w_out, w_gate, w_up, w_down, segments, positions):
    seq_total = segments.shape[0]
    tok_total = seq_total * SEQ
    cos_table, sin_table = rope_tables(positions.reshape(tok_total))
    head_shape = (tok_total, HEADS, HD)
    seq_shape = (seq_total, SEQ, HEADS, HD)
    hidden_one = rms_norm(residual, gain_attn)
    queries = low(rotate(low_back(matmul(hidden_one, w_query)).reshape(head_shape), cos_table, sin_table))
    key_rows = low(rotate(low_back(matmul(hidden_one, w_key)).reshape(head_shape), cos_table, sin_table))
    value_rows = low(low_back(matmul(hidden_one, w_value)))
    attended = lax.map(jax.checkpoint(attend_sequence), (queries.reshape(seq_shape), key_rows.reshape(seq_shape), value_rows.reshape(seq_shape), segments))
    heads_out = low(low_back(attended.reshape(tok_total, D)))
    middle = residual + low_back(matmul(heads_out, w_out))
    hidden_two = rms_norm(middle, gain_ffn)
    gate_pre = low_back(matmul(hidden_two, w_gate))
    up_pre = low_back(matmul(hidden_two, w_up))
    hidden_units = low(gate_pre * jax.nn.sigmoid(gate_pre) * up_pre)
    return middle + low_back(matmul(hidden_units, w_down))

def reference(tokens, gain_attn, gain_ffn, w_query, w_key, w_value, w_out, w_gate, w_up, w_down, grad_output, segments, positions):
    weights = tuple((item.astype(jnp.float32) for item in (gain_attn, gain_ffn, w_query, w_key, w_value, w_out, w_gate, w_up, w_down)))
    group_size = math.gcd(4, NSEQ)
    scan_count = NSEQ // group_size
    inputs_all = (tokens.astype(jnp.float32).reshape(scan_count, group_size * SEQ, D), grad_output.astype(jnp.float32).reshape(scan_count, group_size * SEQ, D), segments.reshape(scan_count, group_size, SEQ), positions.reshape(scan_count, group_size, SEQ))

    def scan_step(totals, inputs):
        block_in, block_grad, block_seg, block_pos = inputs

        def forward(residual, *params):
            return layer_forward(residual, *params, block_seg, block_pos)
        result, pullback = jax.vjp(forward, block_in, *weights)
        gradients = pullback(block_grad)
        totals = tuple((total + grad_item for total, grad_item in zip(totals, gradients[1:])))
        return (totals, (result, gradients[0]))
    empty_grads = tuple((jnp.zeros(item.shape, jnp.float32) for item in weights))
    totals, (results, grad_in) = lax.scan(scan_step, empty_grads, inputs_all)
    output = results.reshape(TOKENS, D)
    grad_tokens = grad_in.reshape(TOKENS, D)
    gain_shape = (N_ROW * N_COL, N_DP, D // (N_ROW * N_COL * N_DP))
    return (output, grad_tokens, totals[0].reshape(gain_shape), totals[1].reshape(gain_shape), totals[2].reshape(N_ROW, N_DP, D // (N_ROW * N_DP), D), totals[3].reshape(N_ROW, N_DP, D // (N_ROW * N_DP), D), totals[4].reshape(N_ROW, N_DP, D // (N_ROW * N_DP), D), totals[5].reshape(N_COL, N_DP, D // (N_COL * N_DP), D), totals[6].reshape(N_ROW, N_DP, D // (N_ROW * N_DP), FF), totals[7].reshape(N_ROW, N_DP, D // (N_ROW * N_DP), FF), totals[8].reshape(N_COL, N_DP, FF // (N_COL * N_DP), D))
```

```python
import jax
import jax.numpy as jnp
from jax import lax
from jax.sharding import PartitionSpec as P

D = 2048
HD = 64


norm_eps = 1e-05
rope_base = 130000.0
masked_score = -1e30


def width_total(partial_sums):
    return lax.psum(partial_sums, ("row", "col"))


def gather_cols(pieces):
    return lax.all_gather(pieces, "col", axis=1, tiled=True)


def sum_cols(partial_sums):
    return lax.psum_scatter(partial_sums.astype(jnp.bfloat16), "col", scatter_dimension=1, tiled=True).astype(jnp.float32)


def gather_rows(pieces):
    return lax.all_gather(pieces, "row", axis=2, tiled=True)


def sum_rows(partial_sums):
    return lax.psum_scatter(partial_sums.astype(jnp.bfloat16), "row", scatter_dimension=2, tiled=True).astype(jnp.float32)


def sum_dp(partial_sums):
    return lax.psum_scatter(partial_sums.astype(jnp.bfloat16), "dp", scatter_dimension=0, tiled=True).astype(jnp.float32)


def product(left, right):
    return jnp.dot(left, right, preferred_element_type=jnp.float32)


def contract_rows(left, right):
    return jnp.einsum("ta,tb->ab", left, right, preferred_element_type=jnp.float32)


def times_transposed(left, right):
    return jnp.einsum("ta,ba->tb", left, right, preferred_element_type=jnp.float32)


def norm_forward(residual, gain_vec):
    squares = width_total(jnp.sum(residual * residual, axis=1))
    scale_inv = lax.rsqrt(squares / D + norm_eps)
    normed = residual * scale_inv[:, None]
    return (normed, scale_inv, (normed * gain_vec).astype(jnp.bfloat16))


def norm_backward(grad_normed_out, normed, scale_inv, gain_vec):
    grad_normed = grad_normed_out * gain_vec
    inner_sum = width_total(jnp.sum(grad_normed * normed, axis=1))
    grad_input = scale_inv[:, None] * (grad_normed - normed * (inner_sum / D)[:, None])
    return (grad_input, jnp.sum(grad_normed_out * normed, axis=0))


def rope_tables(positions):
    half_steps = jnp.arange(HD // 2, dtype=jnp.float32)
    inv_freq = rope_base ** (-2.0 * half_steps / HD)
    angles = positions.astype(jnp.float32)[:, None] * inv_freq[None, :]
    return (jnp.cos(angles)[:, None, :], jnp.sin(angles)[:, None, :])


def rotate(values, cos_table, sin_table):
    half_dim = values.shape[-1] // 2
    first_half = values[..., :half_dim]
    second_half = values[..., half_dim:]
    return jnp.concatenate(
        [
            first_half * cos_table - second_half * sin_table,
            second_half * cos_table + first_half * sin_table,
        ],
        axis=-1,
    )


def unrotate(values, cos_table, sin_table):
    half_dim = values.shape[-1] // 2
    first_half = values[..., :half_dim]
    second_half = values[..., half_dim:]
    return jnp.concatenate(
        [
            first_half * cos_table + second_half * sin_table,
            second_half * cos_table - first_half * sin_table,
        ],
        axis=-1,
    )


def score_rows(query_part, key_rows, segment, row_start):
    row_count = query_part.shape[0]
    seq_len = key_rows.shape[0]
    scores = jnp.einsum(
        "qhd,khd->hqk", query_part, key_rows, preferred_element_type=jnp.float32
    ) * key_rows.shape[2] ** (-0.5)
    query_slot = row_start + jnp.arange(row_count)
    key_slot = jnp.arange(seq_len)
    query_seg = segment[row_start : row_start + row_count]
    allowed = (key_slot[None, :] <= query_slot[:, None]) & (query_seg[:, None] == segment[None, :])
    return jnp.where(allowed[None], scores, masked_score)


def attend_forward(inputs):
    queries, key_rows, value_rows, segment = inputs
    seq_len = queries.shape[0]
    span = min(512, seq_len)
    results = []
    log_parts = []
    for row_start in range(0, seq_len, span):
        scores = score_rows(queries[row_start : row_start + span], key_rows, segment, row_start)
        log_total = jnp.log(jnp.sum(jnp.exp(scores), axis=-1))
        attn_probs = jnp.exp(scores - log_total[..., None]).astype(jnp.bfloat16)
        results.append(
            jnp.einsum("hqk,khd->qhd", attn_probs, value_rows, preferred_element_type=jnp.float32)
        )
        log_parts.append(log_total)
    return (jnp.concatenate(results, axis=0), jnp.concatenate(log_parts, axis=1))


def attend_backward(inputs):
    queries, key_rows, value_rows, segment, log_totals, grad_rows = inputs
    seq_len = queries.shape[0]
    span = min(512, seq_len)
    score_scale = queries.shape[2] ** (-0.5)
    grad_query_parts = []
    grad_keys = jnp.zeros(key_rows.shape, jnp.float32)
    grad_values = jnp.zeros(value_rows.shape, jnp.float32)
    for row_start in range(0, seq_len, span):
        query_part = queries[row_start : row_start + span]
        grad_part = grad_rows[row_start : row_start + span]
        scores = score_rows(query_part, key_rows, segment, row_start)
        attn_probs = jnp.exp(scores - log_totals[:, row_start : row_start + span, None])
        grad_probs = jnp.einsum(
            "qhd,khd->hqk", grad_part, value_rows, preferred_element_type=jnp.float32
        )
        weighted = jnp.sum(attn_probs * grad_probs, axis=-1, keepdims=True)
        grad_scores = (attn_probs * (grad_probs - weighted) * score_scale).astype(jnp.bfloat16)
        grad_query_parts.append(
            jnp.einsum("hqk,khd->qhd", grad_scores, key_rows, preferred_element_type=jnp.float32)
        )
        grad_keys = grad_keys + jnp.einsum(
            "hqk,qhd->khd", grad_scores, query_part, preferred_element_type=jnp.float32
        )
        grad_values = grad_values + jnp.einsum(
            "hqk,qhd->khd",
            attn_probs.astype(jnp.bfloat16),
            grad_part,
            preferred_element_type=jnp.float32,
        )
    return (jnp.concatenate(grad_query_parts, axis=0), grad_keys, grad_values)


def as_blocks(matrix):
    return matrix.reshape((1, 1) + matrix.shape)


def body(
    tokens,
    gain_attn,
    gain_ffn,
    w_query,
    w_key,
    w_value,
    w_out,
    w_gate,
    w_up,
    w_down,
    grad_output,
    segments,
    positions,
):
    residual = tokens.astype(jnp.float32)
    tok_count = residual.shape[0]
    seq_count, seq_len = segments.shape
    cos_table, sin_table = rope_tables(positions.reshape(tok_count))
    normed_one, inv_one, hidden_one = norm_forward(residual, gain_attn)
    gathered_one = gather_cols(hidden_one)
    projected = jnp.stack(
        [
            product(gathered_one, w_query),
            product(gathered_one, w_key),
            product(gathered_one, w_value),
        ]
    )
    local_qkv = sum_rows(projected)
    head_shape = (seq_count, seq_len, local_qkv.shape[2] // HD, HD)
    flat_heads = (tok_count, local_qkv.shape[2] // HD, HD)
    queries = (
        rotate(local_qkv[0].reshape(flat_heads), cos_table, sin_table)
        .astype(jnp.bfloat16)
        .reshape(head_shape)
    )
    key_rows = (
        rotate(local_qkv[1].reshape(flat_heads), cos_table, sin_table)
        .astype(jnp.bfloat16)
        .reshape(head_shape)
    )
    value_rows = local_qkv[2].astype(jnp.bfloat16).reshape(head_shape)
    attended, log_totals = lax.map(attend_forward, (queries, key_rows, value_rows, segments))
    heads_out = attended.reshape(tok_count, -1).astype(jnp.bfloat16)
    heads_all = gather_rows(heads_out[None])[0]
    middle = residual + sum_cols(product(heads_all, w_out))
    normed_two, inv_two, hidden_two = norm_forward(middle, gain_ffn)
    gathered_two = gather_cols(hidden_two)
    gate_up = sum_rows(jnp.stack([product(gathered_two, w_gate), product(gathered_two, w_up)]))
    gate_pre = gate_up[0]
    up_pre = gate_up[1]
    gate_sigmoid = jax.nn.sigmoid(gate_pre)
    hidden_units = (gate_pre * gate_sigmoid * up_pre).astype(jnp.bfloat16)
    units_all = gather_rows(hidden_units[None])[0]
    output = middle + sum_cols(product(units_all, w_down))
    grad_all = gather_cols(grad_output)
    units_all = gather_rows(hidden_units[None])[0]
    grad_w_down = contract_rows(units_all, grad_all)
    grad_units = sum_rows(times_transposed(grad_all, w_down)[None])[0]
    grad_gate = (
        grad_units * up_pre * gate_sigmoid * (1.0 + gate_pre * (1.0 - gate_sigmoid))
    ).astype(jnp.bfloat16)
    grad_up = (grad_units * gate_pre * gate_sigmoid).astype(jnp.bfloat16)
    gathered_two = gather_cols(hidden_two)
    grad_pair = gather_rows(jnp.stack([grad_gate, grad_up]))
    grad_w_gate = contract_rows(gathered_two, grad_pair[0])
    grad_w_up = contract_rows(gathered_two, grad_pair[1])
    grad_two = sum_cols(
        times_transposed(grad_pair[0], w_gate) + times_transposed(grad_pair[1], w_up)
    )
    grad_norm_two, grad_gain_ffn = norm_backward(grad_two, normed_two, inv_two, gain_ffn)
    grad_middle = grad_output.astype(jnp.float32) + grad_norm_two
    grad_branch = gather_cols(grad_middle.astype(jnp.bfloat16))
    heads_all = gather_rows(heads_out[None])[0]
    grad_w_out = contract_rows(heads_all, grad_branch)
    grad_heads = sum_rows(times_transposed(grad_branch, w_out)[None])[0].astype(jnp.bfloat16)
    grad_queries, grad_keys, grad_values = lax.map(
        attend_backward,
        (queries, key_rows, value_rows, segments, log_totals, grad_heads.reshape(head_shape)),
    )
    grad_query_pre = (
        unrotate(grad_queries.reshape(flat_heads), cos_table, sin_table)
        .reshape(tok_count, -1)
        .astype(jnp.bfloat16)
    )
    grad_key_pre = (
        unrotate(grad_keys.reshape(flat_heads), cos_table, sin_table)
        .reshape(tok_count, -1)
        .astype(jnp.bfloat16)
    )
    grad_value_pre = grad_values.reshape(tok_count, -1).astype(jnp.bfloat16)
    grad_triple = gather_rows(jnp.stack([grad_query_pre, grad_key_pre, grad_value_pre]))
    gathered_one = gather_cols(hidden_one)
    grad_w_query = contract_rows(gathered_one, grad_triple[0])
    grad_w_key = contract_rows(gathered_one, grad_triple[1])
    grad_w_value = contract_rows(gathered_one, grad_triple[2])
    grad_one = sum_cols(
        times_transposed(grad_triple[0], w_query)
        + times_transposed(grad_triple[1], w_key)
        + times_transposed(grad_triple[2], w_value)
    )
    grad_norm_one, grad_gain_attn = norm_backward(grad_one, normed_one, inv_one, gain_attn)
    grad_tokens = grad_middle + grad_norm_one
    reduced = (
        lax.psum_scatter(grad_gain_attn, "dp", scatter_dimension=0, tiled=True),
        lax.psum_scatter(grad_gain_ffn, "dp", scatter_dimension=0, tiled=True),
        sum_dp(grad_w_query),
        sum_dp(grad_w_key),
        sum_dp(grad_w_value),
        sum_dp(grad_w_out),
        sum_dp(grad_w_gate),
        sum_dp(grad_w_up),
        sum_dp(grad_w_down),
    )
    gate_share, up_share = (reduced[6], reduced[7])
    return (
        output,
        grad_tokens,
        as_blocks(reduced[0]),
        as_blocks(reduced[1]),
        as_blocks(reduced[2]),
        as_blocks(reduced[3]),
        as_blocks(reduced[4]),
        as_blocks(reduced[5]),
        as_blocks(gate_share),
        as_blocks(up_share),
        as_blocks(reduced[8]),
    )


def solution(mesh):
    return jax.shard_map(
        body,
        mesh=mesh,
        in_specs=(
            P("dp", ("row", "col")),
            P(("row", "col")),
            P(("row", "col")),
            P("row", "col"),
            P("row", "col"),
            P("row", "col"),
            P("col", "row"),
            P("row", "col"),
            P("row", "col"),
            P("col", "row"),
            P("dp", ("row", "col")),
            P("dp", None),
            P("dp", None),
        ),
        out_specs=(
            P("dp", ("row", "col")),
            P("dp", ("row", "col")),
            P(("row", "col"), "dp", None),
            P(("row", "col"), "dp", None),
            P("row", "dp", None, "col"),
            P("row", "dp", None, "col"),
            P("row", "dp", None, "col"),
            P("col", "dp", None, "row"),
            P("row", "dp", None, "col"),
            P("row", "dp", None, "col"),
            P("col", "dp", None, "row"),
        ),
        check_vma=False,
    )
```

```python
import functools

import jax
import jax.numpy as jnp
from jax import lax
from jax.experimental import pallas as pl
from jax.experimental.pallas import tpu as pltpu
from jax.sharding import PartitionSpec as P

MESH = pl.DeviceIdType.MESH
F32 = jnp.float32
BF16 = jnp.bfloat16
HD = 64
N_CHUNK = 4
norm_eps = 1e-05
rope_base = 130000.0
masked_score = -1e30
VMEM_LIMIT = 64 * 1024 * 1024 - 65536


def dot_nn(left, right):
    return lax.dot_general(left, right, (((1,), (0,)), ((), ())), preferred_element_type=F32)


def dot_nt(left, right):
    return lax.dot_general(left, right, (((1,), (1,)), ((), ())), preferred_element_type=F32)


def dot_tn(left, right):
    return lax.dot_general(left, right, (((0,), (0,)), ((), ())), preferred_element_type=F32)


def span(start, size):
    return pl.ds(pl.multiple_of(start, size), size)


def remote(src, dst, send_sem, recv_sem, where):
    return pltpu.make_async_remote_copy(
        src_ref=src,
        dst_ref=dst,
        send_sem=send_sem,
        recv_sem=recv_sem,
        device_id=where,
        device_id_type=MESH,
    )


def greet(peers):
    barrier = pltpu.get_barrier_semaphore()
    count = jnp.int32(0)
    for present, where in peers:

        @pl.when(present)
        def _():
            pl.semaphore_signal(barrier, inc=1, device_id=where, device_id_type=MESH)

        count = count + present.astype(jnp.int32)
    pl.semaphore_wait(barrier, count)


def line_peers(r, c, n_col):
    always = c >= 0
    return [
        (c > 0, {"col": jnp.maximum(c - 1, 0)}),
        (c < n_col - 1, {"col": jnp.minimum(c + 1, n_col - 1)}),
        (always, {"row": 1 - r}),
    ]


def group_peers(r, c, n_col):
    return [
        ((c != at) | (r != half), {"row": jnp.int32(half), "col": jnp.int32(at)})
        for half in range(2)
        for at in range(n_col)
    ]


class Gather:
    def __init__(self, full, send, recv, r, c, n_col, width, n_chunk=N_CHUNK):
        self.full, self.send, self.recv = full, send, recv
        self.r, self.c, self.n_col, self.width = r, c, n_col, width
        self.n_chunk = n_chunk
        self.rows = full.shape[0] // n_chunk

    def piece(self, half, at, chunk):
        return self.full.at[
            span(chunk * self.rows, self.rows),
            span(half * (self.n_col * self.width) + at * self.width, self.width),
        ]

    def copy(self, way, at, chunk):
        piece = self.piece(self.r, at, chunk)
        where = (
            {"col": jnp.maximum(self.c - 1, 0)},
            {"col": jnp.minimum(self.c + 1, self.n_col - 1)},
            {"row": 1 - self.r},
        )[way]
        return remote(
            piece, piece, self.send.at[way, at, chunk], self.recv.at[self.r, at, chunk], where
        )

    def wait(self, half, at, chunk):
        piece = self.piece(half, at, chunk)
        remote(
            piece, piece, self.send.at[0, at, chunk], self.recv.at[half, at, chunk], {"row": 1 - self.r}
        ).wait_recv()

    def start(self, chunk):
        c = self.c

        @pl.when(c > 0)
        def _():
            self.copy(0, c, chunk).start()

        @pl.when(c < self.n_col - 1)
        def _():
            self.copy(1, c, chunk).start()

        self.copy(2, c, chunk).start()

    def relay(self, distance, chunk):
        c, last = self.c, self.n_col - 1

        @pl.when(c + distance <= last)
        def _():
            at = c + distance
            self.wait(self.r, at, chunk)

            @pl.when(c > 0)
            def _():
                self.copy(0, at, chunk).start()

            self.copy(2, at, chunk).start()

        @pl.when(c - distance >= 0)
        def _():
            at = c - distance
            self.wait(self.r, at, chunk)

            @pl.when(c < last)
            def _():
                self.copy(1, at, chunk).start()

            self.copy(2, at, chunk).start()

    def wait_other(self, chunk):
        for at in range(self.n_col):
            self.wait(1 - self.r, at, chunk)

    def finish(self):
        c, last = self.c, self.n_col - 1

        def one(step, carry):
            at, chunk = step // self.n_chunk, step % self.n_chunk

            @pl.when((c > 0) & (at >= c))
            def _():
                self.copy(0, at, chunk).wait_send()

            @pl.when((c < last) & (at <= c))
            def _():
                self.copy(1, at, chunk).wait_send()

            self.copy(2, at, chunk).wait_send()
            return carry

        lax.fori_loop(0, self.n_col * self.n_chunk, one, 0)


class Scatter:
    def __init__(self, part, stage, inbox, send, recv, c, n_col, n_chunk=N_CHUNK):
        self.part, self.stage, self.inbox = part, stage, inbox
        self.send, self.recv, self.c, self.n_col = send, recv, c, n_col
        self.n_chunk = n_chunk

    def copy(self, way, chunk, dest):
        where = jnp.clip(self.c + 1 - 2 * way, 0, self.n_col - 1)
        return remote(
            self.stage.at[chunk, dest],
            self.inbox.at[way, chunk, dest],
            self.send.at[chunk, dest],
            self.recv.at[way, chunk, dest],
            {"col": where},
        )

    def hop(self, way, chunk, dest, fed):
        c, last = self.c, self.n_col - 1
        valid = jnp.where(way == 0, dest > c, dest < c)
        has_in = jnp.where(way == 0, c > 0, c < last)
        if fed:

            @pl.when(valid & has_in)
            def _():
                copy = self.copy(way, chunk, dest)
                copy.wait_recv()
                total = self.part[chunk, dest] + self.inbox[way, chunk, dest].astype(F32)
                self.stage[chunk, dest] = total.astype(BF16)
                copy.start()
        else:

            @pl.when(valid & jnp.logical_not(has_in))
            def _():
                self.stage[chunk, dest] = self.part[chunk, dest].astype(BF16)
                self.copy(way, chunk, dest).start()

    def open(self, chunk):
        last = self.n_col - 1
        for step in range(last):
            self.hop(jnp.int32(0), chunk, jnp.int32(last - step), False)
            self.hop(jnp.int32(1), chunk, jnp.int32(step), False)

    def forward(self, chunk, steps=None):
        last = self.n_col - 1
        near = (self.c >= self.n_col // 2).astype(jnp.int32)
        for step in range(last) if steps is None else steps:
            for way in (near, 1 - near):
                dest = jnp.where(way == 0, last - step, step)
                self.hop(way, chunk, dest, True)

    def total(self, chunk, put):
        c, last = self.c, self.n_col - 1
        put(self.part[chunk, c], True)
        for way, present in ((0, c > 0), (1, c < last)):

            @pl.when(present)
            def _():
                self.copy(way, chunk, c).wait_recv()
                put(self.inbox[way, chunk, c].astype(F32), False)

    def finish(self):
        def one(step, carry):
            chunk, dest = step // self.n_col, step % self.n_col

            @pl.when(dest != self.c)
            def _():
                self.copy(0, chunk, dest).wait_send()

            return carry

        lax.fori_loop(0, self.n_chunk * self.n_col, one, 0)

    @staticmethod
    def scratch(n_col, rows, width, n_chunk=N_CHUNK):
        return [
            pltpu.VMEM((n_chunk, n_col, rows, width), F32),
            pltpu.VMEM((n_chunk, n_col, rows, width), BF16),
            pltpu.VMEM((2, n_chunk, n_col, rows, width), BF16),
            pltpu.SemaphoreType.DMA((n_chunk, n_col)),
            pltpu.SemaphoreType.DMA((2, n_chunk, n_col)),
        ]


def gather_sems(n_col, n_chunk=N_CHUNK):
    return [
        pltpu.SemaphoreType.DMA((3, n_col, n_chunk)),
        pltpu.SemaphoreType.DMA((2, n_col, n_chunk)),
    ]


def lanes(shape):
    return lax.broadcasted_iota(jnp.int32, shape, len(shape) - 1)


def swap_halves(values):
    half, width = HD // 2, values.shape[-1]
    low = (lanes(values.shape) & (HD - 1)) < half
    return jnp.where(
        low, pltpu.roll(values, width - half, 1), pltpu.roll(values, half, 1)
    )


def widen(table, width):
    return jnp.concatenate([table] * (width // table.shape[-1]), axis=-1)


def vmem():
    return pl.BlockSpec(memory_space=pltpu.VMEM)


def anywhere():
    return pl.BlockSpec(memory_space=pl.ANY)


def kernel_call(body, name, ident, outs, out_any, in_specs, scratch, flops):
    return pl.pallas_call(
        body,
        out_shape=outs,
        in_specs=in_specs,
        out_specs=[anywhere() if flag else vmem() for flag in out_any],
        scratch_shapes=scratch,
        compiler_params=pltpu.CompilerParams(
            collective_id=ident, has_side_effects=True, vmem_limit_bytes=VMEM_LIMIT
        ),
        cost_estimate=pl.CostEstimate(flops=flops, bytes_accessed=1 << 24, transcendentals=0),
        name=name,
    )


def project_kernel(
    n_col,
    x, gains, cos_table, sin_table, wq, wk, wv, wo, wg, wu, wd,
    q, k, v, h1, r1, gain_full, wo_other, wg_other, wu_other, wd_other,
    full, hidden, weights, ag_send, ag_recv, g_send, g_recv, w_send, w_recv, local,
):
    r, c = lax.axis_index("row"), lax.axis_index("col")
    width = x.shape[1]
    half = n_col * width
    heads = wq.shape[1] // 2
    units = wg.shape[1] // 2
    me = r * n_col + c
    greet(group_peers(r, c, n_col))
    gather = Gather(full, ag_send, ag_recv, r, c, n_col, width)

    own = pltpu.make_async_copy(x, full.at[:, span(me * width, width)], local.at[0])
    own.start()
    held = [
        pltpu.make_async_copy(
            w.at[:, span(r * heads, heads)],
            weights.at[span(r * half, half), pl.ds(n * heads, heads)],
            local.at[1 + n],
        )
        for n, w in enumerate((wq, wk, wv))
    ]
    for copy in held:
        copy.start()
    own.wait()
    for chunk in range(N_CHUNK):
        gather.start(chunk)

    gain_copies = []
    for half_at in range(2):
        for at in range(n_col):
            to = half_at * n_col + at
            where = {"row": jnp.int32(half_at), "col": jnp.int32(at)}
            gain_copies.append(
                (to, remote(gains, gain_full.at[me], g_send.at[to], g_recv.at[me], where))
            )
    for to, copy in gain_copies:
        pl.when(to != me)(copy.start)
    gain_full[me] = gains[...]

    other = {"row": 1 - r}
    moved = [
        remote(
            w.at[:, span((1 - r) * heads, heads)],
            weights.at[span(r * half, half), pl.ds(n * heads, heads)],
            w_send.at[n], w_recv.at[n], other,
        )
        for n, w in enumerate((wq, wk, wv))
    ]
    moved.append(remote(wo.at[span((1 - r) * heads, heads), :], wo_other, w_send.at[3], w_recv.at[3], other))
    moved.append(remote(wg.at[:, span((1 - r) * units, units)], wg_other, w_send.at[4], w_recv.at[4], other))
    moved.append(remote(wu.at[:, span((1 - r) * units, units)], wu_other, w_send.at[5], w_recv.at[5], other))
    moved.append(remote(wd.at[span((1 - r) * units, units), :], wd_other, w_send.at[6], w_recv.at[6], other))
    for copy in moved:
        copy.start()

    rows = gather.rows

    def chunk_rows(chunk):
        return span(chunk * rows, rows)

    def compute(chunk):
        at = chunk_rows(chunk)
        total = jnp.zeros((rows, 1), F32)
        for block in range(2 * n_col):
            values = full[at, pl.ds(block * width, width)].astype(F32)
            total = total + jnp.sum(values * values, axis=1, keepdims=True)
        scale = lax.rsqrt(total * (1.0 / (2 * half)) + norm_eps)
        r1[at, :] = jnp.broadcast_to(scale, (rows, r1.shape[1]))
        for block in range(2 * n_col):
            values = full[at, pl.ds(block * width, width)].astype(F32)
            hidden[:, pl.ds(block * width, width)] = (
                values * scale * gain_full[block, 0:1, :]
            ).astype(BF16)
        h1[at, :] = hidden[:, span(r * half, half)]
        cos_rows = widen(cos_table[at, :], heads)
        sin_rows = widen(sin_table[at, :], heads)
        for n, out in enumerate((q, k, v)):
            values = dot_nn(hidden[...], weights[:, pl.ds(n * heads, heads)])
            if n < 2:
                values = values * cos_rows + swap_halves(values) * sin_rows
            out[at, :] = values.astype(BF16)

    for distance in range(1, n_col):
        if distance == n_col - 1:
            for copy in held:
                copy.wait()
            for copy in moved[:3]:
                copy.wait_recv()
            for to, copy in gain_copies:

                @pl.when(to != me)
                def _():
                    remote(
                        gains, gain_full.at[to], g_send.at[to], g_recv.at[to], other
                    ).wait_recv()

            def last(chunk, carry):
                gather.relay(distance, chunk)
                gather.wait_other(chunk)
                compute(chunk)
                return carry

            lax.fori_loop(0, N_CHUNK, last, 0)
        else:
            for chunk in range(N_CHUNK):
                gather.relay(distance, chunk)

    gather.finish()
    for to, copy in gain_copies:
        pl.when(to != me)(copy.wait_send)
    for copy in moved[3:]:
        copy.wait_recv()
    for copy in moved:
        copy.wait_send()


def project(n_col, x, gains, cos_table, sin_table, wq, wk, wv, wo, wg, wu, wd):
    tok, width = x.shape
    full = 2 * n_col * width
    half = n_col * width
    heads, units = wq.shape[1] // 2, wg.shape[1] // 2
    shape = jax.ShapeDtypeStruct
    outs = [
        shape((tok, heads), BF16), shape((tok, heads), BF16), shape((tok, heads), BF16),
        shape((tok, half), BF16), shape((tok, 128), F32), shape((2 * n_col, 8, width), F32),
        shape((heads, wo.shape[1]), BF16), shape((half, units), BF16),
        shape((half, units), BF16), shape((units, wd.shape[1]), BF16),
    ]
    scratch = [
        pltpu.VMEM((tok, full), BF16),
        pltpu.VMEM((tok // N_CHUNK, full), BF16),
        pltpu.VMEM((full, 3 * heads), BF16),
        *gather_sems(n_col),
        pltpu.SemaphoreType.DMA((2 * n_col,)),
        pltpu.SemaphoreType.DMA((2 * n_col,)),
        pltpu.SemaphoreType.DMA((7,)),
        pltpu.SemaphoreType.DMA((7,)),
        pltpu.SemaphoreType.DMA((4,)),
    ]
    return kernel_call(
        functools.partial(project_kernel, n_col), "project", 1, outs, [False] * 6 + [True] * 4,
        [anywhere(), vmem(), vmem(), vmem()] + [anywhere()] * 7, scratch, 6 * tok * full * heads,
    )(x, gains, cos_table, sin_table, wq, wk, wv, wo, wg, wu, wd)


def allowed_pairs(seg_col, seg_row, chunk, rows, keys):
    query_at = chunk * rows + lax.broadcasted_iota(jnp.int32, (rows, keys), 0)
    key_at = lanes((rows, keys))
    return (key_at <= query_at) & (seg_col[:, 0:1] == seg_row)


def of_head(values, head):
    return jnp.where((lanes(values.shape) // HD) == head, values, jnp.zeros_like(values))


def attend_kernel(
    n_col,
    q, k, v, seg_row, seg_col, x, wo, dy,
    heads_all, inv_sum, middle, dy_full,
    w_out, part, stage, inbox, rs_send, rs_recv, ag_send, ag_recv, h_send, h_recv, local,
):
    r, c = lax.axis_index("row"), lax.axis_index("col")
    tok, heads = q.shape
    width = x.shape[1]
    rows = tok // N_CHUNK
    me = r * n_col + c
    greet(line_peers(r, c, n_col))
    gather = Gather(dy_full, ag_send, ag_recv, r, c, n_col, width)
    scatter = Scatter(part, stage, inbox, rs_send, rs_recv, c, n_col)
    own = pltpu.make_async_copy(dy, dy_full.at[:, span(me * width, width)], local.at[0])
    own.start()
    load = pltpu.make_async_copy(wo, w_out, local.at[1])
    load.start()
    own.wait()
    for chunk in range(N_CHUNK):
        gather.start(chunk)

    def heads_copy(chunk):
        piece = heads_all.at[pl.ds(chunk * rows, rows), span(r * heads, heads)]
        return remote(piece, piece, h_send.at[chunk], h_recv.at[chunk], {"row": 1 - r})

    def attend(chunk):
        at = pl.ds(chunk * rows, rows)
        keys = (chunk + 1) * rows
        allowed = allowed_pairs(seg_col[at, :], seg_row[:, 0:keys], chunk, rows, keys)

        def head_step(head, carry):
            total, inverse = carry
            scores = dot_nt(of_head(q[at, :], head), k[0:keys, :]) * HD**-0.5
            weights = jnp.exp(jnp.where(allowed, scores, masked_score))
            inv = 1.0 / jnp.sum(weights, axis=1, keepdims=True)
            probs = (weights * inv).astype(BF16)
            total = total + dot_nn(probs, of_head(v[0:keys, :], head))
            inverse = jnp.where(lanes((rows, 128)) == head, inv, inverse)
            return total, inverse

        total, inverse = lax.fori_loop(
            0, heads // HD, head_step, (jnp.zeros((rows, heads), F32), jnp.zeros((rows, 128), F32))
        )
        heads_all[at, span(r * heads, heads)] = total.astype(BF16)
        inv_sum[at, :] = inverse

    def contract(chunk):
        values = heads_all[pl.ds(chunk * rows, rows), :]
        for dest in range(n_col):
            part[chunk, dest] = dot_nn(values, w_out[:, pl.ds(dest * width, width)])

    for chunk in range(N_CHUNK):
        attend(chunk)
        heads_copy(chunk).start()
        if chunk >= 1:
            for n in range(N_CHUNK):
                gather.relay(chunk, n)
        if chunk == 0:
            load.wait()
        heads_copy(chunk).wait_recv()
        contract(chunk)
        scatter.open(chunk)
        if chunk >= 1:
            scatter.forward(chunk - 1)
    scatter.forward(N_CHUNK - 1)
    for chunk in range(N_CHUNK):
        at = pl.ds(chunk * rows, rows)
        middle[at, :] = x[at, :].astype(F32)

        def put(value, first):
            middle[at, :] += value

        scatter.total(chunk, put)
        gather.wait_other(chunk)
    gather.finish()
    scatter.finish()
    for chunk in range(N_CHUNK):
        heads_copy(chunk).wait_send()


def attend(n_col, q, k, v, seg_row, seg_col, x, wo, dy):
    tok, heads = q.shape
    width = x.shape[1]
    shape = jax.ShapeDtypeStruct
    outs = [
        shape((tok, 2 * heads), BF16),
        shape((tok, 128), F32),
        shape((tok, width), F32),
        shape((tok, 2 * n_col * width), BF16),
    ]
    scratch = [
        pltpu.VMEM(wo.shape, BF16),
        *Scatter.scratch(n_col, tok // N_CHUNK, width),
        *gather_sems(n_col),
        pltpu.SemaphoreType.DMA((N_CHUNK,)),
        pltpu.SemaphoreType.DMA((N_CHUNK,)),
        pltpu.SemaphoreType.DMA((2,)),
    ]
    return kernel_call(
        functools.partial(attend_kernel, n_col), "attend", 2, outs, [False] * 4,
        [vmem()] * 6 + [anywhere()] * 2, scratch, 8 * tok * tok * heads,
    )(q, k, v, seg_row, seg_col, x, wo, dy)


class Stats:
    def __init__(self, box, send, recv, r, c, n_col):
        self.box, self.send, self.recv = box, send, recv
        self.r, self.c, self.n_col = r, c, n_col
        self.me = r * n_col + c

    def copy(self, chunk, half, at):
        mine = self.box.at[self.me, chunk]
        where = {"row": jnp.int32(half), "col": jnp.int32(at)}
        return remote(
            mine, mine, self.send.at[half * self.n_col + at, chunk], self.recv.at[self.me, chunk], where
        )

    def each(self, act):
        for half in range(2):
            for at in range(self.n_col):
                pl.when(half * self.n_col + at != self.me)(functools.partial(act, half, at))

    def publish(self, chunk, column):
        wide = jnp.broadcast_to(column, (column.shape[0], 128)).T
        self.box[self.me, chunk] = wide[0:8, :]
        self.each(lambda half, at: self.copy(chunk, half, at).start())

    def total(self, chunk):
        def arrive(half, at):
            slot = self.box.at[half * self.n_col + at, chunk]
            remote(
                slot, slot, self.send.at[0, chunk], self.recv.at[half * self.n_col + at, chunk],
                {"row": 1 - self.r},
            ).wait_recv()

        self.each(arrive)
        total = self.box[0, chunk]
        for at in range(1, 2 * self.n_col):
            total = total + self.box[at, chunk]
        return jnp.concatenate([total] * 16, axis=0).T[:, 0:1]

    def finish(self, n_chunk=N_CHUNK):
        for chunk in range(n_chunk):
            self.each(lambda half, at: self.copy(chunk, half, at).wait_send())

    @staticmethod
    def scratch(n_col, rows, n_chunk=N_CHUNK):
        return [
            pltpu.VMEM((2 * n_col, n_chunk, 8, rows), F32),
            pltpu.SemaphoreType.DMA((2 * n_col, n_chunk)),
            pltpu.SemaphoreType.DMA((2 * n_col, n_chunk)),
        ]


def ffn_kernel(
    n_col,
    middle, gain_full, dy_full, wg, wu, wd, wg_other, wu_other, wd_other,
    h2, units, grad_gate, grad_up, grad_middle, grad_branch, gain_sum,
    full, hidden, gate_own, up_own, down_own, gate_far, up_far, scale_wide, grad_two,
    part, stage, inbox, rs_send, rs_recv, box, st_send, st_recv,
    ag_send, ag_recv, x_send, x_recv, local,
):
    r, c = lax.axis_index("row"), lax.axis_index("col")
    tok, width = middle.shape
    half = n_col * width
    n_unit = down_own.shape[0]
    rows = tok // N_CHUNK
    me = r * n_col + c
    greet(group_peers(r, c, n_col))
    gather = Gather(full, ag_send, ag_recv, r, c, n_col, width)
    scatter = Scatter(part, stage, inbox, rs_send, rs_recv, c, n_col)
    stats = Stats(box, st_send, st_recv, r, c, n_col)
    for chunk in range(N_CHUNK):
        at = pl.ds(chunk * rows, rows)
        full[at, span(me * width, width)] = middle[at, :].astype(BF16)
    gather.start(0)
    gather.start(1)
    mine, far = span(r * n_unit, n_unit), span((1 - r) * n_unit, n_unit)
    near_rows, far_rows = span(r * half, half), span((1 - r) * half, half)
    loads = [
        pltpu.make_async_copy(src, dst, local.at[n])
        for n, (src, dst) in enumerate(
            (
                (wg.at[:, mine], gate_own.at[near_rows, :]),
                (wg_other, gate_own.at[far_rows, :]),
                (wu.at[:, mine], up_own.at[near_rows, :]),
                (wu_other, up_own.at[far_rows, :]),
                (wd.at[mine, :], down_own.at[:, near_rows]),
                (wd_other, down_own.at[:, far_rows]),
                (wg.at[:, far], gate_far),
                (wu.at[:, far], up_far),
            )
        )
    ]
    for copy in loads:
        copy.start()

    def chunk_rows(chunk):
        return span(chunk * rows, rows)

    def exchange(chunk):
        copies = []
        for n, array in enumerate((grad_gate, grad_up, units)):
            piece = array.at[chunk_rows(chunk), mine]
            copies.append(remote(piece, piece, x_send.at[n, chunk], x_recv.at[n, chunk], {"row": 1 - r}))
        return copies

    def norm(chunk):
        at = chunk_rows(chunk)
        total = jnp.zeros((rows, 1), F32)
        for block in range(2 * n_col):
            values = full[at, pl.ds(block * width, width)].astype(F32)
            total = total + jnp.sum(values * values, axis=1, keepdims=True)
        scale = lax.rsqrt(total * (1.0 / (2 * half)) + norm_eps)
        scale_wide[at, :] = jnp.broadcast_to(scale, (rows, scale_wide.shape[1]))
        for block in range(2 * n_col):
            values = full[at, pl.ds(block * width, width)].astype(F32)
            hidden[:, pl.ds(block * width, width)] = (
                values * scale * gain_full[block, 1:2, :]
            ).astype(BF16)
        h2[at, :] = hidden[:, span(r * half, half)]

    def units_part(chunk, first, last):
        at = chunk_rows(chunk)
        tile = 256

        def one(step, carry):
            cols = span(step * tile, tile)
            gate = dot_nn(hidden[...], gate_own[:, cols])
            up = dot_nn(hidden[...], up_own[:, cols])
            grad = dot_nt(dy_full[at, :], down_own[cols, :])
            sig = jax.nn.sigmoid(gate)
            act = gate * sig
            put = span(r * n_unit + step * tile, tile)
            units[at, put] = (act * up).astype(BF16)
            grad_gate[at, put] = (grad * up * sig * (1.0 + gate * (1.0 - sig))).astype(BF16)
            grad_up[at, put] = (grad * act).astype(BF16)
            return carry

        lax.fori_loop(first, last, one, 0)

    def back(chunk):
        at = chunk_rows(chunk)
        for copy in exchange(chunk)[:2]:
            copy.wait_recv()

        def one(dest, carry):
            near = span(r * half + dest * width, width)
            cols = span(dest * width, width)
            part[chunk, dest] = (
                dot_nt(grad_gate[at, mine], gate_own[near, :])
                + dot_nt(grad_gate[at, far], gate_far[cols, :])
                + dot_nt(grad_up[at, mine], up_own[near, :])
                + dot_nt(grad_up[at, far], up_far[cols, :])
            )
            return carry

        lax.fori_loop(0, n_col, one, 0)
        scatter.open(chunk)

    def settle(chunk):
        at = chunk_rows(chunk)

        def put(value, first):
            if first:
                grad_two[at, :] = value
            else:
                grad_two[at, :] += value

        scatter.total(chunk, put)
        normed = middle[at, :] * scale_wide[at, 0:1]
        product = grad_two[at, :] * normed
        stats.publish(chunk, jnp.sum(product * gain_full[me, 1:2, :], axis=1, keepdims=True))
        gain_sum[...] += jnp.sum(product.reshape(rows // 8, 8, width), axis=0)

    def conclude(chunk):
        at = chunk_rows(chunk)
        mean = stats.total(chunk) * (1.0 / (2 * half))
        scale = scale_wide[at, 0:1]
        normed = middle[at, :] * scale
        grad = dy_full[at, span(me * width, width)].astype(F32) + scale * (
            grad_two[at, :] * gain_full[me, 1:2, :] - normed * mean
        )
        grad_middle[at, :] = grad
        grad_branch[at, :] = grad.astype(BF16)

    gain_sum[...] = jnp.zeros_like(gain_sum)
    tiles = n_unit // 256
    for distance in range(1, n_col):
        gather.relay(distance, 0)
    gather.wait_other(0)
    for chunk in range(N_CHUNK):
        if chunk + 2 < N_CHUNK:
            gather.start(chunk + 2)
        norm(chunk)
        if chunk == 0:
            for copy in loads[:6]:
                copy.wait()
        units_part(chunk, 0, tiles // 2)
        if chunk + 1 < N_CHUNK:
            gather.relay(1, chunk + 1)
        units_part(chunk, tiles // 2, tiles)
        for copy in exchange(chunk):
            copy.start()
        if chunk + 1 < N_CHUNK:
            gather.relay(2, chunk + 1)
        if chunk == 0:
            for copy in loads[6:]:
                copy.wait()
        if chunk >= 1:
            back(chunk - 1)
        if chunk >= 2:
            scatter.forward(chunk - 2)
        if chunk + 1 < N_CHUNK:
            gather.relay(3, chunk + 1)
            gather.wait_other(chunk + 1)
    back(N_CHUNK - 1)
    scatter.forward(N_CHUNK - 2)
    for chunk in range(N_CHUNK - 1):
        settle(chunk)
    scatter.forward(N_CHUNK - 1)
    for chunk in range(N_CHUNK - 1):
        conclude(chunk)
    settle(N_CHUNK - 1)
    conclude(N_CHUNK - 1)
    gather.finish()
    scatter.finish()
    stats.finish()
    for chunk in range(N_CHUNK):
        copies = exchange(chunk)
        copies[2].wait_recv()
        for copy in copies:
            copy.wait_send()


def ffn(n_col, middle, gain_full, dy_full, wg, wu, wd, wg_other, wu_other, wd_other):
    tok, width = middle.shape
    half, n_unit = n_col * width, wg.shape[1] // 2
    shape = jax.ShapeDtypeStruct
    outs = [
        shape((tok, half), BF16),
        shape((tok, 2 * n_unit), BF16), shape((tok, 2 * n_unit), BF16), shape((tok, 2 * n_unit), BF16),
        shape((tok, width), F32), shape((tok, width), BF16), shape((8, width), F32),
    ]
    rows = tok // N_CHUNK
    scratch = [
        pltpu.VMEM((tok, 2 * half), BF16),
        pltpu.VMEM((rows, 2 * half), BF16),
        pltpu.VMEM((2 * half, n_unit), BF16),
        pltpu.VMEM((2 * half, n_unit), BF16),
        pltpu.VMEM((n_unit, 2 * half), BF16),
        pltpu.VMEM((half, n_unit), BF16),
        pltpu.VMEM((half, n_unit), BF16),
        pltpu.VMEM((tok, 128), F32),
        pltpu.VMEM((tok, width), F32),
        *Scatter.scratch(n_col, rows, width),
        *Stats.scratch(n_col, rows),
        *gather_sems(n_col),
        pltpu.SemaphoreType.DMA((3, N_CHUNK)),
        pltpu.SemaphoreType.DMA((3, N_CHUNK)),
        pltpu.SemaphoreType.DMA((8,)),
    ]
    return kernel_call(
        functools.partial(ffn_kernel, n_col), "ffn", 3, outs, [False] * 7,
        [vmem()] * 3 + [anywhere()] * 6, scratch, 20 * tok * half * n_unit,
    )(middle, gain_full, dy_full, wg, wu, wd, wg_other, wu_other, wd_other)


class Reduce:
    def __init__(self, tile, out, stage_one, inbox_one, stage_two, inbox_two, send, recv):
        d = lax.axis_index("dp")
        self.x, self.y = d % 2, d // 2
        self.tile, self.out = tile, out
        self.stage_one, self.inbox_one = stage_one, inbox_one
        self.stage_two, self.inbox_two = stage_two, inbox_two
        self.send, self.recv = send, recv
        self.along_x = {"dp": self.y * 2 + 1 - self.x}
        self.along_y = {"dp": (1 - self.y) * 2 + self.x}

    def copy_one(self, side, n):
        return remote(
            self.stage_one.at[side, n], self.inbox_one.at[side, n],
            self.send.at[side, n], self.recv.at[side, n],
            self.along_y if side else self.along_x,
        )

    def copy_two(self, side):
        return remote(
            self.stage_two.at[side], self.inbox_two.at[side],
            self.send.at[side, 2], self.recv.at[side, 2],
            self.along_x if side else self.along_y,
        )

    def first(self, side):
        near = self.x if side else self.y
        for n in (1 - near, near):
            owner = (1 - self.y) * 2 + n if side else n * 2 + 1 - self.x
            self.stage_one[side, n] = self.tile(owner, side).astype(BF16)
            self.copy_one(side, n).start()

    def second(self, side):
        n = 1 - (self.x if side else self.y)
        owner = self.y * 2 + n if side else n * 2 + self.x
        value = self.tile(owner, side)
        self.copy_one(side, n).wait_recv()
        self.stage_two[side] = (value + self.inbox_one[side, n].astype(F32)).astype(BF16)
        self.copy_two(side).start()

    def last(self, side):
        n = self.x if side else self.y
        cols = self.inbox_two.shape[-1]
        value = self.tile(self.y * 2 + self.x, side)
        self.copy_one(side, n).wait_recv()
        value = value + self.inbox_one[side, n].astype(F32)
        self.copy_two(side).wait_recv()
        self.out[:, side * cols : (side + 1) * cols] = value + self.inbox_two[side].astype(F32)

    def finish(self):
        for side in range(2):
            for n in range(2):
                self.copy_one(side, n).wait_send()
            self.copy_two(side).wait_send()

    @staticmethod
    def scratch(rows, cols):
        return [
            pltpu.VMEM((2, 2, rows, cols), BF16),
            pltpu.VMEM((2, 2, rows, cols), BF16),
            pltpu.VMEM((2, rows, cols), BF16),
            pltpu.VMEM((2, rows, cols), BF16),
            pltpu.SemaphoreType.DMA((2, 3)),
            pltpu.SemaphoreType.DMA((2, 3)),
        ]


def square_peers():
    d = lax.axis_index("dp")
    x, y = d % 2, d // 2
    always = d >= 0
    return [(always, {"dp": y * 2 + 1 - x}), (always, {"dp": (1 - y) * 2 + x})]


def branch_kernel(
    n_col, n_sum,
    branch, units, wd, middle, dy_full, h2, grad_gate, wo, wo_other,
    *refs,
):
    (output, grad_heads, branch_half), refs = refs[:3], refs[3:]
    sums, refs = refs[:n_sum], refs[n_sum:]
    (full, down, dy_half, w_out, part, stage, inbox, rs_send, rs_recv, ag_send, ag_recv, local), refs = (
        refs[:12],
        refs[12:],
    )
    r, c = lax.axis_index("row"), lax.axis_index("col")
    tok, width = middle.shape
    half = n_col * width
    heads = grad_heads.shape[1]
    rows = tok // N_CHUNK
    me = r * n_col + c
    greet(line_peers(r, c, n_col) + (square_peers() if n_sum else []))
    gather = Gather(full, ag_send, ag_recv, r, c, n_col, width)
    scatter = Scatter(part, stage, inbox, rs_send, rs_recv, c, n_col)
    own = pltpu.make_async_copy(branch, full.at[:, span(me * width, width)], local.at[0])
    own.start()
    mine, other = span(r * half, half), span((1 - r) * half, half)
    loads = [
        pltpu.make_async_copy(dy_full.at[:, mine], dy_half, local.at[1]),
        pltpu.make_async_copy(wd, down, local.at[2]),
        pltpu.make_async_copy(wo.at[span(r * heads, heads), :], w_out.at[:, mine], local.at[3]),
        pltpu.make_async_copy(wo_other, w_out.at[:, other], local.at[4]),
    ]
    for copy in loads:
        copy.start()
    own.wait()
    for chunk in range(N_CHUNK):
        gather.start(chunk)
    for copy in loads:
        copy.wait()

    def tile_of(left, right, n_row):
        cols = right.shape[1] // 2

        def tile(owner, side):
            return dot_tn(left[:, span(owner * n_row, n_row)], right[:, side * cols : (side + 1) * cols])

        return tile

    panels = []
    if n_sum:
        for n, (left, right) in enumerate(((units, dy_half), (h2, grad_gate))):
            tile = tile_of(left, right, sums[n].shape[0])
            panels.append(Reduce(tile, sums[n], *refs[6 * n : 6 * n + 6]))

    def contract(chunk):
        values = units[pl.ds(chunk * rows, rows), :]
        for dest in range(n_col):
            part[chunk, dest] = dot_nn(values, down[:, pl.ds(dest * width, width)])

    for panel in panels[:1]:
        panel.first(0)
        panel.first(1)
    for chunk in range(N_CHUNK):
        gather.relay(1, chunk)
        contract(chunk)
        scatter.open(chunk)
    for panel in panels[1:]:
        panel.first(0)
        panel.first(1)
    for panel in panels[:1]:
        panel.second(0)
        panel.second(1)
    for chunk in range(N_CHUNK):
        gather.relay(2, chunk)
        scatter.forward(chunk, (0,))
    for chunk in range(N_CHUNK):
        gather.relay(3, chunk)
        scatter.forward(chunk, (1, 2))
    for chunk in range(N_CHUNK):
        at = pl.ds(chunk * rows, rows)
        gather.wait_other(chunk)
        grad_heads[at, :] = dot_nt(full[at, :], w_out[...]).astype(BF16)
        branch_half[at, :] = full[at, mine]
    for panel in panels[1:]:
        panel.second(0)
        panel.second(1)
    for chunk in range(N_CHUNK):
        at = pl.ds(chunk * rows, rows)
        output[at, :] = middle[at, :]

        def put(value, first):
            output[at, :] += value

        scatter.total(chunk, put)
    for panel in panels:
        panel.last(0)
        panel.last(1)
    gather.finish()
    scatter.finish()
    for panel in panels:
        panel.finish()


def branch_back(n_col, n_dp, branch, units, wd, middle, dy_full, h2, grad_gate, wo, wo_other):
    tok, width = middle.shape
    half, heads = n_col * width, wo_other.shape[0]
    rows = tok // N_CHUNK
    shape = jax.ShapeDtypeStruct
    outs = [shape((tok, width), F32), shape((tok, heads), BF16), shape((tok, half), BF16)]
    scratch = [
        pltpu.VMEM((tok, 2 * half), BF16),
        pltpu.VMEM(wd.shape, BF16),
        pltpu.VMEM((tok, half), BF16),
        pltpu.VMEM((heads, 2 * half), BF16),
        *Scatter.scratch(n_col, rows, width),
        *gather_sems(n_col),
        pltpu.SemaphoreType.DMA((5,)),
    ]
    n_sum = 0
    if n_dp == 4:
        n_sum = 2
        down_rows, gate_rows = wd.shape[0] // 4, half // 4
        outs += [shape((down_rows, wd.shape[1]), F32), shape((gate_rows, grad_gate.shape[1]), F32)]
        scratch += Reduce.scratch(down_rows, wd.shape[1] // 2)
        scratch += Reduce.scratch(gate_rows, grad_gate.shape[1] // 2)
    return kernel_call(
        functools.partial(branch_kernel, n_col, n_sum), "branch", 4, outs, [False] * len(outs),
        [anywhere(), vmem(), anywhere(), vmem(), anywhere(), vmem(), vmem(), anywhere(), anywhere()],
        scratch, 12 * tok * half * half,
    )(branch, units, wd, middle, dy_full, h2, grad_gate, wo, wo_other)


def attend_back_kernel(
    n_col, n_dp, n_sum,
    q, k, v, grad_heads, seg_row, seg_col, inv_sum, cos_table, sin_table, x, r1, gain_full, grad_middle,
    gain_two, h1, wq, wk, wv, h2, grad_up, heads_all, branch_half,
    *refs,
):
    (grad_tokens, gain_sums, triple), refs = refs[:3], refs[3:]
    sums, refs = refs[:n_sum], refs[n_sum:]
    (
        weights, grad_k, grad_v, grad_q, grad_one, gain_mine, gain_box, part, stage, inbox, rs_send, rs_recv,
        box, st_send, st_recv, x_send, x_recv, g_send, g_recv, local,
    ), refs = refs[:20], refs[20:]
    r, c, d = lax.axis_index("row"), lax.axis_index("col"), lax.axis_index("dp")
    tok, width = x.shape
    half = n_col * width
    heads = q.shape[1]
    rows = tok // N_CHUNK
    me = r * n_col + c
    dp_peers = [(d != at, {"dp": jnp.int32(at)}) for at in range(n_dp)]
    greet(group_peers(r, c, n_col) + dp_peers)
    scatter = Scatter(part, stage, inbox, rs_send, rs_recv, c, n_col)
    stats = Stats(box, st_send, st_recv, r, c, n_col)
    loads = []
    for n, w in enumerate((wq, wk, wv)):
        for side in range(2):
            loads.append(
                pltpu.make_async_copy(
                    w.at[:, pl.ds(side * heads, heads)],
                    weights.at[:, pl.ds((side * 3 + n) * heads, heads)],
                    local.at[n, side],
                )
            )
    for copy in loads:
        copy.start()

    def tile_of(left, right, n_row):
        cols = right.shape[1] // 2

        def tile(owner, side):
            return dot_tn(left[:, span(owner * n_row, n_row)], right[:, side * cols : (side + 1) * cols])

        return tile

    panels = []
    if n_sum:
        for n, (left, right) in enumerate(((h2, grad_up), (heads_all, branch_half), (h1, triple))):
            tile = tile_of(left, right, sums[n].shape[0])
            panels.append(Reduce(tile, sums[n], *refs[6 * n : 6 * n + 6]))

    def exchange(chunk):
        piece = triple.at[pl.ds(chunk * rows, rows), span(r * 3 * heads, 3 * heads)]
        return remote(piece, piece, x_send.at[chunk], x_recv.at[chunk], {"row": 1 - r})

    def attend(chunk):
        at = pl.ds(chunk * rows, rows)
        keys = (chunk + 1) * rows
        allowed = allowed_pairs(seg_col[at, :], seg_row[:, 0:keys], chunk, rows, keys)
        grad_q[...] = jnp.zeros_like(grad_q)

        def head_step(head, carry):
            query = of_head(q[at, :], head)
            grad = of_head(grad_heads[at, :], head)
            scores = dot_nt(query, k[0:keys, :]) * HD**-0.5
            inv = jnp.sum(jnp.where(lanes((rows, 128)) == head, inv_sum[at, :], 0.0), axis=1, keepdims=True)
            probs = jnp.exp(jnp.where(allowed, scores, masked_score)) * inv
            grad_probs = dot_nt(grad, v[0:keys, :])
            weighted = jnp.sum(probs * grad_probs, axis=1, keepdims=True)
            grad_scores = (probs * (grad_probs - weighted) * HD**-0.5).astype(BF16)
            grad_q[...] += dot_nn(grad_scores, of_head(k[0:keys, :], head))
            grad_k[0:keys, :] += dot_tn(grad_scores, query)
            grad_v[0:keys, :] += dot_tn(probs.astype(BF16), grad)
            return carry

        lax.fori_loop(0, heads // HD, head_step, 0)
        cos_rows = widen(cos_table[at, :], heads)
        sin_rows = widen(sin_table[at, :], heads)
        for n, value in enumerate((grad_q[...], grad_k[at, :])):
            value = value * cos_rows - swap_halves(value) * sin_rows
            triple[at, span((r * 3 + n) * heads, heads)] = value.astype(BF16)
        triple[at, span((r * 3 + 2) * heads, heads)] = grad_v[at, :].astype(BF16)
        exchange(chunk).start()

    def contract(chunk):
        at = pl.ds(chunk * rows, rows)
        exchange(chunk).wait_recv()
        for dest in range(n_col):
            part[chunk, dest] = dot_nt(triple[at, :], weights[dest * width : (dest + 1) * width, :])
        scatter.open(chunk)

    def settle(chunk):
        at = pl.ds(chunk * rows, rows)

        def put(value, first):
            if first:
                grad_one[at, :] = value
            else:
                grad_one[at, :] += value

        scatter.total(chunk, put)
        product = grad_one[at, :] * (x[at, :].astype(F32) * r1[at, 0:1])
        stats.publish(chunk, jnp.sum(product * gain_full[me, 0:1, :], axis=1, keepdims=True))
        gain_mine[0] += jnp.sum(product.reshape(rows // 8, 8, width), axis=0)

    def conclude(chunk):
        at = pl.ds(chunk * rows, rows)
        mean = stats.total(chunk) * (1.0 / (2 * half))
        scale = r1[at, 0:1]
        grad_tokens[at, :] = grad_middle[at, :] + scale * (
            grad_one[at, :] * gain_full[me, 0:1, :] - x[at, :].astype(F32) * scale * mean
        )

    gain_mine[0] = jnp.zeros(gain_mine.shape[1:], F32)
    gain_mine[1] = gain_two[...]
    grad_k[...] = jnp.zeros_like(grad_k)
    grad_v[...] = jnp.zeros_like(grad_v)
    for panel in panels[:1]:
        panel.first(0)
        panel.first(1)
    order = list(reversed(range(N_CHUNK)))
    for n, chunk in enumerate(order):
        attend(chunk)
        if n == 0:
            for copy in loads:
                copy.wait()
        if n >= 1:
            contract(order[n - 1])
        if n >= 2:
            scatter.forward(order[n - 2])
        for panel in panels[1:2]:
            if n < 2:
                panel.first(n)
        for panel in panels[:1]:
            if n >= 2:
                panel.second(n - 2)
    contract(order[-1])
    for panel in panels[2:]:
        panel.first(0)
        panel.first(1)
    scatter.forward(order[-2])
    for chunk in order[:-1]:
        settle(chunk)
    scatter.forward(order[-1])
    for panel in panels[1:2]:
        panel.second(0)
        panel.second(1)
    for chunk in order[:-1]:
        conclude(chunk)
    settle(order[-1])
    gain_box[d] = gain_mine[...]

    def gain_copy(at):
        return remote(gain_box.at[d], gain_box.at[d], g_send.at[at], g_recv.at[d], {"dp": jnp.int32(at)})

    for at in range(n_dp):
        pl.when(at != d)(gain_copy(at).start)
    for panel in panels[2:]:
        panel.second(0)
        panel.second(1)
    conclude(order[-1])
    for at in range(n_dp):

        @pl.when(at != d)
        def _():
            remote(
                gain_box.at[at], gain_box.at[at], g_send.at[at], g_recv.at[at], {"dp": jnp.int32(at)}
            ).wait_recv()

    gain_total = gain_box[0]
    for at in range(1, n_dp):
        gain_total = gain_total + gain_box[at]
    gain_sums[...] = gain_total
    for panel in panels:
        panel.last(0)
        panel.last(1)
    scatter.finish()
    stats.finish()
    for chunk in range(N_CHUNK):
        exchange(chunk).wait_send()
    for at in range(n_dp):
        pl.when(at != d)(gain_copy(at).wait_send)
    for panel in panels:
        panel.finish()


def attend_back(
    n_col, n_dp,
    q, k, v, grad_heads, seg_row, seg_col, inv_sum, cos_table, sin_table, x, r1, gain_full, grad_middle,
    gain_two, h1, wq, wk, wv, h2, grad_up, heads_all, branch_half,
):
    tok, width = x.shape
    half, heads = n_col * width, q.shape[1]
    rows = tok // N_CHUNK
    shape = jax.ShapeDtypeStruct
    outs = [shape((tok, width), F32), shape((2, 8, width), F32), shape((tok, 6 * heads), BF16)]
    scratch = [
        pltpu.VMEM((half, 6 * heads), BF16),
        pltpu.VMEM((tok, heads), F32),
        pltpu.VMEM((tok, heads), F32),
        pltpu.VMEM((rows, heads), F32),
        pltpu.VMEM((tok, width), F32),
        pltpu.VMEM((2, 8, width), F32),
        pltpu.VMEM((n_dp, 2, 8, width), F32),
        *Scatter.scratch(n_col, rows, width),
        *Stats.scratch(n_col, rows),
        pltpu.SemaphoreType.DMA((N_CHUNK,)),
        pltpu.SemaphoreType.DMA((N_CHUNK,)),
        pltpu.SemaphoreType.DMA((n_dp,)),
        pltpu.SemaphoreType.DMA((n_dp,)),
        pltpu.SemaphoreType.DMA((3, 2)),
    ]
    n_sum = 0
    if n_dp == 4:
        n_sum = 3
        for left, right in ((half, grad_up.shape[1]), (2 * heads, half), (half, 6 * heads)):
            outs.append(shape((left // 4, right), F32))
            scratch += Reduce.scratch(left // 4, right // 2)
    return kernel_call(
        functools.partial(attend_back_kernel, n_col, n_dp, n_sum), "attend_back", 5, outs, [False] * len(outs),
        [vmem()] * 15 + [anywhere()] * 3 + [vmem()] * 4, scratch, 16 * tok * tok * heads,
    )(
        q, k, v, grad_heads, seg_row, seg_col, inv_sum, cos_table, sin_table, x, r1, gain_full, grad_middle,
        gain_two, h1, wq, wk, wv, h2, grad_up, heads_all, branch_half,
    )


def rope_tables(positions, width):
    lane = jnp.arange(width) % HD
    inv_freq = rope_base ** (-2.0 * (lane % (HD // 2)).astype(F32) / HD)
    angles = positions.astype(F32)[:, None] * inv_freq[None, :]
    sign = jnp.where(lane < HD // 2, -1.0, 1.0)
    return jnp.cos(angles), jnp.sin(angles) * sign[None, :]


def body(
    n_dp,
    n_col,
    tokens,
    gain_attn,
    gain_ffn,
    w_query,
    w_key,
    w_value,
    w_out,
    w_gate,
    w_up,
    w_down,
    grad_output,
    segments,
    positions,
):
    tok, width = tokens.shape
    heads = w_query.shape[1] // 2
    cos_table, sin_table = rope_tables(positions.reshape(tok), 128)
    gains = jnp.concatenate([gain_attn[None], gain_ffn[None], jnp.zeros((6, width), F32)])
    seg_col = jnp.broadcast_to(segments.reshape(tok, 1), (tok, 128))
    q, k, v, h1, r1, gain_full, wo_other, wg_other, wu_other, wd_other = project(
        n_col, tokens, gains, cos_table, sin_table, w_query, w_key, w_value, w_out, w_gate, w_up, w_down
    )
    heads_all, inv_sum, middle, dy_full = attend(
        n_col, q, k, v, segments, seg_col, tokens, w_out, grad_output
    )
    h2, units, grad_gate, grad_up, grad_middle, branch, gain_two = ffn(
        n_col, middle, gain_full, dy_full, w_gate, w_up, w_down, wg_other, wu_other, wd_other
    )
    output, grad_heads, branch_half, *sums_one = branch_back(
        n_col, n_dp, branch, units, w_down, middle, dy_full, h2, grad_gate, w_out, wo_other
    )
    grad_tokens, gain_sums, triple, *sums_two = attend_back(
        n_col, n_dp, q, k, v, grad_heads, segments, seg_col, inv_sum, cos_table, sin_table, tokens, r1,
        gain_full, grad_middle, gain_two, h1, w_query, w_key, w_value, h2, grad_up, heads_all, branch_half,
    )
    share = width // n_dp
    gain_grads = lax.dynamic_slice(
        jnp.sum(gain_sums, axis=1), (0, lax.axis_index("dp") * share), (2, share)
    )
    if n_dp == 4:
        grad_wd, grad_wg = sums_one
        grad_wu, grad_wo, grad_qkv = sums_two
    else:

        def summed(left, right):
            grad = jnp.einsum("ta,tb->ab", left, right, preferred_element_type=F32).astype(BF16)
            return lax.psum_scatter(grad, "dp", scatter_dimension=0, tiled=True).astype(F32)

        row = lax.axis_index("row")
        dy_half = lax.dynamic_slice(dy_full, (0, row * n_col * width), (tok, n_col * width))
        grad_wd, grad_wg = summed(units, dy_half), summed(h2, grad_gate)
        grad_wu, grad_wo, grad_qkv = summed(h2, grad_up), summed(heads_all, branch_half), summed(h1, triple)
    parts = grad_qkv.reshape(-1, 2, 3, heads)
    grads = [parts[:, :, n].reshape(-1, 2 * heads) for n in range(3)]
    blocks = [m.reshape((1, 1) + m.shape) for m in (*grads, grad_wo, grad_wg, grad_wu, grad_wd)]
    return (output, grad_tokens, gain_grads[0].reshape(1, 1, -1), gain_grads[1].reshape(1, 1, -1), *blocks)


def solution(mesh):
    return jax.shard_map(
        functools.partial(body, mesh.shape["dp"], mesh.shape["col"]),
        mesh=mesh,
        in_specs=(
            P("dp", ("row", "col")),
            P(("row", "col")),
            P(("row", "col")),
            P("row", "col"),
            P("row", "col"),
            P("row", "col"),
            P("col", "row"),
            P("row", "col"),
            P("row", "col"),
            P("col", "row"),
            P("dp", ("row", "col")),
            P("dp", None),
            P("dp", None),
        ),
        out_specs=(
            P("dp", ("row", "col")),
            P("dp", ("row", "col")),
            P(("row", "col"), "dp", None),
            P(("row", "col"), "dp", None),
            P("row", "dp", None, "col"),
            P("row", "dp", None, "col"),
            P("row", "dp", None, "col"),
            P("col", "dp", None, "row"),
            P("row", "dp", None, "col"),
            P("row", "dp", None, "col"),
            P("col", "dp", None, "row"),
        ),
        check_vma=False,
    )
```

```python
import functools

import jax
import jax.numpy as jnp
from jax import lax
from jax.experimental import pallas as pl
from jax.experimental.pallas import tpu as pltpu
from jax.sharding import PartitionSpec as P

MESH = pl.DeviceIdType.MESH
F32 = jnp.float32
BF16 = jnp.bfloat16
HD = 64
N_CHUNK = 4
norm_eps = 1e-05
rope_base = 130000.0
masked_score = -1e30
VMEM_LIMIT = 64 * 1024 * 1024 - 65536


def dot_nn(left, right):
    return lax.dot_general(left, right, (((1,), (0,)), ((), ())), preferred_element_type=F32)


def dot_nt(left, right):
    return lax.dot_general(left, right, (((1,), (1,)), ((), ())), preferred_element_type=F32)


def dot_tn(left, right):
    return lax.dot_general(left, right, (((0,), (0,)), ((), ())), preferred_element_type=F32)


def span(start, size):
    return pl.ds(pl.multiple_of(start, size), size)


def remote(src, dst, send_sem, recv_sem, where):
    return pltpu.make_async_remote_copy(
        src_ref=src,
        dst_ref=dst,
        send_sem=send_sem,
        recv_sem=recv_sem,
        device_id=where,
        device_id_type=MESH,
    )


def greet(peers):
    barrier = pltpu.get_barrier_semaphore()
    count = jnp.int32(0)
    for present, where in peers:

        @pl.when(present)
        def _():
            pl.semaphore_signal(barrier, inc=1, device_id=where, device_id_type=MESH)

        count = count + present.astype(jnp.int32)
    pl.semaphore_wait(barrier, count)


def line_peers(r, c, n_col):
    always = c >= 0
    return [
        (c > 0, {"col": jnp.maximum(c - 1, 0)}),
        (c < n_col - 1, {"col": jnp.minimum(c + 1, n_col - 1)}),
        (always, {"row": 1 - r}),
    ]


def group_peers(r, c, n_col):
    return [
        ((c != at) | (r != half), {"row": jnp.int32(half), "col": jnp.int32(at)})
        for half in range(2)
        for at in range(n_col)
    ]


class Gather:
    def __init__(self, full, send, recv, r, c, n_col, width, n_chunk=N_CHUNK):
        self.full, self.send, self.recv = full, send, recv
        self.r, self.c, self.n_col, self.width = r, c, n_col, width
        self.n_chunk = n_chunk

    def piece(self, half, at, chunk):
        cols = span(half * (self.n_col * self.width) + at * self.width, self.width)
        return self.full.at[chunk, :, cols]

    def copy(self, way, at, chunk):
        piece = self.piece(self.r, at, chunk)
        where = (
            {"col": jnp.maximum(self.c - 1, 0)},
            {"col": jnp.minimum(self.c + 1, self.n_col - 1)},
            {"row": 1 - self.r},
        )[way]
        return remote(
            piece, piece, self.send.at[way, at, chunk], self.recv.at[self.r, at, chunk], where
        )

    def wait(self, half, at, chunk):
        piece = self.piece(half, at, chunk)
        remote(
            piece, piece, self.send.at[0, at, chunk], self.recv.at[half, at, chunk], {"row": 1 - self.r}
        ).wait_recv()

    def start(self, chunk):
        c = self.c

        @pl.when(c > 0)
        def _():
            self.copy(0, c, chunk).start()

        @pl.when(c < self.n_col - 1)
        def _():
            self.copy(1, c, chunk).start()

        self.copy(2, c, chunk).start()

    def relay(self, distance, chunk):
        c, last = self.c, self.n_col - 1

        @pl.when(c + distance <= last)
        def _():
            at = c + distance
            self.wait(self.r, at, chunk)

            @pl.when(c > 0)
            def _():
                self.copy(0, at, chunk).start()

            self.copy(2, at, chunk).start()

        @pl.when(c - distance >= 0)
        def _():
            at = c - distance
            self.wait(self.r, at, chunk)

            @pl.when(c < last)
            def _():
                self.copy(1, at, chunk).start()

            self.copy(2, at, chunk).start()

    def tick(self, now):
        for distance in range(self.n_col - 1, 0, -1):
            chunk = now + 1 - distance

            @pl.when((chunk >= 0) & (chunk < self.n_chunk))
            def _():
                self.relay(distance, chunk)

    def wait_other(self, chunk):
        def one(at, carry):
            self.wait(1 - self.r, at, chunk)
            return carry

        lax.fori_loop(0, self.n_col, one, 0)

    def finish(self):
        c, last = self.c, self.n_col - 1

        def one(step, carry):
            at, chunk = step // self.n_chunk, step % self.n_chunk

            @pl.when((c > 0) & (at >= c))
            def _():
                self.copy(0, at, chunk).wait_send()

            @pl.when((c < last) & (at <= c))
            def _():
                self.copy(1, at, chunk).wait_send()

            self.copy(2, at, chunk).wait_send()
            return carry

        lax.fori_loop(0, self.n_col * self.n_chunk, one, 0)


class Scatter:
    def __init__(self, part, stage, inbox, send, recv, c, n_col, n_chunk=N_CHUNK):
        self.part, self.stage, self.inbox = part, stage, inbox
        self.send, self.recv, self.c, self.n_col = send, recv, c, n_col
        self.n_chunk = n_chunk
        self.width = stage.shape[-1]
        self.middle = (c > 0) & (c < n_col - 1)

    def term(self, chunk, dest):
        return self.part[chunk, :, span(dest * self.width, self.width)]

    def copy(self, way, chunk, dest):
        where = jnp.clip(self.c + 1 - 2 * way, 0, self.n_col - 1)
        return remote(
            self.stage.at[chunk, dest],
            self.inbox.at[way, chunk, dest],
            self.send.at[chunk, dest],
            self.recv.at[way, chunk, dest],
            {"col": where},
        )

    def open(self, chunk):
        @pl.when(jnp.logical_not(self.middle))
        def _():
            way = (self.c > 0).astype(jnp.int32)

            def ship(step, carry):
                dest = jnp.where(way == 0, self.n_col - 1 - step, step)
                self.stage[chunk, dest] = self.term(chunk, dest).astype(BF16)
                self.copy(way, chunk, dest).start()
                return carry

            lax.fori_loop(0, self.n_col - 1, ship, 0)

    def pass_on(self, way, chunk, dest):
        copy = self.copy(way, chunk, dest)
        copy.wait_recv()
        total = self.term(chunk, dest) + self.inbox[way, chunk, dest].astype(F32)
        self.stage[chunk, dest] = total.astype(BF16)
        copy.start()

    def near(self, chunk):
        @pl.when(self.middle)
        def _():
            way = (self.c > 1).astype(jnp.int32)

            def step_on(step, carry):
                self.pass_on(way, chunk, jnp.where(way == 0, self.n_col - 1 - step, step))
                return carry

            lax.fori_loop(0, 2, step_on, 0)

    def far(self, chunk):
        @pl.when(self.middle)
        def _():
            way = (self.c == 1).astype(jnp.int32)
            self.pass_on(way, chunk, jnp.where(self.c == 1, 0, self.n_col - 1))

    def total(self, chunk, out, at):
        c = self.c
        way = (c == 0).astype(jnp.int32)
        self.copy(way, chunk, c).wait_recv()
        out[at, :] = self.term(chunk, c) + self.inbox[way, chunk, c].astype(F32)

        @pl.when(self.middle)
        def _():
            self.copy(1, chunk, c).wait_recv()
            out[at, :] += self.inbox[1, chunk, c].astype(F32)

    def finish(self):
        def one(step, carry):
            chunk, dest = step // self.n_col, step % self.n_col

            @pl.when(dest != self.c)
            def _():
                self.copy(0, chunk, dest).wait_send()

            return carry

        lax.fori_loop(0, self.n_chunk * self.n_col, one, 0)

    @staticmethod
    def scratch(n_col, rows, width, n_chunk=N_CHUNK):
        return [
            pltpu.VMEM((n_chunk, rows, n_col * width), F32),
            pltpu.VMEM((n_chunk, n_col, rows, width), BF16),
            pltpu.VMEM((2, n_chunk, n_col, rows, width), BF16),
            pltpu.SemaphoreType.DMA((n_chunk, n_col)),
            pltpu.SemaphoreType.DMA((2, n_chunk, n_col)),
        ]


def gather_sems(n_col, n_chunk=N_CHUNK):
    return [
        pltpu.SemaphoreType.DMA((3, n_col, n_chunk)),
        pltpu.SemaphoreType.DMA((2, n_col, n_chunk)),
    ]


N_NOTE = 16


def put_notes(full, chunk, cols, values):
    rows = full.shape[1] - N_NOTE
    width = values[0].shape[1]
    at = lax.broadcasted_iota(jnp.int32, (N_NOTE, width), 0)
    notes = jnp.zeros((N_NOTE, width), F32)
    for n, value in enumerate(values):
        for piece in range(3):
            rounded = value.astype(BF16).astype(F32)
            notes = jnp.where(at == 3 * n + piece, rounded, notes)
            value = value - rounded
    full[chunk, rows:, cols] = notes.astype(BF16)


def get_note(full, chunk, cols, n):
    rows = full.shape[1] - N_NOTE
    notes = full[chunk, rows:, cols].astype(F32)
    return (notes[3 * n : 3 * n + 1, :] + notes[3 * n + 1 : 3 * n + 2, :]) + notes[3 * n + 2 : 3 * n + 3, :]


def as_row(column):
    return jnp.broadcast_to(column, (column.shape[0], 128)).T[0:1, :]


def as_column(row):
    return jnp.broadcast_to(row, (128, row.shape[1])).T[:, 0:1]


class Totals:
    def __init__(self, held, sent, inbox, send, recv, r, c):
        self.held, self.sent, self.inbox, self.send, self.recv = held, sent, inbox, send, recv
        self.partners = ({"row": 1 - r}, {"col": c + 1 - 2 * (c % 2)}, {"col": c + 2 - 4 * (c // 2)})

    def note(self, chunk, column):
        self.held[pl.ds(chunk, 1), :] = as_row(column)

    def copy(self, step):
        return remote(
            self.sent.at[step], self.inbox.at[step], self.send.at[step], self.recv.at[step], self.partners[step]
        )

    def exchange(self):
        for step in range(3):
            self.sent[step] = self.held[...]
            copy = self.copy(step)
            copy.start()
            copy.wait_recv()
            self.held[...] += self.inbox[step]

    def column(self, chunk):
        return as_column(self.held[pl.ds(chunk, 1), :])

    def finish(self):
        for step in range(3):
            self.copy(step).wait_send()

    @staticmethod
    def scratch(rows):
        return [
            pltpu.VMEM((8, rows), F32),
            pltpu.VMEM((3, 8, rows), F32),
            pltpu.VMEM((3, 8, rows), F32),
            pltpu.SemaphoreType.DMA((3,)),
            pltpu.SemaphoreType.DMA((3,)),
        ]


def lanes(shape):
    return lax.broadcasted_iota(jnp.int32, shape, len(shape) - 1)


def swap_halves(values):
    half, width = HD // 2, values.shape[-1]
    low = (lanes(values.shape) & (HD - 1)) < half
    return jnp.where(
        low, pltpu.roll(values, width - half, 1), pltpu.roll(values, half, 1)
    )


def widen(table, width):
    return jnp.concatenate([table] * (width // table.shape[-1]), axis=-1)


class Flush:
    def __init__(self, pairs, sems, rows):
        self.pairs, self.sems, self.rows = pairs, sems, rows

    def copy(self, n, chunk):
        source, target = self.pairs[n]
        at = span(chunk * self.rows, self.rows)
        if isinstance(source, tuple):
            source = source[0].at[chunk, 0 : self.rows, source[1]]
        else:
            source = source.at[at, :]
        return pltpu.make_async_copy(source, target.at[at, :], self.sems.at[n, chunk])

    def start(self, chunk, which=None):
        for n in range(len(self.pairs)) if which is None else which:
            self.copy(n, chunk).start()

    def finish(self):
        def one(chunk, carry):
            for n in range(len(self.pairs)):
                self.copy(n, chunk).wait()
            return carry

        lax.fori_loop(0, N_CHUNK, one, 0)


def fetches(pairs, sems):
    copies = [pltpu.make_async_copy(source, target, sems.at[n]) for n, (source, target) in enumerate(pairs)]
    for copy in copies:
        copy.start()
    return copies


def vmem():
    return pl.BlockSpec(memory_space=pltpu.VMEM)


def anywhere():
    return pl.BlockSpec(memory_space=pl.ANY)


def kernel_call(body, name, ident, outs, out_any, in_specs, scratch, flops):
    return pl.pallas_call(
        body,
        out_shape=outs,
        in_specs=in_specs,
        out_specs=[anywhere() if flag else vmem() for flag in out_any],
        scratch_shapes=scratch,
        compiler_params=pltpu.CompilerParams(
            collective_id=ident, has_side_effects=True, vmem_limit_bytes=VMEM_LIMIT
        ),
        cost_estimate=pl.CostEstimate(flops=flops, bytes_accessed=1 << 24, transcendentals=0),
        name=name,
    )


def project_kernel(
    n_col,
    x, gain, positions, segments, rope, dy, wq, wk, wv, wo, wg, wu, wd,
    q_out, k_out, v_out, h1_out, r1, cos_table, sin_table, seg_col, dy_end, dy_mid,
    wo_other, wg_other, wu_other, wd_other,
    full, hidden, weights, q, k, v, h1, ag_send, ag_recv,
    w_send, w_recv, d_send, d_recv, local, flushed,
):
    r, c = lax.axis_index("row"), lax.axis_index("col")
    tok, width = x.shape
    half = n_col * width
    heads = wq.shape[1] // 2
    units = wg.shape[1] // 2
    me = r * n_col + c
    rows = tok // N_CHUNK
    held = fetches(
        [
            (
                w.at[:, span(r * heads, heads)],
                weights.at[span(r * half, half), pl.ds(n * heads, heads)],
            )
            for n, w in enumerate((wq, wk, wv))
        ],
        local,
    )
    mine = span(me * width, width)
    for chunk in range(N_CHUNK):
        values = x[chunk * rows : (chunk + 1) * rows, :]
        full[chunk, 0:rows, mine] = values
        values = values.astype(F32)
        square = as_row(jnp.sum(values * values, axis=1, keepdims=True))
        put_notes(full, chunk, mine, (square, gain[...]))
    greet(group_peers(r, c, n_col))
    gather = Gather(full, ag_send, ag_recv, r, c, n_col, width)
    flush = Flush(((q, q_out), (k, k_out), (v, v_out), (h1, h1_out)), flushed, rows)

    def chunk_rows(chunk):
        return span(chunk * rows, rows)

    gather.start(0)
    gather.start(1)
    other = {"row": 1 - r}
    moved = [
        remote(
            w.at[:, span((1 - r) * heads, heads)],
            weights.at[span(r * half, half), pl.ds(n * heads, heads)],
            w_send.at[n], w_recv.at[n], other,
        )
        for n, w in enumerate((wq, wk, wv))
    ]
    moved.append(remote(wo.at[span((1 - r) * heads, heads), :], wo_other, w_send.at[3], w_recv.at[3], other))
    moved.append(remote(wg.at[:, span((1 - r) * units, units)], wg_other, w_send.at[4], w_recv.at[4], other))
    moved.append(remote(wu.at[:, span((1 - r) * units, units)], wu_other, w_send.at[5], w_recv.at[5], other))
    moved.append(remote(wd.at[span((1 - r) * units, units), :], wd_other, w_send.at[6], w_recv.at[6], other))
    inward = {"col": jnp.where(c == 0, 1, jnp.where(c == 1, 2, jnp.where(c == 2, 1, 2)))}
    at_end = (c == 0) | (c == 3)
    early_end = remote(dy, dy_end, d_send.at[0], d_recv.at[0], inward)
    early_mid = remote(dy, dy_mid, d_send.at[0], d_recv.at[1], inward)

    for copy in moved[:3]:
        copy.start()
    gather.tick(0)
    gather.start(2)
    for copy in moved[3:]:
        copy.start()

    def tables(chunk, carry):
        at = chunk_rows(chunk)
        place = jnp.broadcast_to(positions[:, at].astype(F32), (128, rows)).T
        angles = place * rope[0:1, :]
        cos_table[at, :] = jnp.cos(angles)
        sin_table[at, :] = jnp.sin(angles) * rope[1:2, :]
        seg_col[at, :] = jnp.broadcast_to(segments[:, at].astype(F32), (128, rows)).T
        return carry

    lax.fori_loop(0, N_CHUNK, tables, 0)
    gather.tick(1)
    gather.start(3)
    pl.when(at_end)(early_end.start)
    gather.tick(2)

    def compute(chunk):
        at = chunk_rows(chunk)
        square = jnp.zeros((1, rows), F32)
        for block in range(2 * n_col):
            square = square + get_note(full, chunk, pl.ds(block * width, width), 0)
        scale = lax.rsqrt(as_column(square) * (1.0 / (2 * half)) + norm_eps)
        r1[at, :] = jnp.broadcast_to(scale, (rows, r1.shape[1]))
        for block in range(2 * n_col):
            cols = pl.ds(block * width, width)
            values = full[chunk, 0:rows, cols].astype(F32)
            hidden[:, cols] = (values * scale * get_note(full, chunk, cols, 1)).astype(BF16)
        h1[at, :] = hidden[:, span(r * half, half)]
        values = dot_nn(hidden[...], weights[...])
        cos_rows = widen(cos_table[at, :], heads)
        sin_rows = widen(sin_table[at, :], heads)
        for n, out in enumerate((q, k)):
            part = values[:, n * heads : (n + 1) * heads]
            out[at, :] = (part * cos_rows + swap_halves(part) * sin_rows).astype(BF16)
        v[at, :] = values[:, 2 * heads :].astype(BF16)
        flush.start(chunk)

    for copy in held:
        copy.wait()
    for copy in moved[:3]:
        copy.wait_recv()

    def step(chunk, carry):
        gather.wait_other(chunk)
        compute(chunk)
        gather.tick(chunk + 3)
        pl.when((chunk == 0) & jnp.logical_not(at_end))(early_mid.start)
        return carry

    lax.fori_loop(0, N_CHUNK, step, 0)
    gather.finish()
    for copy in moved[3:]:
        copy.wait_recv()
    for copy in moved:
        copy.wait_send()
    early_end.wait_send()

    @pl.when(jnp.logical_not(at_end))
    def _():
        early_end.wait_recv()
        early_mid.wait_recv()

    flush.finish()


def project(n_col, x, gain, positions, segments, dy, wq, wk, wv, wo, wg, wu, wd):
    tok, width = x.shape
    full = 2 * n_col * width
    half = n_col * width
    heads, units = wq.shape[1] // 2, wg.shape[1] // 2
    lane = jnp.arange(128) % HD
    inv_freq = rope_base ** (-2.0 * (lane % (HD // 2)).astype(F32) / HD)
    rope = jnp.stack([inv_freq, jnp.where(lane < HD // 2, -1.0, 1.0)])
    shape = jax.ShapeDtypeStruct
    outs = [
        shape((tok, heads), BF16), shape((tok, heads), BF16), shape((tok, heads), BF16),
        shape((tok, half), BF16), shape((tok, 128), F32),
        shape((tok, 128), F32), shape((tok, 128), F32), shape((tok, 128), F32),
        shape((tok, width), BF16), shape((tok, width), BF16),
        shape((heads, wo.shape[1]), BF16), shape((half, units), BF16),
        shape((half, units), BF16), shape((units, wd.shape[1]), BF16),
    ]
    scratch = [
        pltpu.VMEM((N_CHUNK, tok // N_CHUNK + N_NOTE, full), BF16),
        pltpu.VMEM((tok // N_CHUNK, full), BF16),
        pltpu.VMEM((full, 3 * heads), BF16),
        *[pltpu.VMEM((tok, heads), BF16)] * 3,
        pltpu.VMEM((tok, half), BF16),
        *gather_sems(n_col),
        pltpu.SemaphoreType.DMA((7,)),
        pltpu.SemaphoreType.DMA((7,)),
        pltpu.SemaphoreType.DMA((1,)),
        pltpu.SemaphoreType.DMA((2,)),
        pltpu.SemaphoreType.DMA((3,)),
        pltpu.SemaphoreType.DMA((4, N_CHUNK)),
    ]
    return kernel_call(
        functools.partial(project_kernel, n_col), "project", 1, outs,
        [True] * 4 + [False] * 4 + [True] * 6,
        [vmem()] * 5 + [anywhere()] * 8, scratch, 6 * tok * full * heads,
    )(x, gain, positions, segments, rope, dy, wq, wk, wv, wo, wg, wu, wd)


def allowed_pairs(seg_col, seg_row, chunk, rows, keys):
    seg_row = seg_row.astype(F32)
    query_at = chunk * rows + lax.broadcasted_iota(jnp.int32, (rows, keys), 0)
    key_at = lanes((rows, keys))
    return (key_at <= query_at) & (seg_col[:, 0:1] == seg_row)


def of_head(values, head):
    return jnp.where((lanes(values.shape) // HD) == head, values, jnp.zeros_like(values))


class LateGather:
    def __init__(self, full, send, recv, r, c, n_col, width):
        self.inner = Gather(full, send, recv, r, c, n_col, width)
        self.c = c
        self.end = (c == 0) | (c == 3)
        self.near_end = jnp.where(c < 2, 0, 3)
        self.far_end = 3 - self.near_end
        self.other = 3 - c
        self.outward = (c >= 2).astype(jnp.int32)

    def copy(self, way, at, chunk):
        piece = self.inner.piece(self.inner.r, at, chunk)
        where = ({"col": self.near_end}, {"col": self.other}, {"row": 1 - self.inner.r})[way]
        return remote(
            piece, piece, self.inner.send.at[way, at, chunk], self.inner.recv.at[self.inner.r, at, chunk], where
        )

    def start(self):
        c = self.c

        def one(chunk, carry):
            self.copy(2, c, chunk).start()

            @pl.when(jnp.logical_not(self.end))
            def _():
                self.copy(0, c, chunk).start()
                self.copy(1, self.near_end, chunk).start()
                self.copy(0, self.other, chunk).start()
                self.copy(2, self.near_end, chunk).start()
                self.copy(2, self.other, chunk).start()

            return carry

        lax.fori_loop(0, N_CHUNK, one, 0)

    def relay(self, chunk):
        @pl.when(jnp.logical_not(self.end))
        def _():
            self.inner.wait(self.inner.r, self.far_end, chunk)
            self.copy(0, self.far_end, chunk).start()
            self.copy(2, self.far_end, chunk).start()

    def collect(self, chunk):
        @pl.when(self.end)
        def _():
            for step in range(3):
                at = jnp.where(self.c == 0, 1 + step, 2 - step)
                self.inner.wait(self.inner.r, at, chunk)
                self.copy(2, at, chunk).start()

    def finish(self):
        def one(step, carry):
            at, chunk = step // 4, step % 4
            self.copy(2, at, chunk).wait_send()

            @pl.when(jnp.logical_not(self.end))
            def _():
                pl.when(at != self.near_end)(lambda: self.copy(0, at, chunk).wait_send())
                pl.when(at == self.near_end)(lambda: self.copy(1, at, chunk).wait_send())

            return carry

        lax.fori_loop(0, 4 * N_CHUNK, one, 0)


def attend_kernel(
    n_col,
    q, k, v, seg_row, seg_col, x, wo, dy, dy_end, dy_mid,
    heads_out, inv_sum, middle_out, dy_out,
    heads_all, middle, dy_full,
    w_out, part, stage, inbox, rs_send, rs_recv, ag_send, ag_recv, h_send, h_recv, local, flushed,
):
    r, c = lax.axis_index("row"), lax.axis_index("col")
    tok, heads = q.shape
    width = x.shape[1]
    rows = tok // N_CHUNK
    me = r * n_col + c
    row_base = r * n_col
    greet(line_peers(r, c, n_col))
    gather = LateGather(dy_full, ag_send, ag_recv, r, c, n_col, width)
    scatter = Scatter(part, stage, inbox, rs_send, rs_recv, c, n_col)
    everything = pl.ds(0, dy_full.shape[2])
    flush = Flush(((heads_all, heads_out), (middle, middle_out), ((dy_full, everything), dy_out)), flushed, rows)

    def block_load(source, block, sem):
        return pltpu.make_async_copy(
            source.reshape(N_CHUNK, rows, width), dy_full.at[:, :, span(block * width, width)], sem
        )

    own = block_load(dy, me, local.at[0])
    own.start()
    early = [
        block_load(dy_end, row_base + gather.near_end, local.at[1]),
        block_load(dy_mid, row_base + gather.other, local.at[2]),
    ]

    @pl.when(jnp.logical_not(gather.end))
    def _():
        for copy in early:
            copy.start()

    load = pltpu.make_async_copy(wo, w_out, local.at[3])
    load.start()
    own.wait()

    @pl.when(jnp.logical_not(gather.end))
    def _():
        for copy in early:
            copy.wait()

    gather.start()

    def heads_copy(chunk):
        piece = heads_all.at[pl.ds(chunk * rows, rows), span(r * heads, heads)]
        return remote(piece, piece, h_send.at[chunk], h_recv.at[chunk], {"row": 1 - r})

    def attend(chunk):
        at = pl.ds(chunk * rows, rows)
        keys = (chunk + 1) * rows
        allowed = allowed_pairs(seg_col[at, :], seg_row[:, 0:keys], chunk, rows, keys)

        def head_step(head, carry):
            total, inverse = carry
            scores = dot_nt(of_head(q[at, :], head), k[0:keys, :]) * HD**-0.5
            weights = jnp.exp(jnp.where(allowed, scores, masked_score))
            inv = 1.0 / jnp.sum(weights, axis=1, keepdims=True)
            probs = (weights * inv).astype(BF16)
            total = total + dot_nn(probs, of_head(v[0:keys, :], head))
            inverse = jnp.where(lanes((rows, 128)) == head, inv, inverse)
            return total, inverse

        total, inverse = lax.fori_loop(
            0, heads // HD, head_step, (jnp.zeros((rows, heads), F32), jnp.zeros((rows, 128), F32))
        )
        heads_all[at, span(r * heads, heads)] = total.astype(BF16)
        inv_sum[at, :] = inverse

    def contract(chunk):
        part[chunk] = dot_nn(heads_all[span(chunk * rows, rows), :], w_out[...])

    for chunk in range(N_CHUNK):
        attend(chunk)
        heads_copy(chunk).start()
        if chunk == 0:
            load.wait()
        if chunk >= 1:
            scatter.near(chunk - 1)
        if chunk >= 2:
            scatter.far(chunk - 2)
            gather.relay(chunk - 2)
        heads_copy(chunk).wait_recv()
        flush.start(chunk, (0,))
        contract(chunk)
        scatter.open(chunk)
    gather.relay(N_CHUNK - 2)
    gather.relay(N_CHUNK - 1)
    scatter.near(N_CHUNK - 1)
    scatter.far(N_CHUNK - 2)
    gather.collect(0)
    scatter.far(N_CHUNK - 1)

    def settle(chunk, carry):
        at = span(chunk * rows, rows)
        scatter.total(chunk, middle, at)
        middle[at, :] += x[at, :].astype(F32)
        pl.when(chunk > 0)(lambda: gather.collect(chunk))
        gather.inner.wait_other(chunk)
        flush.start(chunk, (1, 2))
        return carry

    lax.fori_loop(0, N_CHUNK, settle, 0)
    gather.finish()
    scatter.finish()
    for chunk in range(N_CHUNK):
        heads_copy(chunk).wait_send()
    flush.finish()


def attend(n_col, q, k, v, seg_row, seg_col, x, wo, dy, dy_end, dy_mid):
    tok, heads = q.shape
    width = x.shape[1]
    shape = jax.ShapeDtypeStruct
    outs = [
        shape((tok, 2 * heads), BF16),
        shape((tok, 128), F32),
        shape((tok, width), F32),
        shape((tok, 2 * n_col * width), BF16),
    ]
    scratch = [
        pltpu.VMEM((tok, 2 * heads), BF16),
        pltpu.VMEM((tok, width), F32),
        pltpu.VMEM((N_CHUNK, tok // N_CHUNK, 2 * n_col * width), BF16),
        pltpu.VMEM(wo.shape, BF16),
        *Scatter.scratch(n_col, tok // N_CHUNK, width),
        *gather_sems(n_col),
        pltpu.SemaphoreType.DMA((N_CHUNK,)),
        pltpu.SemaphoreType.DMA((N_CHUNK,)),
        pltpu.SemaphoreType.DMA((4,)),
        pltpu.SemaphoreType.DMA((3, N_CHUNK)),
    ]
    return kernel_call(
        functools.partial(attend_kernel, n_col), "attend", 2, outs, [True, False, True, True],
        [vmem()] * 6 + [anywhere()] * 4, scratch, 8 * tok * tok * heads,
    )(q, k, v, seg_row, seg_col, x, wo, dy, dy_end, dy_mid)


def ffn_kernel(
    n_col, n_sum,
    middle, gain, dy_full, wg, wu, wd, wg_other, wu_other, wd_other,
    h2_out, units_out, gate_out, up_out, middle_grad_out, branch_out, gain_sum, sum_out,
    units, grad_gate, grad_up, grad_middle, grad_branch,
    full, gate_own, up_own, down_own, gate_far, up_far, scale_wide, grad_two,
    part, stage, inbox, rs_send, rs_recv, held, sent, arrived, st_send, st_recv,
    ag_send, ag_recv, x_send, x_recv, local, flushed, *refs,
):
    r, c = lax.axis_index("row"), lax.axis_index("col")
    tok, width = middle.shape
    half = n_col * width
    n_unit = down_own.shape[0]
    rows = tok // N_CHUNK
    me = r * n_col + c
    sums = refs[0:1]

    def chunk_rows(chunk):
        return span(chunk * rows, rows)

    gather = Gather(full, ag_send, ag_recv, r, c, n_col, width)
    scatter = Scatter(part, stage, inbox, rs_send, rs_recv, c, n_col)
    totals = Totals(held, sent, arrived, st_send, st_recv, r, c)
    mine, far = span(r * n_unit, n_unit), span((1 - r) * n_unit, n_unit)
    near_rows, far_rows = span(r * half, half), span((1 - r) * half, half)
    flush = Flush(
        (
            ((full, near_rows), h2_out), (grad_gate, gate_out), (grad_up, up_out), (units, units_out),
            (grad_middle, middle_grad_out), (grad_branch, branch_out),
        ),
        flushed, rows,
    )
    loads = [
        pltpu.make_async_copy(src, dst, local.at[n])
        for n, (src, dst) in enumerate(
            (
                (wg.at[:, mine], gate_own.at[near_rows, :]),
                (wg_other, gate_own.at[far_rows, :]),
                (wu.at[:, mine], up_own.at[near_rows, :]),
                (wu_other, up_own.at[far_rows, :]),
                (wd.at[mine, :], down_own.at[:, near_rows]),
                (wd_other, down_own.at[:, far_rows]),
                (wg.at[:, far], gate_far),
                (wu.at[:, far], up_far),
            )
        )
    ]
    block = span(me * width, width)
    for chunk in range(N_CHUNK):
        values = middle[chunk * rows : (chunk + 1) * rows, :]
        full[chunk, 0:rows, block] = (values * gain[...]).astype(BF16)
        put_notes(full, chunk, block, (as_row(jnp.sum(values * values, axis=1, keepdims=True)),))
    panels = []
    if n_sum:
        tile = tile_of(units, dy_full, sums[0].shape[0], r * half, half // 2)
        panels.append(Reduce(tile, sums, *refs[1:]))
    greet(group_peers(r, c, n_col) + (square_peers() if n_sum else []))
    gather.start(0)
    gather.start(1)
    for copy in loads:
        copy.start()

    def exchange(n, chunk):
        piece = (grad_gate, grad_up, units)[n].at[chunk_rows(chunk), mine]
        return remote(piece, piece, x_send.at[n, chunk], x_recv.at[n, chunk], {"row": 1 - r})

    def norm(chunk):
        square = jnp.zeros((1, rows), F32)
        for at in range(2 * n_col):
            square = square + get_note(full, chunk, pl.ds(at * width, width), 0)
        scale = lax.rsqrt(as_column(square) * (1.0 / (2 * half)) + norm_eps)
        scale_wide[chunk_rows(chunk), :] = jnp.broadcast_to(scale, (rows, scale_wide.shape[1]))

    tile = n_unit // 2

    def units_part(chunk, step):
        at = chunk_rows(chunk)
        scale = scale_wide[at, 0:1]
        cols = span(step * tile, tile)
        gate = dot_nn(full[chunk, 0:rows, :], gate_own[:, cols]) * scale
        up = dot_nn(full[chunk, 0:rows, :], up_own[:, cols]) * scale
        grad = dot_nt(dy_full[at, :], down_own[cols, :])
        sig = jax.nn.sigmoid(gate)
        act = gate * sig
        put = span(r * n_unit + step * tile, tile)
        units[at, put] = (act * up).astype(BF16)
        grad = grad * scale
        grad_gate[at, put] = (grad * up * sig * (1.0 + gate * (1.0 - sig))).astype(BF16)
        grad_up[at, put] = (grad * act).astype(BF16)

    def back(chunk):
        at = chunk_rows(chunk)
        part[chunk] = dot_nt(grad_gate[at, mine], gate_own[near_rows, :]) + dot_nt(
            grad_up[at, mine], up_own[near_rows, :]
        )
        for n in range(3):
            exchange(n, chunk).wait_recv()
        flush.start(chunk, (0, 1, 2, 3))
        part[chunk] += dot_nt(grad_gate[at, far], gate_far[...]) + dot_nt(grad_up[at, far], up_far[...])
        scatter.open(chunk)

    def settle(chunk):
        at = chunk_rows(chunk)
        scatter.total(chunk, grad_two, at)
        product = grad_two[at, :] * middle[at, :]
        totals.note(chunk, jnp.sum(product * gain[...], axis=1, keepdims=True))
        gain_sum[...] += jnp.sum(product.reshape(rows // 8, 8, width), axis=0)

    def conclude(chunk):
        at = chunk_rows(chunk)
        mean = totals.column(chunk) * (1.0 / (2 * half))
        scale = scale_wide[at, 0:1]
        grad = (
            dy_full[at, span(me * width, width)].astype(F32)
            + grad_two[at, :] * gain[...]
            - middle[at, :] * (scale * scale * mean)
        )
        grad_middle[at, :] = grad
        grad_branch[at, :] = grad.astype(BF16)
        flush.start(chunk, (4, 5))

    gain_sum[...] = jnp.zeros_like(gain_sum)
    gather.tick(0)
    gather.start(2)
    gather.tick(1)
    gather.start(3)
    gather.tick(2)
    for copy in loads:
        copy.wait()

    def step(now, carry):
        @pl.when(now < N_CHUNK)
        def _():
            gather.wait_other(now)
            norm(now)

            def part_step(n, carry):
                units_part(now, n)
                return carry

            lax.fori_loop(0, 2, part_step, 0)
            for n in range(3):
                exchange(n, now).start()

        pl.when((now >= 1) & (now <= N_CHUNK))(lambda: scatter.near(now - 1))
        pl.when((now >= 2) & (now <= N_CHUNK + 1))(lambda: scatter.far(now - 2))
        pl.when(now < N_CHUNK)(lambda: back(now))
        gather.tick(now + 3)
        pl.when((now >= 3) & (now <= N_CHUNK + 2))(lambda: settle(now - 3))
        for panel in panels:
            pl.when(now == N_CHUNK - 1)(panel.first)
            pl.when(now == N_CHUNK + 1)(panel.second)
            pl.when(now == N_CHUNK + 1)(panel.merge)
        return carry

    lax.fori_loop(0, N_CHUNK + 3, step, 0)
    totals.exchange()

    def close_up(chunk, carry):
        conclude(chunk)
        return carry

    lax.fori_loop(0, N_CHUNK, close_up, 0)
    gather.finish()
    scatter.finish()
    totals.finish()
    stores = []
    for panel in panels:
        panel.last()
        stores += fetches([(sums[0], sum_out)], local.at[pl.ds(8, 1)])
        panel.finish()

    def close(chunk, carry):
        for n in range(3):
            exchange(n, chunk).wait_send()
        return carry

    lax.fori_loop(0, N_CHUNK, close, 0)
    for copy in stores:
        copy.wait()
    flush.finish()


def ffn(n_col, n_dp, middle, gain, dy_full, wg, wu, wd, wg_other, wu_other, wd_other):
    tok, width = middle.shape
    half, n_unit = n_col * width, wg.shape[1] // 2
    shape = jax.ShapeDtypeStruct
    outs = [
        shape((tok, half), BF16),
        shape((tok, 2 * n_unit), BF16), shape((tok, 2 * n_unit), BF16), shape((tok, 2 * n_unit), BF16),
        shape((tok, width), F32), shape((tok, width), BF16), shape((8, width), F32),
    ]
    n_sum = int(n_dp == 4)
    size = (wd.shape[0] // 4, half // 2) if n_sum else (8, 128)
    outs.append(shape(size, F32))
    rows = tok // N_CHUNK
    scratch = [
        *[pltpu.VMEM((tok, 2 * n_unit), BF16)] * 3,
        pltpu.VMEM((tok, width), F32),
        pltpu.VMEM((tok, width), BF16),
        pltpu.VMEM((N_CHUNK, rows + N_NOTE, 2 * half), BF16),
        pltpu.VMEM((2 * half, n_unit), BF16),
        pltpu.VMEM((2 * half, n_unit), BF16),
        pltpu.VMEM((n_unit, 2 * half), BF16),
        pltpu.VMEM((half, n_unit), BF16),
        pltpu.VMEM((half, n_unit), BF16),
        pltpu.VMEM((tok, 128), F32),
        pltpu.VMEM((tok, width), F32),
        *Scatter.scratch(n_col, rows, width),
        *Totals.scratch(rows),
        *gather_sems(n_col),
        pltpu.SemaphoreType.DMA((3, N_CHUNK)),
        pltpu.SemaphoreType.DMA((3, N_CHUNK)),
        pltpu.SemaphoreType.DMA((9,)),
        pltpu.SemaphoreType.DMA((6, N_CHUNK)),
    ]
    if n_sum:
        scratch += [pltpu.VMEM(size, F32), *Reduce.scratch(size[0], size[1] // 2)]
    return kernel_call(
        functools.partial(ffn_kernel, n_col, n_sum), "ffn", 3, outs, [True] * 6 + [False, True],
        [vmem()] * 3 + [anywhere()] * 6, scratch, 20 * tok * half * n_unit,
    )(middle, gain, dy_full, wg, wu, wd, wg_other, wu_other, wd_other)


class Reduce:
    def __init__(self, tile, outs, stage_one, inbox_one, stage_two, inbox_two, send, recv):
        d = lax.axis_index("dp")
        self.x, self.y = d % 2, d // 2
        self.tile, self.outs = tile, outs
        self.stage_one, self.inbox_one = stage_one, inbox_one
        self.stage_two, self.inbox_two = stage_two, inbox_two
        self.send, self.recv = send, recv
        self.along_x = {"dp": self.y * 2 + 1 - self.x}
        self.along_y = {"dp": (1 - self.y) * 2 + self.x}

    def along(self, side):
        return {"dp": jnp.where(side == 0, self.along_x["dp"], self.along_y["dp"])}

    def copy_one(self, side, n):
        return remote(
            self.stage_one.at[side, n], self.inbox_one.at[side, n],
            self.send.at[side, n], self.recv.at[side, n], self.along(side),
        )

    def copy_two(self, side):
        return remote(
            self.stage_two.at[side], self.inbox_two.at[side],
            self.send.at[side, 2], self.recv.at[side, 2], self.along(1 - side),
        )

    def first(self):
        def one(step, carry):
            side = step % 2
            near = jnp.where(side == 0, self.y, self.x)
            n = jnp.where(step < 2, 1 - near, near)
            owner = jnp.where(side == 0, n * 2 + 1 - self.x, (1 - self.y) * 2 + n)
            self.stage_one[side, n] = self.tile(owner, side).astype(BF16)
            self.copy_one(side, n).start()
            return carry

        lax.fori_loop(0, 4, one, 0)

    def second(self):
        def one(side, carry):
            n = jnp.where(side == 0, 1 - self.y, 1 - self.x)
            owner = jnp.where(side == 0, n * 2 + self.x, self.y * 2 + n)
            value = self.tile(owner, side)
            self.copy_one(side, n).wait_recv()
            self.stage_two[side] = (value + self.inbox_one[side, n].astype(F32)).astype(BF16)
            self.copy_two(side).start()
            return carry

        lax.fori_loop(0, 2, one, 0)

    def put(self, side, value, add):
        each = value.shape[1] // len(self.outs)
        cols = span(side * each, each)
        for n, out in enumerate(self.outs):
            term = value[:, n * each : (n + 1) * each]
            out[:, cols] = out[:, cols] + term if add else term

    def merge(self):
        def one(side, carry):
            n = jnp.where(side == 0, self.y, self.x)
            value = self.tile(self.y * 2 + self.x, side)
            self.copy_one(side, n).wait_recv()
            self.put(side, value + self.inbox_one[side, n].astype(F32), False)
            return carry

        lax.fori_loop(0, 2, one, 0)

    def last(self):
        def one(side, carry):
            self.copy_two(side).wait_recv()
            self.put(side, self.inbox_two[side].astype(F32), True)
            return carry

        lax.fori_loop(0, 2, one, 0)

    def finish(self):
        def one(side, carry):
            for n in range(2):
                self.copy_one(side, n).wait_send()
            self.copy_two(side).wait_send()
            return carry

        lax.fori_loop(0, 2, one, 0)

    @staticmethod
    def scratch(rows, cols):
        return [
            pltpu.VMEM((2, 2, rows, cols), BF16),
            pltpu.VMEM((2, 2, rows, cols), BF16),
            pltpu.VMEM((2, rows, cols), BF16),
            pltpu.VMEM((2, rows, cols), BF16),
            pltpu.SemaphoreType.DMA((2, 3)),
            pltpu.SemaphoreType.DMA((2, 3)),
        ]


def square_peers():
    d = lax.axis_index("dp")
    x, y = d % 2, d // 2
    always = d >= 0
    return [(always, {"dp": y * 2 + 1 - x}), (always, {"dp": (1 - y) * 2 + x})]


def tile_of(left, right, n_row, base=0, width=None):
    cols = (right.shape[1] if width is None else width) // 2

    def tile(owner, side):
        return dot_tn(left[:, span(owner * n_row, n_row)], right[:, span(base + side * cols, cols)])

    return tile


def branch_kernel(
    n_col, n_sum,
    branch, units_in, wd, middle_in, dy_full, h2_in, gate_in, wo, wo_other, heads_in,
    *refs,
):
    (output_out, heads_out, half_out), refs = refs[:3], refs[3:]
    sums_out, refs = refs[:n_sum], refs[n_sum:]
    (
        units, middle, h2, grad_gate, heads_all, branch_half, output, grad_heads,
        full, down, dy_half, w_out, part, stage, inbox, rs_send, rs_recv, ag_send, ag_recv, local, flushed,
    ), refs = refs[:21], refs[21:]
    sums, refs = refs[:n_sum], refs[n_sum:]
    r, c = lax.axis_index("row"), lax.axis_index("col")
    tok, width = middle.shape
    half = n_col * width
    heads = grad_heads.shape[1]
    rows = tok // N_CHUNK
    me = r * n_col + c
    mine, other = span(r * half, half), span((1 - r) * half, half)
    own, dy_load, units_load, down_load, *loads = fetches(
        [
            (branch.reshape(N_CHUNK, rows, width), full.at[:, :, span(me * width, width)]),
            (dy_full.at[:, mine], dy_half),
            (units_in, units),
            (wd, down),
            (h2_in, h2),
            (gate_in, grad_gate),
            (wo.at[span(r * heads, heads), :], w_out.at[:, mine]),
            (wo_other, w_out.at[:, other]),
            (middle_in, middle),
            (heads_in, heads_all),
        ],
        local,
    )
    greet(line_peers(r, c, n_col) + (square_peers() if n_sum else []))
    gather = Gather(full, ag_send, ag_recv, r, c, n_col, width)
    scatter = Scatter(part, stage, inbox, rs_send, rs_recv, c, n_col)
    flush = Flush(((output, output_out), (grad_heads, heads_out), (branch_half, half_out)), flushed, rows)
    own.wait()

    def begin_gather(chunk, carry):
        gather.start(chunk)
        return carry

    lax.fori_loop(0, N_CHUNK, begin_gather, 0)
    panels = []
    if n_sum:
        terms = ((units, dy_half, half // 2, half // 2), (h2, grad_gate, 0, None), (heads_all, branch_half, 0, None))
        for n, (left, right, base, cols) in enumerate(terms):
            tile = tile_of(left, right, sums[n].shape[0], base, cols)
            panels.append(Reduce(tile, (sums[n],), *refs[6 * n : 6 * n + 6]))
    dy_load.wait()
    units_load.wait()
    for panel in panels[:1]:
        panel.first()
    down_load.wait()

    def begin(chunk, carry):
        part[chunk] = dot_nn(units[span(chunk * rows, rows), :], down[...])
        scatter.open(chunk)
        gather.relay(1, chunk)
        return carry

    lax.fori_loop(0, N_CHUNK, begin, 0)
    for copy in loads:
        copy.wait()
    for panel in panels[1:2]:
        panel.first()

    def carry_on(chunk, carry):
        gather.relay(2, chunk)
        scatter.near(chunk)
        return carry

    lax.fori_loop(0, N_CHUNK, carry_on, 0)
    for panel in panels[:1]:
        panel.second()

    def arrive(chunk, carry):
        gather.relay(3, chunk)
        scatter.far(chunk)
        return carry

    lax.fori_loop(0, N_CHUNK, arrive, 0)

    def copy_half(chunk, carry):
        gather.wait_other(chunk)
        branch_half[span(chunk * rows, rows), :] = full[chunk, :, mine]
        return carry

    lax.fori_loop(0, N_CHUNK, copy_half, 0)
    for panel in panels[2:]:
        panel.first()
    for panel in panels[:1]:
        panel.merge()
    for panel in panels[1:2]:
        panel.second()

    def settle(chunk, carry):
        at = span(chunk * rows, rows)
        grad_heads[at, :] = dot_nt(full[chunk], w_out[...]).astype(BF16)
        scatter.total(chunk, output, at)
        output[at, :] += middle[at, :]
        flush.start(chunk)
        return carry

    lax.fori_loop(0, N_CHUNK, settle, 0)
    for panel in panels[1:2]:
        panel.merge()
    for panel in panels[2:]:
        panel.second()
        panel.merge()
    stores = []
    for n, panel in enumerate(panels):
        panel.last()
        stores += fetches([(sums[n], sums_out[n])], local.at[pl.ds(10 + n, 1)])
    gather.finish()
    scatter.finish()
    for panel in panels:
        panel.finish()
    for copy in stores:
        copy.wait()
    flush.finish()


def branch_back(n_col, n_dp, branch, units, wd, middle, dy_full, h2, grad_gate, wo, wo_other, heads_all):
    tok, width = middle.shape
    half, heads = n_col * width, wo_other.shape[0]
    rows = tok // N_CHUNK
    shape = jax.ShapeDtypeStruct
    outs = [shape((tok, width), F32), shape((tok, heads), BF16), shape((tok, half), BF16)]
    scratch = [
        pltpu.VMEM(units.shape, BF16),
        pltpu.VMEM(middle.shape, F32),
        pltpu.VMEM(h2.shape, BF16),
        pltpu.VMEM(grad_gate.shape, BF16),
        pltpu.VMEM(heads_all.shape, BF16),
        pltpu.VMEM((tok, half), BF16),
        pltpu.VMEM((tok, width), F32),
        pltpu.VMEM((tok, heads), BF16),
        pltpu.VMEM((N_CHUNK, rows, 2 * half), BF16),
        pltpu.VMEM(wd.shape, BF16),
        pltpu.VMEM((tok, half), BF16),
        pltpu.VMEM((heads, 2 * half), BF16),
        *Scatter.scratch(n_col, rows, width),
        *gather_sems(n_col),
        pltpu.SemaphoreType.DMA((13,)),
        pltpu.SemaphoreType.DMA((3, N_CHUNK)),
    ]
    n_sum = 0
    if n_dp == 4:
        n_sum = 3
        sizes = [(wd.shape[0] // 4, half // 2), (half // 4, grad_gate.shape[1]), (heads // 2, half)]
        outs += [shape(size, F32) for size in sizes]
        scratch += [pltpu.VMEM(size, F32) for size in sizes]
        for size in sizes:
            scratch += Reduce.scratch(size[0], size[1] // 2)
    return kernel_call(
        functools.partial(branch_kernel, n_col, n_sum), "branch", 4, outs, [True] * len(outs),
        [anywhere()] * 10, scratch, 12 * tok * half * half,
    )(branch, units, wd, middle, dy_full, h2, grad_gate, wo, wo_other, heads_all)


def attend_back_kernel(
    n_col, n_dp, n_sum,
    q_in, k_in, v_in, heads_grad_in, seg_row, seg_col_in, inv_in, cos_in, sin_in, x_in, r1_in, gain, middle_in,
    gain_two, h1_in, wq, wk, wv, h2_in, up_in,
    *refs,
):
    (tokens_out, gain_sums, triple_out), refs = refs[:3], refs[3:]
    sums_out, refs = refs[:n_sum], refs[n_sum:]
    (
        q, k, v, grad_heads, seg_col, inv_sum, cos_table, sin_table, x, r1, grad_middle,
        h1, h2, grad_up, grad_tokens, triple,
        weights, grad_k, grad_v, grad_q, grad_one, gain_mine, gain_box, part, stage, inbox, rs_send, rs_recv,
        held, sent, arrived, st_send, st_recv, x_send, x_recv, g_send, g_recv, local, flushed,
    ), refs = refs[:39], refs[39:]
    sums, refs = refs[:n_sum], refs[n_sum:]
    r, c, d = lax.axis_index("row"), lax.axis_index("col"), lax.axis_index("dp")
    tok, width = x.shape
    half = n_col * width
    heads = q.shape[1]
    rows = tok // N_CHUNK
    me = r * n_col + c
    early = [(h2_in, h2), (up_in, grad_up)]
    first = [
        (q_in, q), (k_in, k), (v_in, v), (heads_grad_in, grad_heads), (seg_col_in, seg_col), (inv_in, inv_sum),
        (cos_in, cos_table), (sin_in, sin_table),
    ]
    later = [(h1_in, h1), (x_in, x), (r1_in, r1)]
    later.append((middle_in, grad_middle))
    for n, w in enumerate((wq, wk, wv)):
        for side in range(2):
            later.append(
                (w.at[:, pl.ds(side * heads, heads)], weights.at[:, pl.ds((side * 3 + n) * heads, heads)])
            )
    copies = fetches(early + first + later, local)
    early, first, later = copies[:2], copies[2:10], copies[10:]
    dp_peers = [(d != at, {"dp": jnp.int32(at)}) for at in range(n_dp)]
    greet(group_peers(r, c, n_col) + dp_peers)
    scatter = Scatter(part, stage, inbox, rs_send, rs_recv, c, n_col)
    totals = Totals(held, sent, arrived, st_send, st_recv, r, c)
    flush = Flush(((grad_tokens, tokens_out),), flushed, rows)
    panels = []
    if n_sum:
        for n, (left, right) in enumerate(((h2, grad_up), (h1, triple))):
            tile = tile_of(left, right, sums[n].shape[0])
            panels.append(Reduce(tile, sums[1:] if n else sums[:1], *refs[6 * n : 6 * n + 6]))

    def exchange(chunk):
        piece = triple.at[span(chunk * rows, rows), span(r * 3 * heads, 3 * heads)]
        return remote(piece, piece, x_send.at[chunk], x_recv.at[chunk], {"row": 1 - r})

    def attend(chunk):
        at = pl.ds(chunk * rows, rows)
        keys = (chunk + 1) * rows
        allowed = allowed_pairs(seg_col[at, :], seg_row[:, 0:keys], chunk, rows, keys)
        grad_q[...] = jnp.zeros_like(grad_q)

        def head_step(head, carry):
            query = of_head(q[at, :], head)
            grad = of_head(grad_heads[at, :], head)
            scores = dot_nt(query, k[0:keys, :]) * HD**-0.5
            inv = jnp.sum(jnp.where(lanes((rows, 128)) == head, inv_sum[at, :], 0.0), axis=1, keepdims=True)
            probs = jnp.exp(jnp.where(allowed, scores, masked_score)) * inv
            grad_probs = dot_nt(grad, v[0:keys, :])
            weighted = jnp.sum(probs * grad_probs, axis=1, keepdims=True)
            grad_scores = (probs * (grad_probs - weighted) * HD**-0.5).astype(BF16)
            grad_q[...] += dot_nn(grad_scores, of_head(k[0:keys, :], head))
            grad_k[0:keys, :] += dot_tn(grad_scores, query)
            grad_v[0:keys, :] += dot_tn(probs.astype(BF16), grad)
            return carry

        lax.fori_loop(0, heads // HD, head_step, 0)
        cos_rows = widen(cos_table[at, :], heads)
        sin_rows = widen(sin_table[at, :], heads)
        for n, value in enumerate((grad_q[...], grad_k[at, :])):
            value = value * cos_rows - swap_halves(value) * sin_rows
            triple[at, span((r * 3 + n) * heads, heads)] = value.astype(BF16)
        triple[at, span((r * 3 + 2) * heads, heads)] = grad_v[at, :].astype(BF16)
        exchange(chunk).start()

    def contract(chunk):
        at = span(chunk * rows, rows)
        exchange(chunk).wait_recv()
        part[chunk] = dot_nt(triple[at, :], weights[...])
        scatter.open(chunk)

    def settle(chunk):
        at = span(chunk * rows, rows)
        scatter.total(chunk, grad_one, at)
        product = grad_one[at, :] * (x[at, :].astype(F32) * r1[at, 0:1])
        totals.note(chunk, jnp.sum(product * gain[...], axis=1, keepdims=True))
        gain_mine[0] += jnp.sum(product.reshape(rows // 8, 8, width), axis=0)

    def conclude(chunk):
        at = span(chunk * rows, rows)
        mean = totals.column(chunk) * (1.0 / (2 * half))
        scale = r1[at, 0:1]
        grad_tokens[at, :] = grad_middle[at, :] + scale * (
            grad_one[at, :] * gain[...] - x[at, :].astype(F32) * (scale * mean)
        )
        flush.start(chunk)

    def gain_copy(at):
        return remote(gain_box.at[d], gain_box.at[d], g_send.at[at], g_recv.at[d], {"dp": at})

    def gain_arrival(at):
        return remote(gain_box.at[at], gain_box.at[at], g_send.at[at], g_recv.at[at], {"dp": at})

    def others(act):
        def one(at, carry):
            pl.when(at != d)(lambda: act(at))
            return carry

        lax.fori_loop(0, n_dp, one, 0)

    def panel_do(n, what):
        if n_sum:
            getattr(panels[n], what)()

    gain_mine[0] = jnp.zeros(gain_mine.shape[1:], F32)
    gain_mine[1] = gain_two[...]
    grad_k[...] = jnp.zeros_like(grad_k)
    grad_v[...] = jnp.zeros_like(grad_v)
    last = N_CHUNK - 1
    for copy in early:
        copy.wait()
    panel_do(0, "first")
    for copy in first:
        copy.wait()
    attend(last)
    for copy in later:
        copy.wait()
    attend(last - 1)
    contract(last)
    panel_do(0, "second")
    attend(last - 2)
    contract(last - 1)
    scatter.near(last)
    attend(last - 3)
    contract(last - 2)
    scatter.near(last - 1)
    scatter.far(last)
    contract(last - 3)
    panel_do(1, "first")
    scatter.near(last - 2)
    scatter.far(last - 1)
    panel_do(0, "merge")
    settle(last)
    scatter.near(last - 3)
    scatter.far(last - 2)
    panel_do(1, "second")

    def settle_step(now, carry):
        pl.when(now == 1)(lambda: scatter.far(0))
        settle(last - now)
        return carry

    lax.fori_loop(1, N_CHUNK, settle_step, 0)
    gain_box[d] = gain_mine[...]
    others(lambda at: gain_copy(at).start())
    panel_do(1, "merge")
    totals.exchange()

    def close_up(step, carry):
        conclude(last - step)
        return carry

    lax.fori_loop(0, N_CHUNK, close_up, 0)
    others(lambda at: gain_arrival(at).wait_recv())
    gain_total = gain_box[0]
    for at in range(1, n_dp):
        gain_total = gain_total + gain_box[at]
    gain_sums[...] = gain_total
    stores = []
    where = len(copies)
    for n, panel in enumerate(panels):
        panel.last()
        for m in range(1, n_sum) if n else range(1):
            stores += fetches([(sums[m], sums_out[m])], local.at[pl.ds(where + m, 1)])
    if not n_sum:
        stores += fetches([(triple, triple_out)], local.at[pl.ds(where, 1)])
    scatter.finish()
    totals.finish()
    for chunk in range(N_CHUNK):
        exchange(chunk).wait_send()
    others(lambda at: gain_copy(at).wait_send())
    for panel in panels:
        panel.finish()
    for copy in stores:
        copy.wait()
    flush.finish()


def attend_back(
    n_col, n_dp,
    q, k, v, grad_heads, seg_row, seg_col, inv_sum, cos_table, sin_table, x, r1, gain, grad_middle,
    gain_two, h1, wq, wk, wv, h2, grad_up,
):
    tok, width = x.shape
    half, heads = n_col * width, q.shape[1]
    rows = tok // N_CHUNK
    shape = jax.ShapeDtypeStruct
    triple = (tok, 6 * heads) if n_dp != 4 else (8, 128)
    outs = [shape((tok, width), F32), shape((2, 8, width), F32), shape(triple, BF16)]
    held = [q, k, v, grad_heads, seg_col, inv_sum, cos_table, sin_table, x, r1, grad_middle]
    held += [h1, h2, grad_up]
    scratch = [
        *[pltpu.VMEM(array.shape, array.dtype) for array in held],
        pltpu.VMEM((tok, width), F32),
        pltpu.VMEM((tok, 6 * heads), BF16),
        pltpu.VMEM((half, 6 * heads), BF16),
        pltpu.VMEM((tok, heads), F32),
        pltpu.VMEM((tok, heads), F32),
        pltpu.VMEM((rows, heads), F32),
        pltpu.VMEM((tok, width), F32),
        pltpu.VMEM((2, 8, width), F32),
        pltpu.VMEM((n_dp, 2, 8, width), F32),
        *Scatter.scratch(n_col, rows, width),
        *Totals.scratch(rows),
        pltpu.SemaphoreType.DMA((N_CHUNK,)),
        pltpu.SemaphoreType.DMA((N_CHUNK,)),
        pltpu.SemaphoreType.DMA((n_dp,)),
        pltpu.SemaphoreType.DMA((n_dp,)),
        pltpu.SemaphoreType.DMA((27,)),
        pltpu.SemaphoreType.DMA((1, N_CHUNK)),
    ]
    n_sum = 0
    if n_dp == 4:
        sizes = [(half // 4, grad_up.shape[1])] + [(half // 4, 2 * heads)] * 3
        n_sum = len(sizes)
        outs += [shape(size, F32) for size in sizes]
        scratch += [pltpu.VMEM(size, F32) for size in sizes]
        for size in sizes[:1] + [(half // 4, 6 * heads)]:
            scratch += Reduce.scratch(size[0], size[1] // 2)
    return kernel_call(
        functools.partial(attend_back_kernel, n_col, n_dp, n_sum), "attend_back", 5, outs,
        [True, False, True] + [True] * n_sum,
        [anywhere()] * 4 + [vmem()] + [anywhere()] * 6 + [vmem(), anywhere(), vmem()] + [anywhere()] * 6,
        scratch, 16 * tok * tok * heads,
    )(
        q, k, v, grad_heads, seg_row, seg_col, inv_sum, cos_table, sin_table, x, r1, gain, grad_middle,
        gain_two, h1, wq, wk, wv, h2, grad_up,
    )


def finish_kernel(groups, share, gain_sums, *refs):
    n_copy = sum(groups)
    sources, refs = refs[:n_copy], refs[n_copy:]
    gain_out, refs = refs[:2], refs[2:]
    results, refs = refs[: len(groups)], refs[len(groups) :]
    held, (get, put) = refs[:n_copy], refs[n_copy:]
    targets = []
    for result, parts in zip(results, groups):
        cols = result.shape[1] // parts
        targets += [result.at[:, pl.ds(part * cols, cols)] for part in range(parts)]
    pieces = 2
    inward, outward = [], []
    for n, (source, keep, target) in enumerate(zip(sources, held, targets)):
        rows = keep.shape[0] // pieces
        for piece in range(pieces):
            at = pl.ds(piece * rows, rows)
            inward.append(pltpu.make_async_copy(source.at[at, :], keep.at[at, :], get.at[n, piece]))
            outward.append(pltpu.make_async_copy(keep.at[at, :], target.at[at, :], put.at[n, piece]))
    for copy in inward:
        copy.start()
    d = lax.axis_index("dp")
    width = gain_sums.shape[-1]
    shift = lax.rem(width - d * share, width)
    for n in range(2):
        moved = pltpu.roll(gain_sums[n], shift, 1)
        gain_out[n][...] = jnp.sum(moved, axis=0, keepdims=True)[:, 0:share]
    for one, two in zip(inward, outward):
        one.wait()
        two.start()
    for copy in outward:
        copy.wait()


def finish(share, gain_sums, arrays):
    shape = jax.ShapeDtypeStruct
    groups = tuple(len(parts) for parts in arrays)
    flat = [part for parts in arrays for part in parts]
    outs = [shape((1, share), F32)] * 2
    outs += [shape((p[0].shape[0], sum(x.shape[1] for x in p)), p[0].dtype) for p in arrays]
    n_copy = len(flat)
    return pl.pallas_call(
        functools.partial(finish_kernel, groups, share),
        out_shape=outs,
        in_specs=[vmem()] + [anywhere()] * n_copy,
        out_specs=[vmem()] * 2 + [anywhere()] * len(arrays),
        scratch_shapes=[pltpu.VMEM(x.shape, x.dtype) for x in flat]
        + [pltpu.SemaphoreType.DMA((n_copy, 2)), pltpu.SemaphoreType.DMA((n_copy, 2))],
        compiler_params=pltpu.CompilerParams(vmem_limit_bytes=VMEM_LIMIT),
        name="finish",
    )(gain_sums, *flat)


def body(
    n_dp,
    n_col,
    tokens,
    gain_attn,
    gain_ffn,
    w_query,
    w_key,
    w_value,
    w_out,
    w_gate,
    w_up,
    w_down,
    grad_output,
    segments,
    positions,
):
    tok, width = tokens.shape
    heads = w_query.shape[1] // 2
    gain_one, gain_two = gain_attn.reshape(1, width), gain_ffn.reshape(1, width)
    (
        q, k, v, h1, r1, cos_table, sin_table, seg_col, dy_end, dy_mid, wo_other, wg_other, wu_other, wd_other,
    ) = project(
        n_col, tokens, gain_one, positions, segments, grad_output,
        w_query, w_key, w_value, w_out, w_gate, w_up, w_down,
    )
    heads_all, inv_sum, middle, dy_full = attend(
        n_col, q, k, v, segments, seg_col, tokens, w_out, grad_output, dy_end, dy_mid
    )
    h2, units, grad_gate, grad_up, grad_middle, branch, gain_sum, down_one = ffn(
        n_col, n_dp, middle, gain_two, dy_full, w_gate, w_up, w_down, wg_other, wu_other, wd_other
    )
    output, grad_heads, branch_half, *sums_one = branch_back(
        n_col, n_dp, branch, units, w_down, middle, dy_full, h2, grad_gate, w_out, wo_other, heads_all
    )
    grad_tokens, gain_sums, triple, *sums_two = attend_back(
        n_col, n_dp, q, k, v, grad_heads, segments, seg_col, inv_sum, cos_table, sin_table, tokens, r1,
        gain_one, grad_middle, gain_sum, h1, w_query, w_key, w_value, h2, grad_up,
    )
    if n_dp == 4:
        down_two, grad_wg, grad_wo = sums_one
        grad_wd = (down_one, down_two)
        grad_wu, *grad_qkv = sums_two
    else:

        def summed(left, right):
            grad = jnp.einsum("ta,tb->ab", left, right, preferred_element_type=F32).astype(BF16)
            return lax.psum_scatter(grad, "dp", scatter_dimension=0, tiled=True).astype(F32)

        row = lax.axis_index("row")
        dy_half = lax.dynamic_slice(dy_full, (0, row * n_col * width), (tok, n_col * width))
        grad_wd, grad_wg = (summed(units, dy_half),), summed(h2, grad_gate)
        grad_wu, grad_wo = summed(h2, grad_up), summed(heads_all, branch_half)
        parts = summed(h1, triple).reshape(-1, 2, 3, heads)
        grad_qkv = [parts[:, :, n].reshape(-1, 2 * heads) for n in range(3)]
    gain_a, gain_b, *results = finish(
        width // n_dp, gain_sums,
        [(m,) for m in (output, grad_tokens, *grad_qkv, grad_wo, grad_wg, grad_wu)] + [grad_wd],
    )
    blocks = [m.reshape((1, 1) + m.shape) for m in results[2:]]
    return (*results[:2], gain_a.reshape(1, 1, -1), gain_b.reshape(1, 1, -1), *blocks)


def solution(mesh):
    return jax.shard_map(
        functools.partial(body, mesh.shape["dp"], mesh.shape["col"]),
        mesh=mesh,
        in_specs=(
            P("dp", ("row", "col")),
            P(("row", "col")),
            P(("row", "col")),
            P("row", "col"),
            P("row", "col"),
            P("row", "col"),
            P("col", "row"),
            P("row", "col"),
            P("row", "col"),
            P("col", "row"),
            P("dp", ("row", "col")),
            P("dp", None),
            P("dp", None),
        ),
        out_specs=(
            P("dp", ("row", "col")),
            P("dp", ("row", "col")),
            P(("row", "col"), "dp", None),
            P(("row", "col"), "dp", None),
            P("row", "dp", None, "col"),
            P("row", "dp", None, "col"),
            P("row", "dp", None, "col"),
            P("col", "dp", None, "row"),
            P("row", "dp", None, "col"),
            P("row", "dp", None, "col"),
            P("col", "dp", None, "row"),
        ),
        check_vma=False,
    )
```

```python
import functools

import jax
import jax.numpy as jnp
from jax import lax
from jax.experimental import pallas as pl
from jax.experimental.pallas import tpu as pltpu
from jax.sharding import PartitionSpec as P

MESH = pl.DeviceIdType.MESH
F32 = jnp.float32
BF16 = jnp.bfloat16
HD = 64
N_CHUNK = 4
norm_eps = 1e-05
rope_base = 130000.0
masked_score = -1e30
VMEM_LIMIT = 64 * 1024 * 1024 - 65536


def dot_nn(left, right):
    return lax.dot_general(left, right, (((1,), (0,)), ((), ())), preferred_element_type=F32)


def dot_nt(left, right):
    return lax.dot_general(left, right, (((1,), (1,)), ((), ())), preferred_element_type=F32)


def dot_tn(left, right):
    return lax.dot_general(left, right, (((0,), (0,)), ((), ())), preferred_element_type=F32)


def span(start, size):
    return pl.ds(pl.multiple_of(start, size), size)


def remote(src, dst, send_sem, recv_sem, where):
    return pltpu.make_async_remote_copy(
        src_ref=src,
        dst_ref=dst,
        send_sem=send_sem,
        recv_sem=recv_sem,
        device_id=where,
        device_id_type=MESH,
    )


def greet(peers):
    barrier = pltpu.get_barrier_semaphore()
    count = jnp.int32(0)
    for present, where in peers:

        @pl.when(present)
        def _():
            pl.semaphore_signal(barrier, inc=1, device_id=where, device_id_type=MESH)

        count = count + present.astype(jnp.int32)
    pl.semaphore_wait(barrier, count)


def line_peers(r, c, n_col):
    always = c >= 0
    return [
        (c > 0, {"col": jnp.maximum(c - 1, 0)}),
        (c < n_col - 1, {"col": jnp.minimum(c + 1, n_col - 1)}),
        (always, {"row": 1 - r}),
    ]


def group_peers(r, c, n_col):
    return [
        ((c != at) | (r != half), {"row": jnp.int32(half), "col": jnp.int32(at)})
        for half in range(2)
        for at in range(n_col)
    ]


class Gather:
    def __init__(self, full, send, recv, r, c, n_col, width, n_chunk=N_CHUNK):
        self.full, self.send, self.recv = full, send, recv
        self.r, self.c, self.n_col, self.width = r, c, n_col, width
        self.n_chunk = n_chunk

    def piece(self, half, at, chunk):
        cols = span(half * (self.n_col * self.width) + at * self.width, self.width)
        return self.full.at[chunk, :, cols]

    def copy(self, way, at, chunk):
        piece = self.piece(self.r, at, chunk)
        where = (
            {"col": jnp.maximum(self.c - 1, 0)},
            {"col": jnp.minimum(self.c + 1, self.n_col - 1)},
            {"row": 1 - self.r},
        )[way]
        return remote(
            piece, piece, self.send.at[way, at, chunk], self.recv.at[self.r, at, chunk], where
        )

    def wait(self, half, at, chunk):
        piece = self.piece(half, at, chunk)
        remote(
            piece, piece, self.send.at[0, at, chunk], self.recv.at[half, at, chunk], {"row": 1 - self.r}
        ).wait_recv()

    def start(self, chunk):
        c = self.c

        @pl.when(c > 0)
        def _():
            self.copy(0, c, chunk).start()

        @pl.when(c < self.n_col - 1)
        def _():
            self.copy(1, c, chunk).start()

        self.copy(2, c, chunk).start()

    def relay(self, distance, chunk):
        c, last = self.c, self.n_col - 1

        @pl.when(c + distance <= last)
        def _():
            at = c + distance
            self.wait(self.r, at, chunk)

            @pl.when(c > 0)
            def _():
                self.copy(0, at, chunk).start()

            self.copy(2, at, chunk).start()

        @pl.when(c - distance >= 0)
        def _():
            at = c - distance
            self.wait(self.r, at, chunk)

            @pl.when(c < last)
            def _():
                self.copy(1, at, chunk).start()

            self.copy(2, at, chunk).start()

    def toward(self, way, at, chunk):
        piece = self.piece(self.r, at, chunk)
        where = {"col": jnp.clip(self.c - 1 + 2 * way, 0, self.n_col - 1)}
        return remote(piece, piece, self.send.at[way, at, chunk], self.recv.at[self.r, at, chunk], where)

    def hand(self, at, chunk, way=None):
        self.wait(self.r, at, chunk)
        if way is not None:
            self.toward(way, at, chunk).start()
        self.copy(2, at, chunk).start()

    def end_relay(self, distance, chunk):
        self.hand(jnp.where(self.c == 0, distance, 3 - distance), chunk)

    def middle_relay(self, kind, chunk):
        outward = (self.c == 2).astype(jnp.int32)
        near_end = 3 * outward
        at = {"a": 3 - self.c, "b": near_end, "c": 3 - near_end}[kind]
        self.hand(at, chunk, 1 - outward if kind == "b" else outward)

    def tick(self, now):
        for distance in range(self.n_col - 1, 0, -1):
            chunk = now + 1 - distance

            @pl.when((chunk >= 0) & (chunk < self.n_chunk))
            def _():
                self.relay(distance, chunk)

    def wait_other(self, chunk):
        def one(at, carry):
            self.wait(1 - self.r, at, chunk)
            return carry

        lax.fori_loop(0, self.n_col, one, 0)

    def finish(self):
        c, last = self.c, self.n_col - 1

        def one(step, carry):
            at, chunk = step // self.n_chunk, step % self.n_chunk

            @pl.when((c > 0) & (at >= c))
            def _():
                self.copy(0, at, chunk).wait_send()

            @pl.when((c < last) & (at <= c))
            def _():
                self.copy(1, at, chunk).wait_send()

            self.copy(2, at, chunk).wait_send()
            return carry

        lax.fori_loop(0, self.n_col * self.n_chunk, one, 0)


class Scatter:
    def __init__(self, part, stage, inbox, send, recv, c, n_col, n_chunk=N_CHUNK):
        self.part, self.stage, self.inbox = part, stage, inbox
        self.send, self.recv, self.c, self.n_col = send, recv, c, n_col
        self.n_chunk = n_chunk
        self.width = stage.shape[-1]
        self.middle = (c > 0) & (c < n_col - 1)

    def term(self, chunk, dest):
        return self.part[chunk, :, span(dest * self.width, self.width)]

    def staged(self, dest):
        return dest - (dest > self.c).astype(jnp.int32)

    def slot(self, way, dest, at):
        inner = ((at == 1) & (way == 1)) | ((at == 2) & (way == 0))
        return jnp.where((dest == at) & inner, 4, dest)

    def copy(self, way, chunk, dest):
        where = jnp.clip(self.c + 1 - 2 * way, 0, self.n_col - 1)
        slot = self.slot(way, dest, where)
        return remote(
            self.stage.at[chunk, self.staged(dest)],
            self.inbox.at[chunk, slot],
            self.send.at[chunk, dest],
            self.recv.at[chunk, slot],
            {"col": where},
        )

    def arrival(self, way, chunk, dest):
        slot = self.slot(way, dest, self.c)
        here = self.inbox.at[chunk, slot]
        remote(here, here, self.send.at[chunk, dest], self.recv.at[chunk, slot], {"col": self.c}).wait_recv()
        return self.inbox[chunk, slot].astype(F32)

    def open(self, chunk):
        @pl.when(jnp.logical_not(self.middle))
        def _():
            way = (self.c > 0).astype(jnp.int32)

            def ship(step, carry):
                dest = jnp.where(way == 0, self.n_col - 1 - step, step)
                self.stage[chunk, self.staged(dest)] = self.term(chunk, dest).astype(BF16)
                self.copy(way, chunk, dest).start()
                return carry

            lax.fori_loop(0, self.n_col - 1, ship, 0)

    def pass_on(self, way, chunk, dest):
        total = self.term(chunk, dest) + self.arrival(way, chunk, dest)
        self.stage[chunk, self.staged(dest)] = total.astype(BF16)
        self.copy(way, chunk, dest).start()

    def near(self, chunk):
        @pl.when(self.middle)
        def _():
            way = (self.c > 1).astype(jnp.int32)

            def step_on(step, carry):
                self.pass_on(way, chunk, jnp.where(way == 0, self.n_col - 1 - step, step))
                return carry

            lax.fori_loop(0, 2, step_on, 0)

    def far(self, chunk):
        @pl.when(self.middle)
        def _():
            way = (self.c == 1).astype(jnp.int32)
            self.pass_on(way, chunk, jnp.where(self.c == 1, 0, self.n_col - 1))

    def total(self, chunk, out, at):
        c = self.c
        way = (c == 0).astype(jnp.int32)
        out[at, :] = self.term(chunk, c) + self.arrival(way, chunk, c)

        @pl.when(self.middle)
        def _():
            out[at, :] += self.arrival(1, chunk, c)

    def finish(self):
        def one(step, carry):
            chunk, dest = step // self.n_col, step % self.n_col

            @pl.when(dest != self.c)
            def _():
                self.copy(0, chunk, dest).wait_send()

            return carry

        lax.fori_loop(0, self.n_chunk * self.n_col, one, 0)

    @staticmethod
    def scratch(n_col, rows, width, n_chunk=N_CHUNK):
        return [
            pltpu.VMEM((n_chunk, rows, n_col * width), F32),
            pltpu.VMEM((n_chunk, n_col - 1, rows, width), BF16),
            pltpu.VMEM((n_chunk, n_col + 1, rows, width), BF16),
            pltpu.SemaphoreType.DMA((n_chunk, n_col)),
            pltpu.SemaphoreType.DMA((n_chunk, n_col + 1)),
        ]


def gather_sems(n_col, n_chunk=N_CHUNK):
    return [
        pltpu.SemaphoreType.DMA((3, n_col, n_chunk)),
        pltpu.SemaphoreType.DMA((2, n_col, n_chunk)),
    ]


N_NOTE = 16


def put_notes(full, chunk, cols, values):
    rows = full.shape[1] - N_NOTE
    width = values[0].shape[1]
    at = lax.broadcasted_iota(jnp.int32, (N_NOTE, width), 0)
    notes = jnp.zeros((N_NOTE, width), F32)
    for n, value in enumerate(values):
        for piece in range(3):
            rounded = value.astype(BF16).astype(F32)
            notes = jnp.where(at == 3 * n + piece, rounded, notes)
            value = value - rounded
    full[chunk, rows:, cols] = notes.astype(BF16)


def get_note(full, chunk, cols, n):
    rows = full.shape[1] - N_NOTE
    notes = full[chunk, rows:, cols].astype(F32)
    return (notes[3 * n : 3 * n + 1, :] + notes[3 * n + 1 : 3 * n + 2, :]) + notes[3 * n + 2 : 3 * n + 3, :]


def as_row(column):
    return jnp.broadcast_to(column, (column.shape[0], 128)).T[0:1, :]


def as_column(row):
    return jnp.broadcast_to(row, (128, row.shape[1])).T[:, 0:1]


class Totals:
    def __init__(self, held, sent, inbox, send, recv, r, c):
        self.held, self.sent, self.inbox, self.send, self.recv = held, sent, inbox, send, recv
        self.partners = ({"row": 1 - r}, {"col": c + 1 - 2 * (c % 2)}, {"col": c + 2 - 4 * (c // 2)})

    def note(self, chunk, column):
        self.held[pl.ds(chunk, 1), :] = as_row(column)

    def copy(self, step):
        return remote(
            self.sent.at[step], self.inbox.at[step], self.send.at[step], self.recv.at[step], self.partners[step]
        )

    def exchange(self):
        for step in range(3):
            self.sent[step] = self.held[...]
            copy = self.copy(step)
            copy.start()
            copy.wait_recv()
            self.held[...] += self.inbox[step]

    def column(self, chunk):
        return as_column(self.held[pl.ds(chunk, 1), :])

    def finish(self):
        for step in range(3):
            self.copy(step).wait_send()

    @staticmethod
    def scratch(rows):
        return [
            pltpu.VMEM((8, rows), F32),
            pltpu.VMEM((3, 8, rows), F32),
            pltpu.VMEM((3, 8, rows), F32),
            pltpu.SemaphoreType.DMA((3,)),
            pltpu.SemaphoreType.DMA((3,)),
        ]


def lanes(shape):
    return lax.broadcasted_iota(jnp.int32, shape, len(shape) - 1)


def swap_halves(values):
    half, width = HD // 2, values.shape[-1]
    low = (lanes(values.shape) & (HD - 1)) < half
    return jnp.where(
        low, pltpu.roll(values, width - half, 1), pltpu.roll(values, half, 1)
    )


def widen(table, width):
    return jnp.concatenate([table] * (width // table.shape[-1]), axis=-1)


class Flush:
    def __init__(self, pairs, sems, rows):
        self.pairs, self.sems, self.rows = pairs, sems, rows

    def copy(self, n, chunk):
        source, target = self.pairs[n]
        at = span(chunk * self.rows, self.rows)
        if isinstance(source, tuple):
            source = source[0].at[chunk, 0 : self.rows, source[1]]
        else:
            source = source.at[at, :]
        return pltpu.make_async_copy(source, target.at[at, :], self.sems.at[n, chunk])

    def start(self, chunk, which=None):
        for n in range(len(self.pairs)) if which is None else which:
            self.copy(n, chunk).start()

    def finish(self):
        def one(chunk, carry):
            for n in range(len(self.pairs)):
                self.copy(n, chunk).wait()
            return carry

        lax.fori_loop(0, N_CHUNK, one, 0)


def fetches(pairs, sems):
    copies = [pltpu.make_async_copy(source, target, sems.at[n]) for n, (source, target) in enumerate(pairs)]
    for copy in copies:
        copy.start()
    return copies


def vmem():
    return pl.BlockSpec(memory_space=pltpu.VMEM)


def anywhere():
    return pl.BlockSpec(memory_space=pl.ANY)


def kernel_call(body, name, ident, outs, out_any, in_specs, scratch, flops):
    return pl.pallas_call(
        body,
        out_shape=outs,
        in_specs=in_specs,
        out_specs=[anywhere() if flag else vmem() for flag in out_any],
        scratch_shapes=scratch,
        compiler_params=pltpu.CompilerParams(
            collective_id=ident, has_side_effects=True, vmem_limit_bytes=VMEM_LIMIT
        ),
        cost_estimate=pl.CostEstimate(flops=flops, bytes_accessed=1 << 24, transcendentals=0),
        name=name,
    )


def project_kernel(
    n_col,
    x, gain, positions, segments, rope, dy, wq, wk, wv, wo, wg, wu, wd,
    q_out, k_out, v_out, h1_out, r1, cos_table, sin_table, seg_col, dy_end, dy_mid,
    wo_other, wg_other, wu_other, wd_other,
    full, hidden, weights, q, k, v, h1, ag_send, ag_recv,
    w_send, w_recv, d_send, d_recv, local, flushed,
):
    r, c = lax.axis_index("row"), lax.axis_index("col")
    tok, width = x.shape
    half = n_col * width
    heads = wq.shape[1] // 2
    units = wg.shape[1] // 2
    me = r * n_col + c
    rows = tok // N_CHUNK
    held = fetches(
        [
            (
                w.at[:, span(r * heads, heads)],
                weights.at[span(r * half, half), pl.ds(n * heads, heads)],
            )
            for n, w in enumerate((wq, wk, wv))
        ],
        local,
    )
    mine = span(me * width, width)
    for chunk in range(N_CHUNK):
        values = x[chunk * rows : (chunk + 1) * rows, :]
        full[chunk, 0:rows, mine] = values
        values = values.astype(F32)
        square = as_row(jnp.sum(values * values, axis=1, keepdims=True))
        put_notes(full, chunk, mine, (square, gain[...]))
    greet(group_peers(r, c, n_col))
    gather = Gather(full, ag_send, ag_recv, r, c, n_col, width)
    flush = Flush(((q, q_out), (k, k_out), (v, v_out), (h1, h1_out)), flushed, rows)

    def chunk_rows(chunk):
        return span(chunk * rows, rows)

    gather.start(0)
    gather.start(1)
    other = {"row": 1 - r}
    moved = [
        remote(
            w.at[:, span((1 - r) * heads, heads)],
            weights.at[span(r * half, half), pl.ds(n * heads, heads)],
            w_send.at[n], w_recv.at[n], other,
        )
        for n, w in enumerate((wq, wk, wv))
    ]
    moved.append(remote(wo.at[span((1 - r) * heads, heads), :], wo_other, w_send.at[3], w_recv.at[3], other))
    moved.append(remote(wg.at[:, span((1 - r) * units, units)], wg_other, w_send.at[4], w_recv.at[4], other))
    moved.append(remote(wu.at[:, span((1 - r) * units, units)], wu_other, w_send.at[5], w_recv.at[5], other))
    moved.append(remote(wd.at[span((1 - r) * units, units), :], wd_other, w_send.at[6], w_recv.at[6], other))
    inward = {"col": jnp.where(c == 0, 1, jnp.where(c == 1, 2, jnp.where(c == 2, 1, 2)))}
    at_end = (c == 0) | (c == 3)
    early_end = remote(dy, dy_end, d_send.at[0], d_recv.at[0], inward)
    early_mid = remote(dy, dy_mid, d_send.at[0], d_recv.at[1], inward)

    for copy in moved[:3]:
        copy.start()
    gather.tick(0)
    gather.start(2)
    for copy in moved[3:]:
        copy.start()

    def tables(chunk, carry):
        at = chunk_rows(chunk)
        place = jnp.broadcast_to(positions[:, at].astype(F32), (128, rows)).T
        angles = place * rope[0:1, :]
        cos_table[at, :] = jnp.cos(angles)
        sin_table[at, :] = jnp.sin(angles) * rope[1:2, :]
        seg_col[at, :] = jnp.broadcast_to(segments[:, at].astype(F32), (128, rows)).T
        return carry

    lax.fori_loop(0, N_CHUNK, tables, 0)
    gather.tick(1)
    gather.start(3)
    pl.when(at_end)(early_end.start)
    gather.tick(2)

    def compute(chunk):
        at = chunk_rows(chunk)
        square = jnp.zeros((1, rows), F32)
        for block in range(2 * n_col):
            square = square + get_note(full, chunk, pl.ds(block * width, width), 0)
        scale = lax.rsqrt(as_column(square) * (1.0 / (2 * half)) + norm_eps)
        r1[at, :] = jnp.broadcast_to(scale, (rows, r1.shape[1]))
        for block in range(2 * n_col):
            cols = pl.ds(block * width, width)
            values = full[chunk, 0:rows, cols].astype(F32)
            hidden[:, cols] = (values * scale * get_note(full, chunk, cols, 1)).astype(BF16)
        h1[at, :] = hidden[:, span(r * half, half)]
        values = dot_nn(hidden[...], weights[...])
        cos_rows = widen(cos_table[at, :], heads)
        sin_rows = widen(sin_table[at, :], heads)
        for n, out in enumerate((q, k)):
            part = values[:, n * heads : (n + 1) * heads]
            out[at, :] = (part * cos_rows + swap_halves(part) * sin_rows).astype(BF16)
        v[at, :] = values[:, 2 * heads :].astype(BF16)
        flush.start(chunk)

    for copy in held:
        copy.wait()
    for copy in moved[:3]:
        copy.wait_recv()

    def step(chunk, carry):
        gather.wait_other(chunk)
        compute(chunk)
        gather.tick(chunk + 3)
        pl.when((chunk == 0) & jnp.logical_not(at_end))(early_mid.start)
        return carry

    lax.fori_loop(0, N_CHUNK, step, 0)
    gather.finish()
    for copy in moved[3:]:
        copy.wait_recv()
    for copy in moved:
        copy.wait_send()
    early_end.wait_send()

    @pl.when(jnp.logical_not(at_end))
    def _():
        early_end.wait_recv()
        early_mid.wait_recv()

    flush.finish()


def project(n_col, x, gain, positions, segments, dy, wq, wk, wv, wo, wg, wu, wd):
    tok, width = x.shape
    full = 2 * n_col * width
    half = n_col * width
    heads, units = wq.shape[1] // 2, wg.shape[1] // 2
    lane = jnp.arange(128) % HD
    inv_freq = rope_base ** (-2.0 * (lane % (HD // 2)).astype(F32) / HD)
    rope = jnp.stack([inv_freq, jnp.where(lane < HD // 2, -1.0, 1.0)])
    shape = jax.ShapeDtypeStruct
    outs = [
        shape((tok, heads), BF16), shape((tok, heads), BF16), shape((tok, heads), BF16),
        shape((tok, half), BF16), shape((tok, 128), F32),
        shape((tok, 128), F32), shape((tok, 128), F32), shape((tok, 128), F32),
        shape((tok, width), BF16), shape((tok, width), BF16),
        shape((heads, wo.shape[1]), BF16), shape((half, units), BF16),
        shape((half, units), BF16), shape((units, wd.shape[1]), BF16),
    ]
    scratch = [
        pltpu.VMEM((N_CHUNK, tok // N_CHUNK + N_NOTE, full), BF16),
        pltpu.VMEM((tok // N_CHUNK, full), BF16),
        pltpu.VMEM((full, 3 * heads), BF16),
        *[pltpu.VMEM((tok, heads), BF16)] * 3,
        pltpu.VMEM((tok, half), BF16),
        *gather_sems(n_col),
        pltpu.SemaphoreType.DMA((7,)),
        pltpu.SemaphoreType.DMA((7,)),
        pltpu.SemaphoreType.DMA((1,)),
        pltpu.SemaphoreType.DMA((2,)),
        pltpu.SemaphoreType.DMA((3,)),
        pltpu.SemaphoreType.DMA((4, N_CHUNK)),
    ]
    return kernel_call(
        functools.partial(project_kernel, n_col), "project", 1, outs,
        [True] * 4 + [False] * 4 + [True] * 6,
        [vmem()] * 5 + [anywhere()] * 8, scratch, 6 * tok * full * heads,
    )(x, gain, positions, segments, rope, dy, wq, wk, wv, wo, wg, wu, wd)


def allowed_pairs(seg_col, seg_row, chunk, rows, keys):
    seg_row = seg_row.astype(F32)
    query_at = chunk * rows + lax.broadcasted_iota(jnp.int32, (rows, keys), 0)
    key_at = lanes((rows, keys))
    return (key_at <= query_at) & (seg_col[:, 0:1] == seg_row)


def of_head(values, head):
    return jnp.where((lanes(values.shape) // HD) == head, values, jnp.zeros_like(values))


class LateGather:
    def __init__(self, full, send, recv, r, c, n_col, width):
        self.inner = Gather(full, send, recv, r, c, n_col, width)
        self.c = c
        self.end = (c == 0) | (c == 3)
        self.near_end = jnp.where(c < 2, 0, 3)
        self.far_end = 3 - self.near_end
        self.other = 3 - c
        self.outward = (c >= 2).astype(jnp.int32)

    def copy(self, way, at, chunk):
        piece = self.inner.piece(self.inner.r, at, chunk)
        where = ({"col": self.near_end}, {"col": self.other}, {"row": 1 - self.inner.r})[way]
        return remote(
            piece, piece, self.inner.send.at[way, at, chunk], self.inner.recv.at[self.inner.r, at, chunk], where
        )

    def start(self, chunk):
        c = self.c
        self.copy(2, c, chunk).start()

        @pl.when(jnp.logical_not(self.end))
        def _():
            self.copy(0, c, chunk).start()
            self.copy(1, self.near_end, chunk).start()
            self.copy(0, self.other, chunk).start()
            self.copy(2, self.near_end, chunk).start()
            self.copy(2, self.other, chunk).start()

    def relay(self, chunk):
        @pl.when(jnp.logical_not(self.end))
        def _():
            self.inner.wait(self.inner.r, self.far_end, chunk)
            self.copy(0, self.far_end, chunk).start()
            self.copy(2, self.far_end, chunk).start()

    def collect(self, chunk):
        @pl.when(self.end)
        def _():
            for step in range(3):
                at = jnp.where(self.c == 0, 1 + step, 2 - step)
                self.inner.wait(self.inner.r, at, chunk)
                self.copy(2, at, chunk).start()

    def finish(self):
        def one(step, carry):
            at, chunk = step // 4, step % 4
            self.copy(2, at, chunk).wait_send()

            @pl.when(jnp.logical_not(self.end))
            def _():
                pl.when(at != self.near_end)(lambda: self.copy(0, at, chunk).wait_send())
                pl.when(at == self.near_end)(lambda: self.copy(1, at, chunk).wait_send())

            return carry

        lax.fori_loop(0, 4 * N_CHUNK, one, 0)


def layer_kernel(
    n_col, n_sum,
    q_in, k_in, v_in, seg_row, seg_col_in, x_in, gain, wo, dy, dy_end, dy_mid,
    wg, wu, wd, wg_other, wu_other, wd_other,
    heads_out, inv_sum, middle_out, dy_out,
    h2_out, units_out, gate_out, up_out, middle_grad_out, branch_out, gain_sum, sum_out,
    q, k, v, seg_col, x, heads_all, middle, dy_full, w_out,
    units, grad_gate, grad_up, grad_middle,
    full, gate_own, up_own, down_own, gate_far, up_far,
    part, stage_z, inbox_z, z_send, z_recv, stage_f, inbox_f, f_send, f_recv,
    held, sent, arrived, t_send, t_recv, dy_send, dy_recv, ag_send, ag_recv,
    h_send, h_recv, x_send, x_recv, local, flushed, *refs,
):
    r, c = lax.axis_index("row"), lax.axis_index("col")
    tok, heads = q.shape
    width = x.shape[1]
    half = n_col * width
    n_unit = down_own.shape[0]
    rows = tok // N_CHUNK
    me = r * n_col + c
    row_base = r * n_col
    sums = refs[0:1]
    mine, far = span(r * n_unit, n_unit), span((1 - r) * n_unit, n_unit)
    near_rows, far_rows = span(r * half, half), span((1 - r) * half, half)
    block = span(me * width, width)
    everything = pl.ds(0, dy_full.shape[2])

    def chunk_rows(chunk):
        return span(chunk * rows, rows)

    scale_wide, grad_branch = seg_col, x
    late = LateGather(dy_full, dy_send, dy_recv, r, c, n_col, width)
    gather = Gather(full, ag_send, ag_recv, r, c, n_col, width)
    scatter_z = Scatter(part, stage_z, inbox_z, z_send, z_recv, c, n_col)
    scatter_f = Scatter(part, stage_f, inbox_f, f_send, f_recv, c, n_col)
    totals = Totals(held, sent, arrived, t_send, t_recv, r, c)
    flush = Flush(
        (
            ((full, near_rows), h2_out), (grad_gate, gate_out), (grad_up, up_out), (units, units_out),
            (grad_middle, middle_grad_out), (grad_branch, branch_out),
            (heads_all, heads_out), (middle, middle_out), ((dy_full, everything), dy_out),
        ),
        flushed, rows,
    )
    panels = []
    if n_sum:

        def tile(owner, side):
            cols = half // 4
            n_row = sums[0].shape[0]
            right = dy_full[:, :, span(r * half + side * cols, cols)].reshape(tok, cols)
            return dot_tn(units[:, span(owner * n_row, n_row)], right)

        panels.append(Reduce(tile, sums, *refs[1:]))

    def block_load(source, at):
        return source.reshape(N_CHUNK, rows, width), dy_full.at[:, :, span(at * width, width)]

    own, *first = fetches(
        [block_load(dy, me), (q_in, q), (k_in, k), (v_in, v), (seg_col_in, seg_col), (wo, w_out), (x_in, x)],
        local,
    )
    early = [
        pltpu.make_async_copy(*block_load(dy_end, row_base + late.near_end), local.at[7]),
        pltpu.make_async_copy(*block_load(dy_mid, row_base + late.other), local.at[8]),
    ]

    @pl.when(jnp.logical_not(late.end))
    def _():
        for copy in early:
            copy.start()

    greet(group_peers(r, c, n_col) + (square_peers() if n_sum else []))
    loads = fetches(
        [
            (wg.at[:, mine], gate_own.at[near_rows, :]),
            (wg_other, gate_own.at[far_rows, :]),
            (wu.at[:, mine], up_own.at[near_rows, :]),
            (wu_other, up_own.at[far_rows, :]),
            (wd.at[mine, :], down_own.at[:, near_rows]),
            (wd_other, down_own.at[:, far_rows]),
            (wg.at[:, far], gate_far),
            (wu.at[:, far], up_far),
        ],
        local.at[pl.ds(9, 8)],
    )
    own.wait()

    @pl.when(jnp.logical_not(late.end))
    def _():
        for copy in early:
            copy.wait()


    def heads_copy(chunk):
        piece = heads_all.at[pl.ds(chunk * rows, rows), span(r * heads, heads)]
        return remote(piece, piece, h_send.at[chunk], h_recv.at[chunk], {"row": 1 - r})

    def attend(chunk):
        at = pl.ds(chunk * rows, rows)
        keys = (chunk + 1) * rows
        allowed = allowed_pairs(seg_col[at, :], seg_row[:, 0:keys], chunk, rows, keys)

        def head_step(head, carry):
            total, inverse = carry
            scores = dot_nt(of_head(q[at, :], head), k[0:keys, :]) * HD**-0.5
            weights = jnp.exp(jnp.where(allowed, scores, masked_score))
            inv = 1.0 / jnp.sum(weights, axis=1, keepdims=True)
            probs = (weights * inv).astype(BF16)
            total = total + dot_nn(probs, of_head(v[0:keys, :], head))
            inverse = jnp.where(lanes((rows, 128)) == head, inv, inverse)
            return total, inverse

        total, inverse = lax.fori_loop(
            0, heads // HD, head_step, (jnp.zeros((rows, heads), F32), jnp.zeros((rows, 128), F32))
        )
        heads_all[at, span(r * heads, heads)] = total.astype(BF16)
        inv_sum[at, :] = inverse
        heads_copy(chunk).start()

    def contract(chunk):
        heads_copy(chunk).wait_recv()
        flush.start(chunk, (6,))
        part[chunk] = dot_nn(heads_all[span(chunk * rows, rows), :], w_out[...])
        scatter_z.open(chunk)

    def settle_z(chunk):
        at = chunk_rows(chunk)
        scatter_z.total(chunk, middle, at)
        values = middle[at, :] + x[at, :].astype(F32)
        middle[at, :] = values
        full[chunk, 0:rows, block] = (values * gain[...]).astype(BF16)
        put_notes(full, chunk, block, (as_row(jnp.sum(values * values, axis=1, keepdims=True)),))
        gather.start(chunk)
        flush.start(chunk, (7,))

    def exchange(n, chunk):
        piece = (grad_gate, grad_up, units)[n].at[chunk_rows(chunk), mine]
        return remote(piece, piece, x_send.at[n, chunk], x_recv.at[n, chunk], {"row": 1 - r})

    def norm(chunk):
        square = jnp.zeros((1, rows), F32)
        for at in range(2 * n_col):
            square = square + get_note(full, chunk, pl.ds(at * width, width), 0)
        scale = lax.rsqrt(as_column(square) * (1.0 / (2 * half)) + norm_eps)
        scale_wide[chunk_rows(chunk), :] = jnp.broadcast_to(scale, (rows, scale_wide.shape[1]))

    size = n_unit // 2

    def units_part(chunk, step):
        at = chunk_rows(chunk)
        scale = scale_wide[at, 0:1]
        cols = span(step * size, size)
        gate = dot_nn(full[chunk, 0:rows, :], gate_own[:, cols]) * scale
        up = dot_nn(full[chunk, 0:rows, :], up_own[:, cols]) * scale
        grad = dot_nt(dy_full[chunk], down_own[cols, :])
        sig = jax.nn.sigmoid(gate)
        act = gate * sig
        put = span(r * n_unit + step * size, size)
        units[at, put] = (act * up).astype(BF16)
        grad = grad * scale
        grad_gate[at, put] = (grad * up * sig * (1.0 + gate * (1.0 - sig))).astype(BF16)
        grad_up[at, put] = (grad * act).astype(BF16)

    def back(chunk):
        at = chunk_rows(chunk)
        part[chunk] = dot_nt(grad_gate[at, mine], gate_own[near_rows, :]) + dot_nt(
            grad_up[at, mine], up_own[near_rows, :]
        )
        for n in range(2):
            exchange(n, chunk).wait_recv()
        part[chunk] += dot_nt(grad_gate[at, far], gate_far[...]) + dot_nt(grad_up[at, far], up_far[...])
        scatter_f.open(chunk)
        exchange(2, chunk).wait_recv()
        flush.start(chunk, (0, 1, 2, 3, 8))

    def settle_f(chunk):
        at = chunk_rows(chunk)
        scatter_f.total(chunk, grad_middle, at)
        product = grad_middle[at, :] * middle[at, :]
        totals.note(chunk, jnp.sum(product * gain[...], axis=1, keepdims=True))
        gain_sum[...] += jnp.sum(product.reshape(rows // 8, 8, width), axis=0)

    def conclude(chunk):
        at = chunk_rows(chunk)
        mean = totals.column(chunk) * (1.0 / (2 * half))
        scale = scale_wide[at, 0:1]
        grad = (
            dy_full[chunk, :, block].astype(F32)
            + grad_middle[at, :] * gain[...]
            - middle[at, :] * (scale * scale * mean)
        )
        grad_middle[at, :] = grad
        grad_branch[at, :] = grad.astype(BF16)
        flush.start(chunk, (4, 5))

    middle_role = scatter_z.middle

    def at_end(*acts):
        @pl.when(jnp.logical_not(middle_role))
        def _():
            for act, *what in acts:
                act(*what)

    def at_middle(*acts):
        @pl.when(middle_role)
        def _():
            for act, *what in acts:
                act(*what)

    near, far_sum = scatter_z.near, scatter_z.far
    near_f, far_f = scatter_f.near, scatter_f.far
    end_relay, middle_relay = gather.end_relay, gather.middle_relay
    gain_sum[...] = jnp.zeros_like(gain_sum)
    at_end(*[(late.start, chunk) for chunk in range(N_CHUNK)])
    at_middle((late.start, 0), (late.start, 1), (late.start, 2))
    for copy in first:
        copy.wait()
    at_middle((late.relay, 0), (late.start, 3))
    attend(0)
    contract(0)
    at_middle((near, 0))
    attend(1)
    attend(2)
    at_middle((far_sum, 0))
    contract(1)
    at_middle((near, 1), (far_sum, 1))
    contract(2)
    at_middle((near, 2), (far_sum, 2))
    settle_z(0)
    settle_z(1)
    attend(3)
    at_middle((middle_relay, "b", 0))
    at_end((late.collect, 0))
    at_middle((middle_relay, "a", 0), (middle_relay, "b", 1), (middle_relay, "c", 0))
    settle_z(2)
    at_middle((late.relay, 1), (middle_relay, "c", 1), (middle_relay, "a", 1), (middle_relay, "a", 2))
    at_end((end_relay, 1, 0))
    contract(3)
    at_middle((near, 3), (middle_relay, "b", 2))
    at_end((end_relay, 3, 0), (end_relay, 2, 0))
    for copy in loads:
        copy.wait()

    def step(now, carry):
        late.inner.wait_other(now)
        gather.wait_other(now)
        norm(now)

        def part_step(n, carry):
            units_part(now, n)
            return carry

        lax.fori_loop(0, 2, part_step, 0)
        for n in range(3):
            exchange(n, now).start()
        pl.when(now == 1)(lambda: at_middle((near_f, 0), (middle_relay, "a", 3)))
        pl.when(now == 3)(lambda: at_middle((far_f, 1), (near_f, 2), (far_f, 2)))
        back(now)

        @pl.when(now == 0)
        def _():
            at_end((end_relay, 2, 1), (end_relay, 1, 1))
            at_middle((far_sum, 3))
            settle_z(3)
            at_middle((middle_relay, "c", 2), (late.relay, 2))
            at_end((end_relay, 3, 1), (late.collect, 1))

        @pl.when(now == 1)
        def _():
            at_middle((middle_relay, "b", 3), (late.relay, 3))
            at_end((end_relay, 1, 2), (end_relay, 2, 2), (end_relay, 2, 3), (end_relay, 3, 2), (late.collect, 2))

        @pl.when(now == 2)
        def _():
            at_middle((middle_relay, "c", 3), (far_f, 0), (near_f, 1))
            at_end((end_relay, 3, 3), (end_relay, 1, 3), (late.collect, 3))

        return carry

    lax.fori_loop(0, N_CHUNK, step, 0)
    for panel in panels:
        panel.first()
    at_middle((near_f, 3), (far_f, 3))
    for panel in panels:
        panel.second()

    def drain(now, carry):
        settle_f(now)
        return carry

    lax.fori_loop(0, N_CHUNK, drain, 0)
    totals.exchange()

    def close_up(chunk, carry):
        conclude(chunk)
        return carry

    lax.fori_loop(0, N_CHUNK, close_up, 0)
    gather.finish()
    late.finish()
    scatter_z.finish()
    scatter_f.finish()
    totals.finish()
    stores = []
    for panel in panels:
        panel.merge()
        panel.last()
        stores += fetches([(sums[0], sum_out)], local.at[pl.ds(17, 1)])
        panel.finish()

    def close(chunk, carry):
        heads_copy(chunk).wait_send()
        for n in range(3):
            exchange(n, chunk).wait_send()
        return carry

    lax.fori_loop(0, N_CHUNK, close, 0)
    for copy in stores:
        copy.wait()
    flush.finish()


def layer(
    n_col, n_dp, q, k, v, seg_row, seg_col, x, gain, wo, dy, dy_end, dy_mid,
    wg, wu, wd, wg_other, wu_other, wd_other,
):
    tok, heads = q.shape
    width = x.shape[1]
    half, n_unit = n_col * width, wg.shape[1] // 2
    rows = tok // N_CHUNK
    shape = jax.ShapeDtypeStruct
    n_sum = int(n_dp == 4)
    size = (wd.shape[0] // 4, half // 2) if n_sum else (8, 128)
    outs = [
        shape((tok, 2 * heads), BF16), shape((tok, 128), F32), shape((tok, width), F32),
        shape((tok, 2 * half), BF16), shape((tok, half), BF16),
        shape((tok, 2 * n_unit), BF16), shape((tok, 2 * n_unit), BF16), shape((tok, 2 * n_unit), BF16),
        shape((tok, width), F32), shape((tok, width), BF16), shape((8, width), F32), shape(size, F32),
    ]
    scatter = Scatter.scratch(n_col, rows, width)
    scratch = [
        *[pltpu.VMEM(array.shape, array.dtype) for array in (q, k, v, seg_col, x)],
        pltpu.VMEM((tok, 2 * heads), BF16),
        pltpu.VMEM((tok, width), F32),
        pltpu.VMEM((N_CHUNK, rows, 2 * half), BF16),
        pltpu.VMEM(wo.shape, BF16),
        *[pltpu.VMEM((tok, 2 * n_unit), BF16)] * 3,
        pltpu.VMEM((tok, width), F32),
        pltpu.VMEM((N_CHUNK, rows + N_NOTE, 2 * half), BF16),
        pltpu.VMEM((2 * half, n_unit), BF16),
        pltpu.VMEM((2 * half, n_unit), BF16),
        pltpu.VMEM((n_unit, 2 * half), BF16),
        pltpu.VMEM((half, n_unit), BF16),
        pltpu.VMEM((half, n_unit), BF16),
        *scatter,
        *scatter[1:],
        *Totals.scratch(rows),
        *gather_sems(n_col),
        *gather_sems(n_col),
        pltpu.SemaphoreType.DMA((N_CHUNK,)),
        pltpu.SemaphoreType.DMA((N_CHUNK,)),
        pltpu.SemaphoreType.DMA((3, N_CHUNK)),
        pltpu.SemaphoreType.DMA((3, N_CHUNK)),
        pltpu.SemaphoreType.DMA((18,)),
        pltpu.SemaphoreType.DMA((9, N_CHUNK)),
    ]
    if n_sum:
        scratch += [pltpu.VMEM(size, F32), *Reduce.scratch(size[0], size[1] // 2)]
    return kernel_call(
        functools.partial(layer_kernel, n_col, n_sum), "layer", 2, outs,
        [True, False, True, True] + [True] * 6 + [False, True],
        [anywhere()] * 3 + [vmem(), anywhere(), anywhere(), vmem()] + [anywhere()] * 10,
        scratch, 20 * tok * half * n_unit,
    )(
        q, k, v, seg_row, seg_col, x, gain, wo, dy, dy_end, dy_mid,
        wg, wu, wd, wg_other, wu_other, wd_other,
    )


class Reduce:
    def __init__(self, tile, outs, stage_one, inbox_one, stage_two, inbox_two, send, recv):
        d = lax.axis_index("dp")
        self.x, self.y = d % 2, d // 2
        self.tile, self.outs = tile, outs
        self.stage_one, self.inbox_one = stage_one, inbox_one
        self.stage_two, self.inbox_two = stage_two, inbox_two
        self.send, self.recv = send, recv
        self.along_x = {"dp": self.y * 2 + 1 - self.x}
        self.along_y = {"dp": (1 - self.y) * 2 + self.x}

    def along(self, side):
        return {"dp": jnp.where(side == 0, self.along_x["dp"], self.along_y["dp"])}

    def copy_one(self, side, n):
        return remote(
            self.stage_one.at[side, n], self.inbox_one.at[side, n],
            self.send.at[side, n], self.recv.at[side, n], self.along(side),
        )

    def copy_two(self, side):
        return remote(
            self.stage_two.at[side], self.inbox_two.at[side],
            self.send.at[side, 2], self.recv.at[side, 2], self.along(1 - side),
        )

    def first(self):
        def one(step, carry):
            side = step % 2
            near = jnp.where(side == 0, self.y, self.x)
            n = jnp.where(step < 2, 1 - near, near)
            owner = jnp.where(side == 0, n * 2 + 1 - self.x, (1 - self.y) * 2 + n)
            self.stage_one[side, n] = self.tile(owner, side).astype(BF16)
            self.copy_one(side, n).start()
            return carry

        lax.fori_loop(0, 4, one, 0)

    def second(self):
        def one(side, carry):
            n = jnp.where(side == 0, 1 - self.y, 1 - self.x)
            owner = jnp.where(side == 0, n * 2 + self.x, self.y * 2 + n)
            value = self.tile(owner, side)
            self.copy_one(side, n).wait_recv()
            self.stage_two[side] = (value + self.inbox_one[side, n].astype(F32)).astype(BF16)
            self.copy_two(side).start()
            return carry

        lax.fori_loop(0, 2, one, 0)

    def put(self, side, value, add):
        each = value.shape[1] // len(self.outs)
        cols = span(side * each, each)
        for n, out in enumerate(self.outs):
            term = value[:, n * each : (n + 1) * each]
            out[:, cols] = out[:, cols] + term if add else term

    def merge(self):
        def one(side, carry):
            n = jnp.where(side == 0, self.y, self.x)
            value = self.tile(self.y * 2 + self.x, side)
            self.copy_one(side, n).wait_recv()
            self.put(side, value + self.inbox_one[side, n].astype(F32), False)
            return carry

        lax.fori_loop(0, 2, one, 0)

    def last(self):
        def one(side, carry):
            self.copy_two(side).wait_recv()
            self.put(side, self.inbox_two[side].astype(F32), True)
            return carry

        lax.fori_loop(0, 2, one, 0)

    def finish(self):
        def one(side, carry):
            for n in range(2):
                self.copy_one(side, n).wait_send()
            self.copy_two(side).wait_send()
            return carry

        lax.fori_loop(0, 2, one, 0)

    @staticmethod
    def scratch(rows, cols):
        return [
            pltpu.VMEM((2, 2, rows, cols), BF16),
            pltpu.VMEM((2, 2, rows, cols), BF16),
            pltpu.VMEM((2, rows, cols), BF16),
            pltpu.VMEM((2, rows, cols), BF16),
            pltpu.SemaphoreType.DMA((2, 3)),
            pltpu.SemaphoreType.DMA((2, 3)),
        ]


def square_peers():
    d = lax.axis_index("dp")
    x, y = d % 2, d // 2
    always = d >= 0
    return [(always, {"dp": y * 2 + 1 - x}), (always, {"dp": (1 - y) * 2 + x})]


def tile_of(left, right, n_row, base=0, width=None):
    cols = (right.shape[1] if width is None else width) // 2

    def tile(owner, side):
        return dot_tn(left[:, span(owner * n_row, n_row)], right[:, span(base + side * cols, cols)])

    return tile


def branch_kernel(
    n_col, n_sum,
    branch, units_in, wd, middle_in, dy_full, h2_in, gate_in, wo, wo_other, heads_in,
    *refs,
):
    (output_out, heads_out, half_out), refs = refs[:3], refs[3:]
    sums_out, refs = refs[:n_sum], refs[n_sum:]
    (
        units, middle, h2, grad_gate, heads_all, branch_half, output, grad_heads,
        full, down, dy_half, w_out, part, stage, inbox, rs_send, rs_recv, ag_send, ag_recv, local, flushed,
    ), refs = refs[:21], refs[21:]
    sums, refs = refs[:n_sum], refs[n_sum:]
    r, c = lax.axis_index("row"), lax.axis_index("col")
    tok, width = middle.shape
    half = n_col * width
    heads = grad_heads.shape[1]
    rows = tok // N_CHUNK
    me = r * n_col + c
    mine, other = span(r * half, half), span((1 - r) * half, half)
    own, dy_load, units_load, down_load, *loads = fetches(
        [
            (branch.reshape(N_CHUNK, rows, width), full.at[:, :, span(me * width, width)]),
            (dy_full.at[:, mine], dy_half),
            (units_in, units),
            (wd, down),
            (h2_in, h2),
            (gate_in, grad_gate),
            (wo.at[span(r * heads, heads), :], w_out.at[:, mine]),
            (wo_other, w_out.at[:, other]),
            (middle_in, middle),
            (heads_in, heads_all),
        ],
        local,
    )
    greet(line_peers(r, c, n_col) + (square_peers() if n_sum else []))
    gather = Gather(full, ag_send, ag_recv, r, c, n_col, width)
    scatter = Scatter(part, stage, inbox, rs_send, rs_recv, c, n_col)
    flush = Flush(((output, output_out), (grad_heads, heads_out), (branch_half, half_out)), flushed, rows)
    own.wait()

    def begin_gather(chunk, carry):
        gather.start(chunk)
        return carry

    lax.fori_loop(0, N_CHUNK, begin_gather, 0)
    panels = []
    if n_sum:
        terms = ((units, dy_half, half // 2, half // 2), (h2, grad_gate, 0, None), (heads_all, branch_half, 0, None))
        for n, (left, right, base, cols) in enumerate(terms):
            tile = tile_of(left, right, sums[n].shape[0], base, cols)
            panels.append(Reduce(tile, (sums[n],), *refs[6 * n : 6 * n + 6]))
    dy_load.wait()
    units_load.wait()
    for panel in panels[:1]:
        panel.first()
    down_load.wait()

    def begin(chunk, carry):
        part[chunk] = dot_nn(units[span(chunk * rows, rows), :], down[...])
        scatter.open(chunk)
        gather.relay(1, chunk)
        return carry

    lax.fori_loop(0, N_CHUNK, begin, 0)
    for copy in loads:
        copy.wait()
    for panel in panels[1:2]:
        panel.first()

    def carry_on(chunk, carry):
        gather.relay(2, chunk)
        scatter.near(chunk)
        return carry

    lax.fori_loop(0, N_CHUNK, carry_on, 0)
    for panel in panels[:1]:
        panel.second()

    def arrive(chunk, carry):
        gather.relay(3, chunk)
        scatter.far(chunk)
        return carry

    lax.fori_loop(0, N_CHUNK, arrive, 0)

    def copy_half(chunk, carry):
        gather.wait_other(chunk)
        branch_half[span(chunk * rows, rows), :] = full[chunk, :, mine]
        return carry

    lax.fori_loop(0, N_CHUNK, copy_half, 0)
    for panel in panels[2:]:
        panel.first()
    for panel in panels[:1]:
        panel.merge()
    for panel in panels[1:2]:
        panel.second()

    def settle(chunk, carry):
        at = span(chunk * rows, rows)
        grad_heads[at, :] = dot_nt(full[chunk], w_out[...]).astype(BF16)
        scatter.total(chunk, output, at)
        output[at, :] += middle[at, :]
        flush.start(chunk)
        return carry

    lax.fori_loop(0, N_CHUNK, settle, 0)
    for panel in panels[1:2]:
        panel.merge()
    for panel in panels[2:]:
        panel.second()
        panel.merge()
    stores = []
    for n, panel in enumerate(panels):
        panel.last()
        stores += fetches([(sums[n], sums_out[n])], local.at[pl.ds(10 + n, 1)])
    gather.finish()
    scatter.finish()
    for panel in panels:
        panel.finish()
    for copy in stores:
        copy.wait()
    flush.finish()


def branch_back(n_col, n_dp, branch, units, wd, middle, dy_full, h2, grad_gate, wo, wo_other, heads_all):
    tok, width = middle.shape
    half, heads = n_col * width, wo_other.shape[0]
    rows = tok // N_CHUNK
    shape = jax.ShapeDtypeStruct
    outs = [shape((tok, width), F32), shape((tok, heads), BF16), shape((tok, half), BF16)]
    scratch = [
        pltpu.VMEM(units.shape, BF16),
        pltpu.VMEM(middle.shape, F32),
        pltpu.VMEM(h2.shape, BF16),
        pltpu.VMEM(grad_gate.shape, BF16),
        pltpu.VMEM(heads_all.shape, BF16),
        pltpu.VMEM((tok, half), BF16),
        pltpu.VMEM((tok, width), F32),
        pltpu.VMEM((tok, heads), BF16),
        pltpu.VMEM((N_CHUNK, rows, 2 * half), BF16),
        pltpu.VMEM(wd.shape, BF16),
        pltpu.VMEM((tok, half), BF16),
        pltpu.VMEM((heads, 2 * half), BF16),
        *Scatter.scratch(n_col, rows, width),
        *gather_sems(n_col),
        pltpu.SemaphoreType.DMA((13,)),
        pltpu.SemaphoreType.DMA((3, N_CHUNK)),
    ]
    n_sum = 0
    if n_dp == 4:
        n_sum = 3
        sizes = [(wd.shape[0] // 4, half // 2), (half // 4, grad_gate.shape[1]), (heads // 2, half)]
        outs += [shape(size, F32) for size in sizes]
        scratch += [pltpu.VMEM(size, F32) for size in sizes]
        for size in sizes:
            scratch += Reduce.scratch(size[0], size[1] // 2)
    return kernel_call(
        functools.partial(branch_kernel, n_col, n_sum), "branch", 4, outs, [True] * len(outs),
        [anywhere()] * 10, scratch, 12 * tok * half * half,
    )(branch, units, wd, middle, dy_full, h2, grad_gate, wo, wo_other, heads_all)


def attend_back_kernel(
    n_col, n_dp, n_sum,
    q_in, k_in, v_in, heads_grad_in, seg_row, seg_col_in, inv_in, cos_in, sin_in, x_in, r1_in, gain, middle_in,
    gain_two, h1_in, wq, wk, wv, h2_in, up_in,
    *refs,
):
    (tokens_out, gain_sums, triple_out), refs = refs[:3], refs[3:]
    sums_out, refs = refs[:n_sum], refs[n_sum:]
    (
        q, k, v, grad_heads, seg_col, inv_sum, cos_table, sin_table, x, r1, grad_middle,
        h1, h2, grad_up, grad_tokens, triple,
        weights, grad_k, grad_v, grad_q, grad_one, gain_mine, gain_box, part, stage, inbox, rs_send, rs_recv,
        held, sent, arrived, st_send, st_recv, x_send, x_recv, g_send, g_recv, local, flushed,
    ), refs = refs[:39], refs[39:]
    sums, refs = refs[:n_sum], refs[n_sum:]
    r, c, d = lax.axis_index("row"), lax.axis_index("col"), lax.axis_index("dp")
    tok, width = x.shape
    half = n_col * width
    heads = q.shape[1]
    rows = tok // N_CHUNK
    me = r * n_col + c
    early = [(h2_in, h2), (up_in, grad_up)]
    first = [
        (q_in, q), (k_in, k), (v_in, v), (heads_grad_in, grad_heads), (seg_col_in, seg_col), (inv_in, inv_sum),
        (cos_in, cos_table), (sin_in, sin_table),
    ]
    later = [(h1_in, h1), (x_in, x), (r1_in, r1)]
    later.append((middle_in, grad_middle))
    for n, w in enumerate((wq, wk, wv)):
        for side in range(2):
            later.append(
                (w.at[:, pl.ds(side * heads, heads)], weights.at[:, pl.ds((side * 3 + n) * heads, heads)])
            )
    copies = fetches(early + first + later, local)
    early, first, later = copies[:2], copies[2:10], copies[10:]
    dp_peers = [(d != at, {"dp": jnp.int32(at)}) for at in range(n_dp)]
    greet(group_peers(r, c, n_col) + dp_peers)
    scatter = Scatter(part, stage, inbox, rs_send, rs_recv, c, n_col)
    totals = Totals(held, sent, arrived, st_send, st_recv, r, c)
    flush = Flush(((grad_tokens, tokens_out),), flushed, rows)
    panels = []
    if n_sum:
        for n, (left, right) in enumerate(((h2, grad_up), (h1, triple))):
            tile = tile_of(left, right, sums[n].shape[0])
            panels.append(Reduce(tile, sums[1:] if n else sums[:1], *refs[6 * n : 6 * n + 6]))

    def exchange(chunk):
        piece = triple.at[span(chunk * rows, rows), span(r * 3 * heads, 3 * heads)]
        return remote(piece, piece, x_send.at[chunk], x_recv.at[chunk], {"row": 1 - r})

    def attend(chunk):
        at = pl.ds(chunk * rows, rows)
        keys = (chunk + 1) * rows
        allowed = allowed_pairs(seg_col[at, :], seg_row[:, 0:keys], chunk, rows, keys)
        grad_q[...] = jnp.zeros_like(grad_q)

        def head_step(head, carry):
            query = of_head(q[at, :], head)
            grad = of_head(grad_heads[at, :], head)
            scores = dot_nt(query, k[0:keys, :]) * HD**-0.5
            inv = jnp.sum(jnp.where(lanes((rows, 128)) == head, inv_sum[at, :], 0.0), axis=1, keepdims=True)
            probs = jnp.exp(jnp.where(allowed, scores, masked_score)) * inv
            grad_probs = dot_nt(grad, v[0:keys, :])
            weighted = jnp.sum(probs * grad_probs, axis=1, keepdims=True)
            grad_scores = (probs * (grad_probs - weighted) * HD**-0.5).astype(BF16)
            grad_q[...] += dot_nn(grad_scores, of_head(k[0:keys, :], head))
            grad_k[0:keys, :] += dot_tn(grad_scores, query)
            grad_v[0:keys, :] += dot_tn(probs.astype(BF16), grad)
            return carry

        lax.fori_loop(0, heads // HD, head_step, 0)
        cos_rows = widen(cos_table[at, :], heads)
        sin_rows = widen(sin_table[at, :], heads)
        for n, value in enumerate((grad_q[...], grad_k[at, :])):
            value = value * cos_rows - swap_halves(value) * sin_rows
            triple[at, span((r * 3 + n) * heads, heads)] = value.astype(BF16)
        triple[at, span((r * 3 + 2) * heads, heads)] = grad_v[at, :].astype(BF16)
        exchange(chunk).start()

    def contract(chunk):
        at = span(chunk * rows, rows)
        exchange(chunk).wait_recv()
        part[chunk] = dot_nt(triple[at, :], weights[...])
        scatter.open(chunk)

    def settle(chunk):
        at = span(chunk * rows, rows)
        scatter.total(chunk, grad_one, at)
        product = grad_one[at, :] * (x[at, :].astype(F32) * r1[at, 0:1])
        totals.note(chunk, jnp.sum(product * gain[...], axis=1, keepdims=True))
        gain_mine[0] += jnp.sum(product.reshape(rows // 8, 8, width), axis=0)

    def conclude(chunk):
        at = span(chunk * rows, rows)
        mean = totals.column(chunk) * (1.0 / (2 * half))
        scale = r1[at, 0:1]
        grad_tokens[at, :] = grad_middle[at, :] + scale * (
            grad_one[at, :] * gain[...] - x[at, :].astype(F32) * (scale * mean)
        )
        flush.start(chunk)

    def gain_copy(at):
        return remote(gain_box.at[d], gain_box.at[d], g_send.at[at], g_recv.at[d], {"dp": at})

    def gain_arrival(at):
        return remote(gain_box.at[at], gain_box.at[at], g_send.at[at], g_recv.at[at], {"dp": at})

    def others(act):
        def one(at, carry):
            pl.when(at != d)(lambda: act(at))
            return carry

        lax.fori_loop(0, n_dp, one, 0)

    def panel_do(n, what):
        if n_sum:
            getattr(panels[n], what)()

    gain_mine[0] = jnp.zeros(gain_mine.shape[1:], F32)
    gain_mine[1] = gain_two[...]
    grad_k[...] = jnp.zeros_like(grad_k)
    grad_v[...] = jnp.zeros_like(grad_v)
    last = N_CHUNK - 1
    for copy in early:
        copy.wait()
    panel_do(0, "first")
    for copy in first:
        copy.wait()
    attend(last)
    for copy in later:
        copy.wait()
    attend(last - 1)
    contract(last)
    panel_do(0, "second")
    attend(last - 2)
    contract(last - 1)
    scatter.near(last)
    attend(last - 3)
    contract(last - 2)
    scatter.near(last - 1)
    scatter.far(last)
    contract(last - 3)
    panel_do(1, "first")
    scatter.near(last - 2)
    scatter.far(last - 1)
    panel_do(0, "merge")
    settle(last)
    scatter.near(last - 3)
    scatter.far(last - 2)
    panel_do(1, "second")

    def settle_step(now, carry):
        pl.when(now == 1)(lambda: scatter.far(0))
        settle(last - now)
        return carry

    lax.fori_loop(1, N_CHUNK, settle_step, 0)
    gain_box[d] = gain_mine[...]
    others(lambda at: gain_copy(at).start())
    panel_do(1, "merge")
    totals.exchange()

    def close_up(step, carry):
        conclude(last - step)
        return carry

    lax.fori_loop(0, N_CHUNK, close_up, 0)
    others(lambda at: gain_arrival(at).wait_recv())
    gain_total = gain_box[0]
    for at in range(1, n_dp):
        gain_total = gain_total + gain_box[at]
    gain_sums[...] = gain_total
    stores = []
    where = len(copies)
    for n, panel in enumerate(panels):
        panel.last()
        for m in range(1, n_sum) if n else range(1):
            stores += fetches([(sums[m], sums_out[m])], local.at[pl.ds(where + m, 1)])
    if not n_sum:
        stores += fetches([(triple, triple_out)], local.at[pl.ds(where, 1)])
    scatter.finish()
    totals.finish()
    for chunk in range(N_CHUNK):
        exchange(chunk).wait_send()
    others(lambda at: gain_copy(at).wait_send())
    for panel in panels:
        panel.finish()
    for copy in stores:
        copy.wait()
    flush.finish()


def attend_back(
    n_col, n_dp,
    q, k, v, grad_heads, seg_row, seg_col, inv_sum, cos_table, sin_table, x, r1, gain, grad_middle,
    gain_two, h1, wq, wk, wv, h2, grad_up,
):
    tok, width = x.shape
    half, heads = n_col * width, q.shape[1]
    rows = tok // N_CHUNK
    shape = jax.ShapeDtypeStruct
    triple = (tok, 6 * heads) if n_dp != 4 else (8, 128)
    outs = [shape((tok, width), F32), shape((2, 8, width), F32), shape(triple, BF16)]
    held = [q, k, v, grad_heads, seg_col, inv_sum, cos_table, sin_table, x, r1, grad_middle]
    held += [h1, h2, grad_up]
    scratch = [
        *[pltpu.VMEM(array.shape, array.dtype) for array in held],
        pltpu.VMEM((tok, width), F32),
        pltpu.VMEM((tok, 6 * heads), BF16),
        pltpu.VMEM((half, 6 * heads), BF16),
        pltpu.VMEM((tok, heads), F32),
        pltpu.VMEM((tok, heads), F32),
        pltpu.VMEM((rows, heads), F32),
        pltpu.VMEM((tok, width), F32),
        pltpu.VMEM((2, 8, width), F32),
        pltpu.VMEM((n_dp, 2, 8, width), F32),
        *Scatter.scratch(n_col, rows, width),
        *Totals.scratch(rows),
        pltpu.SemaphoreType.DMA((N_CHUNK,)),
        pltpu.SemaphoreType.DMA((N_CHUNK,)),
        pltpu.SemaphoreType.DMA((n_dp,)),
        pltpu.SemaphoreType.DMA((n_dp,)),
        pltpu.SemaphoreType.DMA((27,)),
        pltpu.SemaphoreType.DMA((1, N_CHUNK)),
    ]
    n_sum = 0
    if n_dp == 4:
        sizes = [(half // 4, grad_up.shape[1])] + [(half // 4, 2 * heads)] * 3
        n_sum = len(sizes)
        outs += [shape(size, F32) for size in sizes]
        scratch += [pltpu.VMEM(size, F32) for size in sizes]
        for size in sizes[:1] + [(half // 4, 6 * heads)]:
            scratch += Reduce.scratch(size[0], size[1] // 2)
    return kernel_call(
        functools.partial(attend_back_kernel, n_col, n_dp, n_sum), "attend_back", 5, outs,
        [True, False, True] + [True] * n_sum,
        [anywhere()] * 4 + [vmem()] + [anywhere()] * 6 + [vmem(), anywhere(), vmem()] + [anywhere()] * 6,
        scratch, 16 * tok * tok * heads,
    )(
        q, k, v, grad_heads, seg_row, seg_col, inv_sum, cos_table, sin_table, x, r1, gain, grad_middle,
        gain_two, h1, wq, wk, wv, h2, grad_up,
    )


def finish_kernel(groups, share, gain_sums, *refs):
    n_copy = sum(groups)
    sources, refs = refs[:n_copy], refs[n_copy:]
    gain_out, refs = refs[:2], refs[2:]
    results, refs = refs[: len(groups)], refs[len(groups) :]
    held, (get, put) = refs[:n_copy], refs[n_copy:]
    targets = []
    for result, parts in zip(results, groups):
        cols = result.shape[1] // parts
        targets += [result.at[:, pl.ds(part * cols, cols)] for part in range(parts)]
    pieces = 2
    inward, outward = [], []
    for n, (source, keep, target) in enumerate(zip(sources, held, targets)):
        rows = keep.shape[0] // pieces
        for piece in range(pieces):
            at = pl.ds(piece * rows, rows)
            inward.append(pltpu.make_async_copy(source.at[at, :], keep.at[at, :], get.at[n, piece]))
            outward.append(pltpu.make_async_copy(keep.at[at, :], target.at[at, :], put.at[n, piece]))
    for copy in inward:
        copy.start()
    d = lax.axis_index("dp")
    width = gain_sums.shape[-1]
    shift = lax.rem(width - d * share, width)
    for n in range(2):
        moved = pltpu.roll(gain_sums[n], shift, 1)
        gain_out[n][...] = jnp.sum(moved, axis=0, keepdims=True)[:, 0:share]
    for one, two in zip(inward, outward):
        one.wait()
        two.start()
    for copy in outward:
        copy.wait()


def finish(share, gain_sums, arrays):
    shape = jax.ShapeDtypeStruct
    groups = tuple(len(parts) for parts in arrays)
    flat = [part for parts in arrays for part in parts]
    outs = [shape((1, share), F32)] * 2
    outs += [shape((p[0].shape[0], sum(x.shape[1] for x in p)), p[0].dtype) for p in arrays]
    n_copy = len(flat)
    return pl.pallas_call(
        functools.partial(finish_kernel, groups, share),
        out_shape=outs,
        in_specs=[vmem()] + [anywhere()] * n_copy,
        out_specs=[vmem()] * 2 + [anywhere()] * len(arrays),
        scratch_shapes=[pltpu.VMEM(x.shape, x.dtype) for x in flat]
        + [pltpu.SemaphoreType.DMA((n_copy, 2)), pltpu.SemaphoreType.DMA((n_copy, 2))],
        compiler_params=pltpu.CompilerParams(vmem_limit_bytes=VMEM_LIMIT),
        name="finish",
    )(gain_sums, *flat)


def body(
    n_dp,
    n_col,
    tokens,
    gain_attn,
    gain_ffn,
    w_query,
    w_key,
    w_value,
    w_out,
    w_gate,
    w_up,
    w_down,
    grad_output,
    segments,
    positions,
):
    tok, width = tokens.shape
    heads = w_query.shape[1] // 2
    gain_one, gain_two = gain_attn.reshape(1, width), gain_ffn.reshape(1, width)
    (
        q, k, v, h1, r1, cos_table, sin_table, seg_col, dy_end, dy_mid, wo_other, wg_other, wu_other, wd_other,
    ) = project(
        n_col, tokens, gain_one, positions, segments, grad_output,
        w_query, w_key, w_value, w_out, w_gate, w_up, w_down,
    )
    (
        heads_all, inv_sum, middle, dy_full,
        h2, units, grad_gate, grad_up, grad_middle, branch, gain_sum, down_one,
    ) = layer(
        n_col, n_dp, q, k, v, segments, seg_col, tokens, gain_two, w_out, grad_output, dy_end, dy_mid,
        w_gate, w_up, w_down, wg_other, wu_other, wd_other,
    )
    output, grad_heads, branch_half, *sums_one = branch_back(
        n_col, n_dp, branch, units, w_down, middle, dy_full, h2, grad_gate, w_out, wo_other, heads_all
    )
    grad_tokens, gain_sums, triple, *sums_two = attend_back(
        n_col, n_dp, q, k, v, grad_heads, segments, seg_col, inv_sum, cos_table, sin_table, tokens, r1,
        gain_one, grad_middle, gain_sum, h1, w_query, w_key, w_value, h2, grad_up,
    )
    if n_dp == 4:
        down_two, grad_wg, grad_wo = sums_one
        grad_wd = (down_one, down_two)
        grad_wu, *grad_qkv = sums_two
    else:

        def summed(left, right):
            grad = jnp.einsum("ta,tb->ab", left, right, preferred_element_type=F32).astype(BF16)
            return lax.psum_scatter(grad, "dp", scatter_dimension=0, tiled=True).astype(F32)

        row = lax.axis_index("row")
        dy_half = lax.dynamic_slice(dy_full, (0, row * n_col * width), (tok, n_col * width))
        grad_wd, grad_wg = (summed(units, dy_half),), summed(h2, grad_gate)
        grad_wu, grad_wo = summed(h2, grad_up), summed(heads_all, branch_half)
        parts = summed(h1, triple).reshape(-1, 2, 3, heads)
        grad_qkv = [parts[:, :, n].reshape(-1, 2 * heads) for n in range(3)]
    gain_a, gain_b, *results = finish(
        width // n_dp, gain_sums,
        [(m,) for m in (output, grad_tokens, *grad_qkv, grad_wo, grad_wg, grad_wu)] + [grad_wd],
    )
    blocks = [m.reshape((1, 1) + m.shape) for m in results[2:]]
    return (*results[:2], gain_a.reshape(1, 1, -1), gain_b.reshape(1, 1, -1), *blocks)


def solution(mesh):
    return jax.shard_map(
        functools.partial(body, mesh.shape["dp"], mesh.shape["col"]),
        mesh=mesh,
        in_specs=(
            P("dp", ("row", "col")),
            P(("row", "col")),
            P(("row", "col")),
            P("row", "col"),
            P("row", "col"),
            P("row", "col"),
            P("col", "row"),
            P("row", "col"),
            P("row", "col"),
            P("col", "row"),
            P("dp", ("row", "col")),
            P("dp", None),
            P("dp", None),
        ),
        out_specs=(
            P("dp", ("row", "col")),
            P("dp", ("row", "col")),
            P(("row", "col"), "dp", None),
            P(("row", "col"), "dp", None),
            P("row", "dp", None, "col"),
            P("row", "dp", None, "col"),
            P("row", "dp", None, "col"),
            P("col", "dp", None, "row"),
            P("row", "dp", None, "col"),
            P("row", "dp", None, "col"),
            P("col", "dp", None, "row"),
        ),
        check_vma=False,
    )
```

```python
import functools

import jax
import jax.numpy as jnp
import numpy as np
from jax import lax
from jax.experimental import pallas as pl
from jax.experimental.pallas import tpu as pltpu
from jax.sharding import PartitionSpec as P

MESH = pl.DeviceIdType.MESH
F32 = jnp.float32
BF16 = jnp.bfloat16
HD = 64
N_CHUNK = 4
norm_eps = 1e-05
rope_base = 130000.0
masked_score = -1e30
VMEM_LIMIT = 64 * 1024 * 1024 - 65536


def dot_nn(left, right):
    return lax.dot_general(left, right, (((1,), (0,)), ((), ())), preferred_element_type=F32)


def dot_nt(left, right):
    return lax.dot_general(left, right, (((1,), (1,)), ((), ())), preferred_element_type=F32)


def dot_tn(left, right):
    return lax.dot_general(left, right, (((0,), (0,)), ((), ())), preferred_element_type=F32)


def span(start, size):
    return pl.ds(pl.multiple_of(start, size), size)


def remote(src, dst, send_sem, recv_sem, where):
    return pltpu.make_async_remote_copy(
        src_ref=src,
        dst_ref=dst,
        send_sem=send_sem,
        recv_sem=recv_sem,
        device_id=where,
        device_id_type=MESH,
    )


def greet(peers):
    barrier = pltpu.get_barrier_semaphore()
    count = jnp.int32(0)
    for present, where in peers:

        @pl.when(present)
        def _():
            pl.semaphore_signal(barrier, inc=1, device_id=where, device_id_type=MESH)

        count = count + present.astype(jnp.int32)
    pl.semaphore_wait(barrier, count)


def line_peers(r, c, n_col):
    always = c >= 0
    return [
        (c > 0, {"col": jnp.maximum(c - 1, 0)}),
        (c < n_col - 1, {"col": jnp.minimum(c + 1, n_col - 1)}),
        (always, {"row": 1 - r}),
    ]


def group_peers(r, c, n_col):
    return [
        ((c != at) | (r != half), {"row": jnp.int32(half), "col": jnp.int32(at)})
        for half in range(2)
        for at in range(n_col)
    ]


class Gather:
    def __init__(self, full, send, recv, r, c, n_col, width, n_chunk=N_CHUNK):
        self.full, self.send, self.recv = full, send, recv
        self.r, self.c, self.n_col, self.width = r, c, n_col, width
        self.n_chunk = n_chunk

    def piece(self, half, at, chunk):
        cols = span(half * (self.n_col * self.width) + at * self.width, self.width)
        return self.full.at[chunk, :, cols]

    def copy(self, way, at, chunk):
        piece = self.piece(self.r, at, chunk)
        where = (
            {"col": jnp.maximum(self.c - 1, 0)},
            {"col": jnp.minimum(self.c + 1, self.n_col - 1)},
            {"row": 1 - self.r},
        )[way]
        return remote(
            piece, piece, self.send.at[way, at, chunk], self.recv.at[self.r, at, chunk], where
        )

    def wait(self, half, at, chunk):
        piece = self.piece(half, at, chunk)
        remote(
            piece, piece, self.send.at[0, at, chunk], self.recv.at[half, at, chunk], {"row": 1 - self.r}
        ).wait_recv()

    def start(self, chunk):
        c = self.c

        @pl.when(c > 0)
        def _():
            self.copy(0, c, chunk).start()

        @pl.when(c < self.n_col - 1)
        def _():
            self.copy(1, c, chunk).start()

        self.copy(2, c, chunk).start()

    def relay(self, distance, chunk):
        c, last = self.c, self.n_col - 1

        @pl.when(c + distance <= last)
        def _():
            at = c + distance
            self.wait(self.r, at, chunk)

            @pl.when(c > 0)
            def _():
                self.copy(0, at, chunk).start()

            self.copy(2, at, chunk).start()

        @pl.when(c - distance >= 0)
        def _():
            at = c - distance
            self.wait(self.r, at, chunk)

            @pl.when(c < last)
            def _():
                self.copy(1, at, chunk).start()

            self.copy(2, at, chunk).start()

    def toward(self, way, at, chunk):
        piece = self.piece(self.r, at, chunk)
        where = {"col": jnp.clip(self.c - 1 + 2 * way, 0, self.n_col - 1)}
        return remote(piece, piece, self.send.at[way, at, chunk], self.recv.at[self.r, at, chunk], where)

    def hand(self, at, chunk, way=None):
        self.wait(self.r, at, chunk)
        if way is not None:
            self.toward(way, at, chunk).start()
        self.copy(2, at, chunk).start()

    def end_relay(self, distance, chunk):
        self.hand(jnp.where(self.c == 0, distance, 3 - distance), chunk)

    def middle_relay(self, kind, chunk):
        outward = (self.c == 2).astype(jnp.int32)
        near_end = 3 * outward
        at = {"a": 3 - self.c, "b": near_end, "c": 3 - near_end}[kind]
        self.hand(at, chunk, 1 - outward if kind == "b" else outward)

    def tick(self, now):
        for distance in range(self.n_col - 1, 0, -1):
            chunk = now + 1 - distance

            @pl.when((chunk >= 0) & (chunk < self.n_chunk))
            def _():
                self.relay(distance, chunk)

    def wait_other(self, chunk):
        def one(at, carry):
            self.wait(1 - self.r, at, chunk)
            return carry

        lax.fori_loop(0, self.n_col, one, 0)

    def finish(self):
        c, last = self.c, self.n_col - 1

        def one(step, carry):
            at, chunk = step // self.n_chunk, step % self.n_chunk

            @pl.when((c > 0) & (at >= c))
            def _():
                self.copy(0, at, chunk).wait_send()

            @pl.when((c < last) & (at <= c))
            def _():
                self.copy(1, at, chunk).wait_send()

            self.copy(2, at, chunk).wait_send()
            return carry

        lax.fori_loop(0, self.n_col * self.n_chunk, one, 0)


class Scatter:
    def __init__(self, part, stage, inbox, send, recv, c, n_col, n_chunk=N_CHUNK):
        self.part, self.stage, self.inbox = part, stage, inbox
        self.send, self.recv, self.c, self.n_col = send, recv, c, n_col
        self.n_chunk = n_chunk
        self.width = stage.shape[-1]
        self.middle = (c > 0) & (c < n_col - 1)

    def term(self, chunk, dest):
        return self.part[chunk, :, span(dest * self.width, self.width)]

    def staged(self, dest):
        return dest - (dest > self.c).astype(jnp.int32)

    def slot(self, way, dest, at):
        inner = ((at == 1) & (way == 1)) | ((at == 2) & (way == 0))
        return jnp.where((dest == at) & inner, 4, dest)

    def copy(self, way, chunk, dest):
        where = jnp.clip(self.c + 1 - 2 * way, 0, self.n_col - 1)
        slot = self.slot(way, dest, where)
        return remote(
            self.stage.at[chunk, self.staged(dest)],
            self.inbox.at[chunk, slot],
            self.send.at[chunk, dest],
            self.recv.at[chunk, slot],
            {"col": where},
        )

    def arrival(self, way, chunk, dest):
        slot = self.slot(way, dest, self.c)
        here = self.inbox.at[chunk, slot]
        remote(here, here, self.send.at[chunk, dest], self.recv.at[chunk, slot], {"col": self.c}).wait_recv()
        return self.inbox[chunk, slot].astype(F32)

    def open(self, chunk):
        @pl.when(jnp.logical_not(self.middle))
        def _():
            way = (self.c > 0).astype(jnp.int32)

            def ship(step, carry):
                dest = jnp.where(way == 0, self.n_col - 1 - step, step)
                self.stage[chunk, self.staged(dest)] = self.term(chunk, dest).astype(BF16)
                self.copy(way, chunk, dest).start()
                return carry

            lax.fori_loop(0, self.n_col - 1, ship, 0)

    def pass_on(self, way, chunk, dest):
        total = self.term(chunk, dest) + self.arrival(way, chunk, dest)
        self.stage[chunk, self.staged(dest)] = total.astype(BF16)
        self.copy(way, chunk, dest).start()

    def near(self, chunk):
        @pl.when(self.middle)
        def _():
            way = (self.c > 1).astype(jnp.int32)

            def step_on(step, carry):
                self.pass_on(way, chunk, jnp.where(way == 0, self.n_col - 1 - step, step))
                return carry

            lax.fori_loop(0, 2, step_on, 0)

    def far(self, chunk):
        @pl.when(self.middle)
        def _():
            way = (self.c == 1).astype(jnp.int32)
            self.pass_on(way, chunk, jnp.where(self.c == 1, 0, self.n_col - 1))

    def total(self, chunk, out, at):
        c = self.c
        way = (c == 0).astype(jnp.int32)
        out[at, :] = self.term(chunk, c) + self.arrival(way, chunk, c)

        @pl.when(self.middle)
        def _():
            out[at, :] += self.arrival(1, chunk, c)

    def finish(self):
        def one(step, carry):
            chunk, dest = step // self.n_col, step % self.n_col

            @pl.when(dest != self.c)
            def _():
                self.copy(0, chunk, dest).wait_send()

            return carry

        lax.fori_loop(0, self.n_chunk * self.n_col, one, 0)

    @staticmethod
    def scratch(n_col, rows, width, n_chunk=N_CHUNK):
        return [
            pltpu.VMEM((n_chunk, rows, n_col * width), F32),
            pltpu.VMEM((n_chunk, n_col - 1, rows, width), BF16),
            pltpu.VMEM((n_chunk, n_col + 1, rows, width), BF16),
            pltpu.SemaphoreType.DMA((n_chunk, n_col)),
            pltpu.SemaphoreType.DMA((n_chunk, n_col + 1)),
        ]


def gather_sems(n_col, n_chunk=N_CHUNK):
    return [
        pltpu.SemaphoreType.DMA((3, n_col, n_chunk)),
        pltpu.SemaphoreType.DMA((2, n_col, n_chunk)),
    ]


N_NOTE = 16


def put_notes(full, chunk, cols, values):
    rows = full.shape[1] - N_NOTE
    width = values[0].shape[1]
    at = lax.broadcasted_iota(jnp.int32, (N_NOTE, width), 0)
    notes = jnp.zeros((N_NOTE, width), F32)
    for n, value in enumerate(values):
        for piece in range(3):
            rounded = value.astype(BF16).astype(F32)
            notes = jnp.where(at == 3 * n + piece, rounded, notes)
            value = value - rounded
    full[chunk, rows:, cols] = notes.astype(BF16)


def get_note(full, chunk, cols, n):
    rows = full.shape[1] - N_NOTE
    notes = full[chunk, rows:, cols].astype(F32)
    return (notes[3 * n : 3 * n + 1, :] + notes[3 * n + 1 : 3 * n + 2, :]) + notes[3 * n + 2 : 3 * n + 3, :]


def as_row(column):
    return jnp.broadcast_to(column, (column.shape[0], 128)).T[0:1, :]


def as_column(row):
    return jnp.broadcast_to(row, (128, row.shape[1])).T[:, 0:1]


class Totals:
    def __init__(self, held, sent, inbox, send, recv, r, c):
        self.held, self.sent, self.inbox, self.send, self.recv = held, sent, inbox, send, recv
        self.partners = ({"row": 1 - r}, {"col": c + 1 - 2 * (c % 2)}, {"col": c + 2 - 4 * (c // 2)})

    def note(self, chunk, column):
        self.held[pl.ds(chunk, 1), :] = as_row(column)

    def copy(self, step):
        return remote(
            self.sent.at[step], self.inbox.at[step], self.send.at[step], self.recv.at[step], self.partners[step]
        )

    def step(self, n):
        if n > 0:
            self.copy(n - 1).wait_recv()
            self.held[...] += self.inbox[n - 1]
        if n < 3:
            self.sent[n] = self.held[...]
            self.copy(n).start()

    def exchange(self):
        for n in range(4):
            self.step(n)

    def column(self, chunk):
        return as_column(self.held[pl.ds(chunk, 1), :])

    def finish(self):
        for step in range(3):
            self.copy(step).wait_send()

    @staticmethod
    def scratch(rows):
        return [
            pltpu.VMEM((8, rows), F32),
            pltpu.VMEM((3, 8, rows), F32),
            pltpu.VMEM((3, 8, rows), F32),
            pltpu.SemaphoreType.DMA((3,)),
            pltpu.SemaphoreType.DMA((3,)),
        ]


def lanes(shape):
    return lax.broadcasted_iota(jnp.int32, shape, len(shape) - 1)


def swap_halves(values):
    half, width = HD // 2, values.shape[-1]
    low = (lanes(values.shape) & (HD - 1)) < half
    return jnp.where(
        low, pltpu.roll(values, width - half, 1), pltpu.roll(values, half, 1)
    )


def widen(table, width):
    return jnp.concatenate([table] * (width // table.shape[-1]), axis=-1)


class Flush:
    def __init__(self, pairs, sems, rows):
        self.pairs, self.sems, self.rows = pairs, sems, rows

    def copy(self, n, chunk):
        source, target = self.pairs[n]
        at = span(chunk * self.rows, self.rows)
        if isinstance(source, tuple):
            source = source[0].at[chunk, 0 : self.rows, source[1]]
        else:
            source = source.at[at, :]
        return pltpu.make_async_copy(source, target.at[at, :], self.sems.at[n, chunk])

    def start(self, chunk, which=None):
        for n in range(len(self.pairs)) if which is None else which:
            self.copy(n, chunk).start()

    def finish(self):
        def one(chunk, carry):
            for n in range(len(self.pairs)):
                self.copy(n, chunk).wait()
            return carry

        lax.fori_loop(0, N_CHUNK, one, 0)


def fetches(pairs, sems):
    copies = [pltpu.make_async_copy(source, target, sems.at[n]) for n, (source, target) in enumerate(pairs)]
    for copy in copies:
        copy.start()
    return copies


def vmem():
    return pl.BlockSpec(memory_space=pltpu.VMEM)


def anywhere():
    return pl.BlockSpec(memory_space=pl.ANY)


def kernel_call(body, name, ident, outs, out_any, in_specs, scratch, flops):
    return pl.pallas_call(
        body,
        out_shape=outs,
        in_specs=in_specs,
        out_specs=[anywhere() if flag else vmem() for flag in out_any],
        scratch_shapes=scratch,
        compiler_params=pltpu.CompilerParams(
            collective_id=ident, has_side_effects=True, vmem_limit_bytes=VMEM_LIMIT
        ),
        cost_estimate=pl.CostEstimate(flops=flops, bytes_accessed=1 << 24, transcendentals=0),
        name=name,
    )


def project_kernel(
    n_col,
    x, gain, positions, segments, rope, dy, wq, wk, wv, wo, wg, wu, wd,
    q_out, k_out, v_out, h1_out, r1, cos_table, sin_table, seg_col, dy_end, dy_mid,
    wo_other, wg_other, wu_other, wd_other,
    full, hidden, weights, q, k, v, h1, ag_send, ag_recv,
    w_send, w_recv, d_send, d_recv, local, flushed,
):
    r, c = lax.axis_index("row"), lax.axis_index("col")
    tok, width = x.shape
    half = n_col * width
    heads = wq.shape[1] // 2
    units = wg.shape[1] // 2
    me = r * n_col + c
    rows = tok // N_CHUNK
    held = fetches(
        [
            (
                w.at[:, span(r * heads, heads)],
                weights.at[span(r * half, half), pl.ds(n * heads, heads)],
            )
            for n, w in enumerate((wq, wk, wv))
        ],
        local,
    )
    mine = span(me * width, width)

    def prepare(chunk, carry):
        values = x[span(chunk * rows, rows), :]
        full[chunk, 0:rows, mine] = values
        values = values.astype(F32)
        square = as_row(jnp.sum(values * values, axis=1, keepdims=True))
        put_notes(full, chunk, mine, (square, gain[...]))
        return carry

    lax.fori_loop(0, N_CHUNK, prepare, 0)
    greet(group_peers(r, c, n_col))
    gather = Gather(full, ag_send, ag_recv, r, c, n_col, width)
    flush = Flush(((q, q_out), (k, k_out), (v, v_out), (h1, h1_out)), flushed, rows)

    def chunk_rows(chunk):
        return span(chunk * rows, rows)

    gather.start(0)
    gather.start(1)
    other = {"row": 1 - r}
    moved = [
        remote(
            w.at[:, span((1 - r) * heads, heads)],
            weights.at[span(r * half, half), pl.ds(n * heads, heads)],
            w_send.at[n], w_recv.at[n], other,
        )
        for n, w in enumerate((wq, wk, wv))
    ]
    moved.append(remote(wo.at[span((1 - r) * heads, heads), :], wo_other, w_send.at[3], w_recv.at[3], other))
    moved.append(remote(wg.at[:, span((1 - r) * units, units)], wg_other, w_send.at[4], w_recv.at[4], other))
    moved.append(remote(wu.at[:, span((1 - r) * units, units)], wu_other, w_send.at[5], w_recv.at[5], other))
    moved.append(remote(wd.at[span((1 - r) * units, units), :], wd_other, w_send.at[6], w_recv.at[6], other))
    inward = {"col": jnp.where(c == 0, 1, jnp.where(c == 1, 2, jnp.where(c == 2, 1, 2)))}
    at_end = (c == 0) | (c == 3)
    early_end = remote(dy, dy_end, d_send.at[0], d_recv.at[0], inward)
    early_mid = remote(dy, dy_mid, d_send.at[0], d_recv.at[1], inward)

    for copy in moved[:3]:
        copy.start()
    gather.tick(0)
    gather.start(2)
    for copy in moved[3:]:
        copy.start()

    def tables(chunk, carry):
        at = chunk_rows(chunk)
        place = jnp.broadcast_to(positions[:, at].astype(F32), (128, rows)).T
        angles = place * rope[0:1, :]
        cos_table[at, :] = jnp.cos(angles)
        sin_table[at, :] = jnp.sin(angles) * rope[1:2, :]
        seg_col[at, :] = jnp.broadcast_to(segments[:, at].astype(F32), (128, rows)).T
        return carry

    lax.fori_loop(0, N_CHUNK, tables, 0)
    gather.tick(1)
    gather.start(3)
    pl.when(at_end)(early_end.start)
    gather.tick(2)

    def compute(chunk):
        at = chunk_rows(chunk)
        square = jnp.zeros((1, rows), F32)
        for block in range(2 * n_col):
            square = square + get_note(full, chunk, pl.ds(block * width, width), 0)
        scale = lax.rsqrt(as_column(square) * (1.0 / (2 * half)) + norm_eps)
        r1[at, :] = jnp.broadcast_to(scale, (rows, r1.shape[1]))
        for block in range(2 * n_col):
            cols = pl.ds(block * width, width)
            values = full[chunk, 0:rows, cols].astype(F32)
            hidden[:, cols] = (values * scale * get_note(full, chunk, cols, 1)).astype(BF16)
        h1[at, :] = hidden[:, span(r * half, half)]
        values = dot_nn(hidden[...], weights[...])
        cos_rows = widen(cos_table[at, :], heads)
        sin_rows = widen(sin_table[at, :], heads)
        for n, out in enumerate((q, k)):
            part = values[:, n * heads : (n + 1) * heads]
            out[at, :] = (part * cos_rows + swap_halves(part) * sin_rows).astype(BF16)
        v[at, :] = values[:, 2 * heads :].astype(BF16)
        flush.start(chunk)

    for copy in held:
        copy.wait()
    for copy in moved[:3]:
        copy.wait_recv()

    def step(chunk, carry):
        gather.wait_other(chunk)
        compute(chunk)
        gather.tick(chunk + 3)
        pl.when((chunk == 0) & jnp.logical_not(at_end))(early_mid.start)
        return carry

    lax.fori_loop(0, N_CHUNK, step, 0)
    gather.finish()
    for copy in moved[3:]:
        copy.wait_recv()
    for copy in moved:
        copy.wait_send()
    early_end.wait_send()

    @pl.when(jnp.logical_not(at_end))
    def _():
        early_end.wait_recv()
        early_mid.wait_recv()

    flush.finish()


def project(n_col, x, gain, positions, segments, dy, wq, wk, wv, wo, wg, wu, wd):
    tok, width = x.shape
    full = 2 * n_col * width
    half = n_col * width
    heads, units = wq.shape[1] // 2, wg.shape[1] // 2
    lane = np.arange(128) % HD
    inv_freq = rope_base ** (-2.0 * (lane % (HD // 2)) / HD)
    rope = jnp.asarray(np.stack([inv_freq, np.where(lane < HD // 2, -1.0, 1.0)]), F32)
    shape = jax.ShapeDtypeStruct
    outs = [
        shape((tok, heads), BF16), shape((tok, heads), BF16), shape((tok, heads), BF16),
        shape((tok, half), BF16), shape((tok, 128), F32),
        shape((tok, 128), F32), shape((tok, 128), F32), shape((tok, 128), F32),
        shape((tok, width), BF16), shape((tok, width), BF16),
        shape((heads, wo.shape[1]), BF16), shape((half, units), BF16),
        shape((half, units), BF16), shape((units, wd.shape[1]), BF16),
    ]
    scratch = [
        pltpu.VMEM((N_CHUNK, tok // N_CHUNK + N_NOTE, full), BF16),
        pltpu.VMEM((tok // N_CHUNK, full), BF16),
        pltpu.VMEM((full, 3 * heads), BF16),
        *[pltpu.VMEM((tok, heads), BF16)] * 3,
        pltpu.VMEM((tok, half), BF16),
        *gather_sems(n_col),
        pltpu.SemaphoreType.DMA((7,)),
        pltpu.SemaphoreType.DMA((7,)),
        pltpu.SemaphoreType.DMA((1,)),
        pltpu.SemaphoreType.DMA((2,)),
        pltpu.SemaphoreType.DMA((3,)),
        pltpu.SemaphoreType.DMA((4, N_CHUNK)),
    ]
    return kernel_call(
        functools.partial(project_kernel, n_col), "project", 1, outs,
        [True] * 4 + [False] * 4 + [True] * 6,
        [vmem()] * 5 + [anywhere()] * 8, scratch, 6 * tok * full * heads,
    )(x, gain, positions, segments, rope, dy, wq, wk, wv, wo, wg, wu, wd)


def allowed_pairs(seg_col, seg_row, chunk, rows, keys):
    seg_row = seg_row.astype(F32)
    query_at = chunk * rows + lax.broadcasted_iota(jnp.int32, (rows, keys), 0)
    key_at = lanes((rows, keys))
    return (key_at <= query_at) & (seg_col[:, 0:1] == seg_row)


def of_head(values, head):
    return jnp.where((lanes(values.shape) // HD) == head, values, jnp.zeros_like(values))


class LateGather:
    def __init__(self, full, send, recv, r, c, n_col, width):
        self.inner = Gather(full, send, recv, r, c, n_col, width)
        self.c = c
        self.end = (c == 0) | (c == 3)
        self.near_end = jnp.where(c < 2, 0, 3)
        self.far_end = 3 - self.near_end
        self.other = 3 - c
        self.outward = (c >= 2).astype(jnp.int32)

    def copy(self, way, at, chunk):
        piece = self.inner.piece(self.inner.r, at, chunk)
        where = ({"col": self.near_end}, {"col": self.other}, {"row": 1 - self.inner.r})[way]
        return remote(
            piece, piece, self.inner.send.at[way, at, chunk], self.inner.recv.at[self.inner.r, at, chunk], where
        )

    def start(self, chunk):
        c = self.c
        self.copy(2, c, chunk).start()

        @pl.when(jnp.logical_not(self.end))
        def _():
            self.copy(0, c, chunk).start()
            self.copy(1, self.near_end, chunk).start()
            self.copy(0, self.other, chunk).start()
            self.copy(2, self.near_end, chunk).start()
            self.copy(2, self.other, chunk).start()

    def relay(self, chunk):
        @pl.when(jnp.logical_not(self.end))
        def _():
            self.inner.wait(self.inner.r, self.far_end, chunk)
            self.copy(0, self.far_end, chunk).start()
            self.copy(2, self.far_end, chunk).start()

    def collect(self, chunk):
        @pl.when(self.end)
        def _():
            for step in range(3):
                at = jnp.where(self.c == 0, 1 + step, 2 - step)
                self.inner.wait(self.inner.r, at, chunk)
                self.copy(2, at, chunk).start()

    def finish(self):
        def one(step, carry):
            at, chunk = step // 4, step % 4
            self.copy(2, at, chunk).wait_send()

            @pl.when(jnp.logical_not(self.end))
            def _():
                pl.when(at != self.near_end)(lambda: self.copy(0, at, chunk).wait_send())
                pl.when(at == self.near_end)(lambda: self.copy(1, at, chunk).wait_send())

            return carry

        lax.fori_loop(0, 4 * N_CHUNK, one, 0)


def layer_kernel(
    n_col, n_sum,
    q_in, k_in, v_in, seg_row, seg_col_in, x_in, gain, wo, dy, dy_end, dy_mid,
    wg, wu, wd, wg_other, wu_other, wd_other,
    heads_out, inv_sum, middle_out, dy_out,
    h2_out, units_out, gate_out, up_out, two_out, scale_out, gain_sum, held, sum_out,
    q, k, v, seg_col, x, heads_all, middle, dy_full, w_out,
    units, grad_gate, grad_up, grad_two,
    full, gate_own, up_own, down_own, gate_far, up_far,
    part, stage_z, inbox_z, z_send, z_recv, stage_f, inbox_f, f_send, f_recv,
    dy_send, dy_recv, ag_send, ag_recv,
    h_send, h_recv, x_send, x_recv, local, flushed, *refs,
):
    r, c = lax.axis_index("row"), lax.axis_index("col")
    tok, heads = q.shape
    width = x.shape[1]
    half = n_col * width
    n_unit = down_own.shape[0]
    rows = tok // N_CHUNK
    me = r * n_col + c
    row_base = r * n_col
    sums = refs[0:1]
    mine, far = span(r * n_unit, n_unit), span((1 - r) * n_unit, n_unit)
    near_rows, far_rows = span(r * half, half), span((1 - r) * half, half)
    block = span(me * width, width)
    everything = pl.ds(0, dy_full.shape[2])

    def chunk_rows(chunk):
        return span(chunk * rows, rows)

    scale_wide = seg_col
    late = LateGather(dy_full, dy_send, dy_recv, r, c, n_col, width)
    gather = Gather(full, ag_send, ag_recv, r, c, n_col, width)
    scatter_z = Scatter(part, stage_z, inbox_z, z_send, z_recv, c, n_col)
    scatter_f = Scatter(part, stage_f, inbox_f, f_send, f_recv, c, n_col)
    flush = Flush(
        (
            ((full, near_rows), h2_out), (grad_gate, gate_out), (grad_up, up_out), (units, units_out),
            (grad_two, two_out), (scale_wide, scale_out),
            (heads_all, heads_out), (middle, middle_out), ((dy_full, everything), dy_out),
        ),
        flushed, rows,
    )
    panels = []
    if n_sum:

        def tile(owner, side):
            cols = half // 4
            n_row = sums[0].shape[0]
            right = dy_full[:, :, span(r * half + side * cols, cols)].reshape(tok, cols)
            return dot_tn(units[:, span(owner * n_row, n_row)], right)

        panels.append(Reduce(tile, sums, *refs[1:]))

    def block_load(source, at):
        return source.reshape(N_CHUNK, rows, width), dy_full.at[:, :, span(at * width, width)]

    own, *first = fetches(
        [block_load(dy, me), (q_in, q), (k_in, k), (v_in, v), (seg_col_in, seg_col), (wo, w_out), (x_in, x)],
        local,
    )
    early = [
        pltpu.make_async_copy(*block_load(dy_end, row_base + late.near_end), local.at[7]),
        pltpu.make_async_copy(*block_load(dy_mid, row_base + late.other), local.at[8]),
    ]

    @pl.when(jnp.logical_not(late.end))
    def _():
        for copy in early:
            copy.start()

    greet(line_peers(r, c, n_col) + (square_peers() if n_sum else []))
    loads = fetches(
        [
            (wg.at[:, mine], gate_own.at[near_rows, :]),
            (wg_other, gate_own.at[far_rows, :]),
            (wu.at[:, mine], up_own.at[near_rows, :]),
            (wu_other, up_own.at[far_rows, :]),
            (wd.at[mine, :], down_own.at[:, near_rows]),
            (wd_other, down_own.at[:, far_rows]),
            (wg.at[:, far], gate_far),
            (wu.at[:, far], up_far),
        ],
        local.at[pl.ds(9, 8)],
    )
    own.wait()

    @pl.when(jnp.logical_not(late.end))
    def _():
        for copy in early:
            copy.wait()


    def heads_copy(chunk):
        piece = heads_all.at[pl.ds(chunk * rows, rows), span(r * heads, heads)]
        return remote(piece, piece, h_send.at[chunk], h_recv.at[chunk], {"row": 1 - r})

    def attend(chunk):
        at = pl.ds(chunk * rows, rows)
        keys = (chunk + 1) * rows
        allowed = allowed_pairs(seg_col[at, :], seg_row[:, 0:keys], chunk, rows, keys)

        def head_step(head, carry):
            total, inverse = carry
            scores = dot_nt(of_head(q[at, :], head), k[0:keys, :]) * HD**-0.5
            weights = jnp.exp(jnp.where(allowed, scores, masked_score))
            inv = 1.0 / jnp.sum(weights, axis=1, keepdims=True)
            probs = (weights * inv).astype(BF16)
            total = total + dot_nn(probs, of_head(v[0:keys, :], head))
            inverse = jnp.where(lanes((rows, 128)) == head, inv, inverse)
            return total, inverse

        total, inverse = lax.fori_loop(
            0, heads // HD, head_step, (jnp.zeros((rows, heads), F32), jnp.zeros((rows, 128), F32))
        )
        heads_all[at, span(r * heads, heads)] = total.astype(BF16)
        inv_sum[at, :] = inverse
        heads_copy(chunk).start()

    def contract(chunk):
        heads_copy(chunk).wait_recv()
        flush.start(chunk, (6,))
        part[chunk] = dot_nn(heads_all[span(chunk * rows, rows), :], w_out[...])
        scatter_z.open(chunk)

    def settle_z(chunk):
        at = chunk_rows(chunk)
        scatter_z.total(chunk, middle, at)
        values = middle[at, :] + x[at, :].astype(F32)
        middle[at, :] = values
        full[chunk, 0:rows, block] = (values * gain[...]).astype(BF16)
        put_notes(full, chunk, block, (as_row(jnp.sum(values * values, axis=1, keepdims=True)),))
        gather.start(chunk)
        flush.start(chunk, (7,))

    def exchange(n, chunk):
        piece = (grad_gate, grad_up, units)[n].at[chunk_rows(chunk), mine]
        return remote(piece, piece, x_send.at[n, chunk], x_recv.at[n, chunk], {"row": 1 - r})

    def norm(chunk):
        square = jnp.zeros((1, rows), F32)
        for at in range(2 * n_col):
            square = square + get_note(full, chunk, pl.ds(at * width, width), 0)
        scale = lax.rsqrt(as_column(square) * (1.0 / (2 * half)) + norm_eps)
        scale_wide[chunk_rows(chunk), :] = jnp.broadcast_to(scale, (rows, scale_wide.shape[1]))

    size = n_unit // 2

    def units_part(chunk, step):
        at = chunk_rows(chunk)
        scale = scale_wide[at, 0:1]
        cols = span(step * size, size)
        gate = dot_nn(full[chunk, 0:rows, :], gate_own[:, cols]) * scale
        up = dot_nn(full[chunk, 0:rows, :], up_own[:, cols]) * scale
        grad = dot_nt(dy_full[chunk], down_own[cols, :])
        sig = jax.nn.sigmoid(gate)
        act = gate * sig
        put = span(r * n_unit + step * size, size)
        units[at, put] = (act * up).astype(BF16)
        grad = grad * scale
        grad_gate[at, put] = (grad * up * sig * (1.0 + gate * (1.0 - sig))).astype(BF16)
        grad_up[at, put] = (grad * act).astype(BF16)

    def back(chunk):
        at = chunk_rows(chunk)
        part[chunk] = dot_nt(grad_gate[at, mine], gate_own[near_rows, :]) + dot_nt(
            grad_up[at, mine], up_own[near_rows, :]
        )
        for n in range(2):
            exchange(n, chunk).wait_recv()
        part[chunk] += dot_nt(grad_gate[at, far], gate_far[...]) + dot_nt(grad_up[at, far], up_far[...])
        scatter_f.open(chunk)
        exchange(2, chunk).wait_recv()
        flush.start(chunk, (0, 1, 2, 3, 5, 8))

    def settle_f(chunk):
        at = chunk_rows(chunk)
        scatter_f.total(chunk, grad_two, at)
        product = grad_two[at, :] * middle[at, :]
        held[pl.ds(chunk, 1), :] = as_row(jnp.sum(product * gain[...], axis=1, keepdims=True))
        gain_sum[...] += jnp.sum(product.reshape(rows // 8, 8, width), axis=0)
        flush.start(chunk, (4,))

    middle_role = scatter_z.middle

    def at_end(*acts):
        @pl.when(jnp.logical_not(middle_role))
        def _():
            for act, *what in acts:
                act(*what)

    def at_middle(*acts):
        @pl.when(middle_role)
        def _():
            for act, *what in acts:
                act(*what)

    near, far_sum = scatter_z.near, scatter_z.far
    near_f, far_f = scatter_f.near, scatter_f.far
    end_relay, middle_relay = gather.end_relay, gather.middle_relay
    gain_sum[...] = jnp.zeros_like(gain_sum)
    held[...] = jnp.zeros_like(held)
    at_end(*[(late.start, chunk) for chunk in range(N_CHUNK)])
    at_middle((late.start, 0), (late.start, 1), (late.start, 2))
    for copy in first:
        copy.wait()
    at_middle((late.relay, 0), (late.start, 3))
    attend(0)
    contract(0)
    at_middle((near, 0))
    attend(1)
    attend(2)
    at_middle((far_sum, 0))
    contract(1)
    at_middle((near, 1), (far_sum, 1))
    contract(2)
    at_middle((near, 2), (far_sum, 2))

    def settle_first(chunk, carry):
        settle_z(chunk)
        return carry

    lax.fori_loop(0, 2, settle_first, 0)
    attend(3)
    at_middle((middle_relay, "b", 0))
    at_end((late.collect, 0))
    at_middle((middle_relay, "a", 0), (middle_relay, "b", 1), (middle_relay, "c", 0))
    settle_z(2)
    at_middle((late.relay, 1), (middle_relay, "c", 1), (middle_relay, "a", 1), (middle_relay, "a", 2))
    at_end((end_relay, 1, 0))
    contract(3)
    at_middle((near, 3), (middle_relay, "b", 2))
    at_end((end_relay, 3, 0), (end_relay, 2, 0))
    for copy in loads:
        copy.wait()

    def step(now, carry):
        late.inner.wait_other(now)
        gather.wait_other(now)
        norm(now)

        def part_step(n, carry):
            units_part(now, n)
            return carry

        lax.fori_loop(0, 2, part_step, 0)
        for n in range(3):
            exchange(n, now).start()
        pl.when(now == 1)(lambda: at_middle((near_f, 0), (middle_relay, "a", 3)))
        pl.when(now == 3)(lambda: at_middle((far_f, 1), (near_f, 2), (far_f, 2)))
        back(now)

        @pl.when(now == 0)
        def _():
            at_end((end_relay, 2, 1), (end_relay, 1, 1))
            at_middle((far_sum, 3))
            settle_z(3)
            at_middle((middle_relay, "c", 2), (late.relay, 2))
            at_end((end_relay, 3, 1), (late.collect, 1))

        @pl.when(now == 1)
        def _():
            at_middle((middle_relay, "b", 3), (late.relay, 3))
            at_end((end_relay, 1, 2), (end_relay, 2, 2), (end_relay, 2, 3), (end_relay, 3, 2), (late.collect, 2))

        @pl.when(now == 2)
        def _():
            at_middle((middle_relay, "c", 3), (far_f, 0), (near_f, 1))
            at_end((end_relay, 3, 3), (end_relay, 1, 3), (late.collect, 3))

        return carry

    lax.fori_loop(0, N_CHUNK, step, 0)
    for panel in panels:
        panel.first()
    at_middle((near_f, 3), (far_f, 3))
    for panel in panels:
        panel.second()

    def drain(now, carry):
        settle_f(now)
        return carry

    lax.fori_loop(0, N_CHUNK, drain, 0)
    gather.finish()
    late.finish()
    scatter_z.finish()
    scatter_f.finish()
    stores = []
    for panel in panels:
        panel.merge()
        panel.last()
        stores += fetches([(sums[0], sum_out)], local.at[pl.ds(17, 1)])
        panel.finish()

    def close(chunk, carry):
        heads_copy(chunk).wait_send()
        for n in range(3):
            exchange(n, chunk).wait_send()
        return carry

    lax.fori_loop(0, N_CHUNK, close, 0)
    for copy in stores:
        copy.wait()
    flush.finish()


def layer(
    n_col, n_dp, q, k, v, seg_row, seg_col, x, gain, wo, dy, dy_end, dy_mid,
    wg, wu, wd, wg_other, wu_other, wd_other,
):
    tok, heads = q.shape
    width = x.shape[1]
    half, n_unit = n_col * width, wg.shape[1] // 2
    rows = tok // N_CHUNK
    shape = jax.ShapeDtypeStruct
    n_sum = int(n_dp == 4)
    size = (wd.shape[0] // 4, half // 2) if n_sum else (8, 128)
    outs = [
        shape((tok, 2 * heads), BF16), shape((tok, 128), F32), shape((tok, width), F32),
        shape((tok, 2 * half), BF16), shape((tok, half), BF16),
        shape((tok, 2 * n_unit), BF16), shape((tok, 2 * n_unit), BF16), shape((tok, 2 * n_unit), BF16),
        shape((tok, width), F32), shape((tok, 128), F32), shape((8, width), F32), shape((8, rows), F32),
        shape(size, F32),
    ]
    scatter = Scatter.scratch(n_col, rows, width)
    scratch = [
        *[pltpu.VMEM(array.shape, array.dtype) for array in (q, k, v, seg_col, x)],
        pltpu.VMEM((tok, 2 * heads), BF16),
        pltpu.VMEM((tok, width), F32),
        pltpu.VMEM((N_CHUNK, rows, 2 * half), BF16),
        pltpu.VMEM(wo.shape, BF16),
        *[pltpu.VMEM((tok, 2 * n_unit), BF16)] * 3,
        pltpu.VMEM((tok, width), F32),
        pltpu.VMEM((N_CHUNK, rows + N_NOTE, 2 * half), BF16),
        pltpu.VMEM((2 * half, n_unit), BF16),
        pltpu.VMEM((2 * half, n_unit), BF16),
        pltpu.VMEM((n_unit, 2 * half), BF16),
        pltpu.VMEM((half, n_unit), BF16),
        pltpu.VMEM((half, n_unit), BF16),
        *scatter,
        *scatter[1:],
        *gather_sems(n_col),
        *gather_sems(n_col),
        pltpu.SemaphoreType.DMA((N_CHUNK,)),
        pltpu.SemaphoreType.DMA((N_CHUNK,)),
        pltpu.SemaphoreType.DMA((3, N_CHUNK)),
        pltpu.SemaphoreType.DMA((3, N_CHUNK)),
        pltpu.SemaphoreType.DMA((18,)),
        pltpu.SemaphoreType.DMA((9, N_CHUNK)),
    ]
    if n_sum:
        scratch += [pltpu.VMEM(size, F32), *Reduce.scratch(size[0], size[1] // 2)]
    return kernel_call(
        functools.partial(layer_kernel, n_col, n_sum), "layer", 2, outs,
        [True, False, True, True] + [True] * 6 + [False, False, True],
        [anywhere()] * 3 + [vmem(), anywhere(), anywhere(), vmem()] + [anywhere()] * 10,
        scratch, 20 * tok * half * n_unit,
    )(
        q, k, v, seg_row, seg_col, x, gain, wo, dy, dy_end, dy_mid,
        wg, wu, wd, wg_other, wu_other, wd_other,
    )


class Reduce:
    def __init__(self, tile, outs, stage_one, inbox_one, stage_two, inbox_two, send, recv):
        d = lax.axis_index("dp")
        self.x, self.y = d % 2, d // 2
        self.tile, self.outs = tile, outs
        self.stage_one, self.inbox_one = stage_one, inbox_one
        self.stage_two, self.inbox_two = stage_two, inbox_two
        self.send, self.recv = send, recv
        self.along_x = {"dp": self.y * 2 + 1 - self.x}
        self.along_y = {"dp": (1 - self.y) * 2 + self.x}

    def along(self, side):
        return {"dp": jnp.where(side == 0, self.along_x["dp"], self.along_y["dp"])}

    def copy_one(self, side, n):
        return remote(
            self.stage_one.at[side, n], self.inbox_one.at[side, n],
            self.send.at[side, n], self.recv.at[side, n], self.along(side),
        )

    def copy_two(self, side):
        return remote(
            self.stage_two.at[side], self.inbox_two.at[side],
            self.send.at[side, 2], self.recv.at[side, 2], self.along(1 - side),
        )

    def first(self):
        def one(step, carry):
            side = step % 2
            near = jnp.where(side == 0, self.y, self.x)
            n = jnp.where(step < 2, 1 - near, near)
            owner = jnp.where(side == 0, n * 2 + 1 - self.x, (1 - self.y) * 2 + n)
            self.stage_one[side, n] = self.tile(owner, side).astype(BF16)
            self.copy_one(side, n).start()
            return carry

        lax.fori_loop(0, 4, one, 0)

    def second(self):
        def one(side, carry):
            n = jnp.where(side == 0, 1 - self.y, 1 - self.x)
            owner = jnp.where(side == 0, n * 2 + self.x, self.y * 2 + n)
            value = self.tile(owner, side)
            self.copy_one(side, n).wait_recv()
            self.stage_two[side] = (value + self.inbox_one[side, n].astype(F32)).astype(BF16)
            self.copy_two(side).start()
            return carry

        lax.fori_loop(0, 2, one, 0)

    def put(self, side, value, add):
        each = value.shape[1] // len(self.outs)
        cols = span(side * each, each)
        for n, out in enumerate(self.outs):
            term = value[:, n * each : (n + 1) * each]
            out[:, cols] = out[:, cols] + term if add else term

    def merge(self):
        def one(side, carry):
            n = jnp.where(side == 0, self.y, self.x)
            value = self.tile(self.y * 2 + self.x, side)
            self.copy_one(side, n).wait_recv()
            self.put(side, value + self.inbox_one[side, n].astype(F32), False)
            return carry

        lax.fori_loop(0, 2, one, 0)

    def last(self):
        def one(side, carry):
            self.copy_two(side).wait_recv()
            self.put(side, self.inbox_two[side].astype(F32), True)
            return carry

        lax.fori_loop(0, 2, one, 0)

    def finish(self):
        def one(side, carry):
            for n in range(2):
                self.copy_one(side, n).wait_send()
            self.copy_two(side).wait_send()
            return carry

        lax.fori_loop(0, 2, one, 0)

    @staticmethod
    def scratch(rows, cols):
        return [
            pltpu.VMEM((2, 2, rows, cols), BF16),
            pltpu.VMEM((2, 2, rows, cols), BF16),
            pltpu.VMEM((2, rows, cols), BF16),
            pltpu.VMEM((2, rows, cols), BF16),
            pltpu.SemaphoreType.DMA((2, 3)),
            pltpu.SemaphoreType.DMA((2, 3)),
        ]


def square_peers():
    d = lax.axis_index("dp")
    x, y = d % 2, d // 2
    always = d >= 0
    return [(always, {"dp": y * 2 + 1 - x}), (always, {"dp": (1 - y) * 2 + x})]


def pick(step, table):
    value = jnp.int32(table[0])
    for n in range(1, len(table)):
        value = jnp.where(step == n, table[n], value)
    return value


def tile_of(left, right, n_row, base=0, width=None):
    cols = (right.shape[1] if width is None else width) // 2

    def tile(owner, side):
        return dot_tn(left[:, span(owner * n_row, n_row)], right[:, span(base + side * cols, cols)])

    return tile


def far_peers(c):
    return [(c >= 0, {"col": c + 2 - 4 * (c // 2)})]


def branch_kernel(
    n_col, n_sum,
    two_in, scale_in, sums_in, gain, units_in, wd, middle_in, dy_full, h2_in, gate_in, wo, wo_other, heads_in,
    *refs,
):
    (output_out, heads_out, half_out, middle_grad_out), refs = refs[:4], refs[4:]
    sums_out, refs = refs[:n_sum], refs[n_sum:]
    (
        units, middle, h2, grad_gate, heads_all, branch_half, output, grad_heads, grad_middle, scale_wide,
        full, down, dy_half, w_out, part, stage, inbox, rs_send, rs_recv,
        held, sent, arrived, t_send, t_recv, ag_send, ag_recv, local, flushed,
    ), refs = refs[:28], refs[28:]
    sums, refs = refs[:n_sum], refs[n_sum:]
    r, c = lax.axis_index("row"), lax.axis_index("col")
    tok, width = middle.shape
    half = n_col * width
    heads = grad_heads.shape[1]
    rows = tok // N_CHUNK
    me = r * n_col + c
    mine, other, block = span(r * half, half), span((1 - r) * half, half), span(me * width, width)
    copies = fetches(
        [
            (dy_full.at[:, mine], dy_half), (units_in, units), (two_in, grad_middle), (middle_in, middle),
            (scale_in, scale_wide), (wd, down), (h2_in, h2), (gate_in, grad_gate),
            (wo.at[span(r * heads, heads), :], w_out.at[:, mine]), (wo_other, w_out.at[:, other]),
            (heads_in, heads_all),
        ],
        local,
    )
    totals = Totals(held, sent, arrived, t_send, t_recv, r, c)
    held[...] = sums_in[...]
    greet(line_peers(r, c, n_col) + far_peers(c) + (square_peers() if n_sum else []))
    totals.step(0)
    gather = Gather(full, ag_send, ag_recv, r, c, n_col, width)
    scatter = Scatter(part, stage, inbox, rs_send, rs_recv, c, n_col)
    flush = Flush(
        ((output, output_out), (grad_heads, heads_out), (branch_half, half_out), (grad_middle, middle_grad_out)),
        flushed, rows,
    )
    panels = []
    if n_sum:
        terms = ((units, dy_half, half // 2, half // 2), (h2, grad_gate, 0, None), (heads_all, branch_half, 0, None))
        for n, (left, right, base, cols) in enumerate(terms):
            tile = tile_of(left, right, sums[n].shape[0], base, cols)
            panels.append(Reduce(tile, (sums[n],), *refs[6 * n : 6 * n + 6]))

    def panel_do(n, *whats):
        if n_sum:
            for what in whats:
                getattr(panels[n], what)()

    def at_end(*acts):
        @pl.when(jnp.logical_not(scatter.middle))
        def _():
            for distance, chunk in acts:
                gather.end_relay(distance, chunk)

    def at_middle(*acts):
        @pl.when(scatter.middle)
        def _():
            for act, *what in acts:
                act(*what)

    def conclude(chunk):
        at = span(chunk * rows, rows)
        mean = totals.column(chunk) * (1.0 / (2 * half))
        scale = scale_wide[at, 0:1]
        grad = (
            dy_half[at, span(c * width, width)].astype(F32)
            + grad_middle[at, :] * gain[...]
            - middle[at, :] * (scale * scale * mean)
        )
        grad_middle[at, :] = grad
        full[chunk, :, block] = grad.astype(BF16)
        gather.start(chunk)
        flush.start(chunk, (3,))

    def outward(chunk):
        part[chunk] = dot_nn(units[span(chunk * rows, rows), :], down[...])
        scatter.open(chunk)

    def heads_back(chunk):
        at = span(chunk * rows, rows)
        gather.wait_other(chunk)
        branch_half[at, :] = full[chunk, :, mine]
        grad_heads[at, :] = dot_nt(full[chunk], w_out[...]).astype(BF16)
        flush.start(chunk, (1, 2))

    def settle(chunk):
        at = span(chunk * rows, rows)
        scatter.total(chunk, output, at)
        output[at, :] += middle[at, :]
        flush.start(chunk, (0,))

    relay, near, far = gather.middle_relay, scatter.near, scatter.far
    totals.step(1)
    for copy in copies[:2]:
        copy.wait()
    panel_do(0, "first")
    totals.step(2)
    for copy in copies[2:6]:
        copy.wait()
    def store(n):
        return pltpu.make_async_copy(sums[n], sums_out[n], local.at[11 + n])

    def stored(n):
        if n_sum:
            store(n).start()

    def after_first():
        for copy in copies[6:]:
            copy.wait()
        panel_do(1, "first")
        totals.step(3)

        def one(step, carry):
            conclude(pick(step, (1, 2, 0, 3)))
            return carry

        lax.fori_loop(0, N_CHUNK, one, 0)
        at_middle((relay, "a", 2), (relay, "a", 0), (relay, "b", 1), (relay, "b", 2), (relay, "c", 1))
        at_end((2, 2))
        at_middle((relay, "b", 3), (relay, "a", 1), (near, 3))

    def after_third():
        at_middle((relay, "c", 3), (relay, "b", 0), (far, 3))
        at_end((2, 1), (3, 1), (2, 0), (1, 2), (1, 1))
        panel_do(1, "second")

    def after_fifth():
        panel_do(1, "merge")
        panel_do(0, "second")
        at_end((3, 2))
        at_middle((near, 2), (far, 0))

    def after_sixth():
        panel_do(1, "last")
        stored(1)
        at_end((1, 0), (3, 3), (3, 0))
        at_middle((far, 2))

    def after_seventh():
        at_middle((near, 1))
        at_end((2, 3), (1, 3))

    def stage(now, carry):
        turn = pick(now, (0, 0, 0, 1, 0, 1, 1, 1))
        chunk = pick(now, (3, 0, 2, 1, 1, 2, 0, 3))
        pl.when(turn == 0)(lambda: outward(chunk))
        pl.when(turn == 1)(lambda: heads_back(chunk))
        pl.when(now == 0)(after_first)
        pl.when(now == 1)(lambda: at_middle((relay, "a", 3)))
        pl.when(now == 2)(after_third)
        pl.when(now == 3)(lambda: at_middle((relay, "c", 2), (near, 0), (relay, "c", 0)))
        pl.when(now == 4)(after_fifth)
        pl.when(now == 5)(after_sixth)
        pl.when(now == 6)(after_seventh)
        return carry

    lax.fori_loop(0, 8, stage, 0)
    panel_do(2, "first")

    def before_last():
        panel_do(2, "second")
        panel_do(0, "merge", "last")
        stored(0)

    def close_up(now, carry):
        pl.when(now == 1)(lambda: at_middle((far, 1)))
        pl.when(now == 3)(before_last)
        settle(pick(now, (2, 0, 3, 1)))
        return carry

    lax.fori_loop(0, N_CHUNK, close_up, 0)
    panel_do(2, "merge", "last")
    stored(2)
    gather.finish()
    scatter.finish()
    totals.finish()
    for n, panel in enumerate(panels):
        panel.finish()
        store(n).wait()
    flush.finish()


def branch_back(
    n_col, n_dp, two, scale, held, gain, units, wd, middle, dy_full, h2, grad_gate, wo, wo_other, heads_all
):
    tok, width = middle.shape
    half, heads = n_col * width, wo_other.shape[0]
    rows = tok // N_CHUNK
    shape = jax.ShapeDtypeStruct
    outs = [
        shape((tok, width), F32), shape((tok, heads), BF16), shape((tok, half), BF16), shape((tok, width), F32)
    ]
    scratch = [
        pltpu.VMEM(units.shape, BF16),
        pltpu.VMEM(middle.shape, F32),
        pltpu.VMEM(h2.shape, BF16),
        pltpu.VMEM(grad_gate.shape, BF16),
        pltpu.VMEM(heads_all.shape, BF16),
        pltpu.VMEM((tok, half), BF16),
        pltpu.VMEM((tok, width), F32),
        pltpu.VMEM((tok, heads), BF16),
        pltpu.VMEM((tok, width), F32),
        pltpu.VMEM(scale.shape, F32),
        pltpu.VMEM((N_CHUNK, rows, 2 * half), BF16),
        pltpu.VMEM(wd.shape, BF16),
        pltpu.VMEM((tok, half), BF16),
        pltpu.VMEM((heads, 2 * half), BF16),
        *Scatter.scratch(n_col, rows, width),
        *Totals.scratch(rows),
        *gather_sems(n_col),
        pltpu.SemaphoreType.DMA((14,)),
        pltpu.SemaphoreType.DMA((4, N_CHUNK)),
    ]
    n_sum = 0
    if n_dp == 4:
        n_sum = 3
        sizes = [(wd.shape[0] // 4, half // 2), (half // 4, grad_gate.shape[1]), (heads // 2, half)]
        outs += [shape(size, F32) for size in sizes]
        scratch += [pltpu.VMEM(size, F32) for size in sizes]
        for size in sizes:
            scratch += Reduce.scratch(size[0], size[1] // 2)
    return kernel_call(
        functools.partial(branch_kernel, n_col, n_sum), "branch", 4, outs, [True] * len(outs),
        [anywhere(), anywhere(), vmem(), vmem()] + [anywhere()] * 9, scratch, 12 * tok * half * half,
    )(two, scale, held, gain, units, wd, middle, dy_full, h2, grad_gate, wo, wo_other, heads_all)


def attend_back_kernel(
    n_col, n_dp, n_sum,
    q_in, k_in, v_in, heads_grad_in, seg_row, seg_col_in, inv_in, cos_in, sin_in, x_in, r1_in, gain, middle_in,
    gain_two, h1_in, wq, wk, wv, h2_in, up_in,
    *refs,
):
    (tokens_out, gain_sums, triple_out), refs = refs[:3], refs[3:]
    sums_out, refs = refs[:n_sum], refs[n_sum:]
    (
        q, k, v, grad_heads, seg_col, inv_sum, cos_table, sin_table, x, r1, grad_middle,
        h1, h2, grad_up, grad_tokens, triple,
        weights, grad_k, grad_v, grad_q, grad_one, gain_mine, gain_box, part, stage, inbox, rs_send, rs_recv,
        held, sent, arrived, st_send, st_recv, x_send, x_recv, g_send, g_recv, local, flushed,
    ), refs = refs[:39], refs[39:]
    sums, refs = refs[:n_sum], refs[n_sum:]
    r, c, d = lax.axis_index("row"), lax.axis_index("col"), lax.axis_index("dp")
    tok, width = x.shape
    half = n_col * width
    heads = q.shape[1]
    rows = tok // N_CHUNK
    me = r * n_col + c
    early = [(h2_in, h2), (up_in, grad_up)]
    first = [
        (q_in, q), (k_in, k), (v_in, v), (heads_grad_in, grad_heads), (seg_col_in, seg_col), (inv_in, inv_sum),
        (cos_in, cos_table), (sin_in, sin_table),
    ]
    later = [(h1_in, h1), (x_in, x), (r1_in, r1)]
    later.append((middle_in, grad_middle))
    for n, w in enumerate((wq, wk, wv)):
        for side in range(2):
            later.append(
                (w.at[:, pl.ds(side * heads, heads)], weights.at[:, pl.ds((side * 3 + n) * heads, heads)])
            )
    copies = fetches(early + first + later, local)
    early, first, later = copies[:2], copies[2:10], copies[10:]
    dp_peers = [(d != at, {"dp": jnp.int32(at)}) for at in range(n_dp)]
    greet(group_peers(r, c, n_col) + dp_peers)
    scatter = Scatter(part, stage, inbox, rs_send, rs_recv, c, n_col)
    totals = Totals(held, sent, arrived, st_send, st_recv, r, c)
    flush = Flush(((grad_tokens, tokens_out),), flushed, rows)
    panels = []
    if n_sum:
        for n, (left, right) in enumerate(((h2, grad_up), (h1, triple))):
            tile = tile_of(left, right, sums[n].shape[0])
            panels.append(Reduce(tile, sums[1:] if n else sums[:1], *refs[6 * n : 6 * n + 6]))

    def exchange(chunk):
        piece = triple.at[span(chunk * rows, rows), span(r * 3 * heads, 3 * heads)]
        return remote(piece, piece, x_send.at[chunk], x_recv.at[chunk], {"row": 1 - r})

    def attend(chunk):
        at = pl.ds(chunk * rows, rows)
        keys = (chunk + 1) * rows
        allowed = allowed_pairs(seg_col[at, :], seg_row[:, 0:keys], chunk, rows, keys)
        grad_q[...] = jnp.zeros_like(grad_q)

        def head_step(head, carry):
            query = of_head(q[at, :], head)
            grad = of_head(grad_heads[at, :], head)
            scores = dot_nt(query, k[0:keys, :]) * HD**-0.5
            inv = jnp.sum(jnp.where(lanes((rows, 128)) == head, inv_sum[at, :], 0.0), axis=1, keepdims=True)
            probs = jnp.exp(jnp.where(allowed, scores, masked_score)) * inv
            grad_probs = dot_nt(grad, v[0:keys, :])
            weighted = jnp.sum(probs * grad_probs, axis=1, keepdims=True)
            grad_scores = (probs * (grad_probs - weighted) * HD**-0.5).astype(BF16)
            grad_q[...] += dot_nn(grad_scores, of_head(k[0:keys, :], head))
            grad_k[0:keys, :] += dot_tn(grad_scores, query)
            grad_v[0:keys, :] += dot_tn(probs.astype(BF16), grad)
            return carry

        lax.fori_loop(0, heads // HD, head_step, 0)
        cos_rows = widen(cos_table[at, :], heads)
        sin_rows = widen(sin_table[at, :], heads)
        for n, value in enumerate((grad_q[...], grad_k[at, :])):
            value = value * cos_rows - swap_halves(value) * sin_rows
            triple[at, span((r * 3 + n) * heads, heads)] = value.astype(BF16)
        triple[at, span((r * 3 + 2) * heads, heads)] = grad_v[at, :].astype(BF16)
        exchange(chunk).start()

    def contract(chunk):
        at = span(chunk * rows, rows)
        exchange(chunk).wait_recv()
        part[chunk] = dot_nt(triple[at, :], weights[...])
        scatter.open(chunk)

    def settle(chunk):
        at = span(chunk * rows, rows)
        scatter.total(chunk, grad_one, at)
        product = grad_one[at, :] * (x[at, :].astype(F32) * r1[at, 0:1])
        totals.note(chunk, jnp.sum(product * gain[...], axis=1, keepdims=True))
        gain_mine[0] += jnp.sum(product.reshape(rows // 8, 8, width), axis=0)

    def conclude(chunk):
        at = span(chunk * rows, rows)
        mean = totals.column(chunk) * (1.0 / (2 * half))
        scale = r1[at, 0:1]
        grad_tokens[at, :] = grad_middle[at, :] + scale * (
            grad_one[at, :] * gain[...] - x[at, :].astype(F32) * (scale * mean)
        )
        flush.start(chunk)

    def gain_copy(at):
        return remote(gain_box.at[d], gain_box.at[d], g_send.at[at], g_recv.at[d], {"dp": at})

    def gain_arrival(at):
        return remote(gain_box.at[at], gain_box.at[at], g_send.at[at], g_recv.at[at], {"dp": at})

    def others(act):
        def one(at, carry):
            pl.when(at != d)(lambda: act(at))
            return carry

        lax.fori_loop(0, n_dp, one, 0)

    def panel_do(n, what):
        if n_sum:
            getattr(panels[n], what)()

    gain_mine[0] = jnp.zeros(gain_mine.shape[1:], F32)
    gain_mine[1] = gain_two[...]
    grad_k[...] = jnp.zeros_like(grad_k)
    grad_v[...] = jnp.zeros_like(grad_v)
    last = N_CHUNK - 1
    for copy in early:
        copy.wait()
    panel_do(0, "first")
    for copy in first:
        copy.wait()
    attend(last)
    for copy in later:
        copy.wait()
    contract(last)
    attend(last - 1)
    panel_do(0, "second")
    contract(last - 1)
    scatter.near(last)
    attend(last - 2)
    attend(last - 3)
    contract(last - 2)
    scatter.near(last - 1)
    scatter.far(last)
    contract(last - 3)
    panel_do(1, "first")
    scatter.far(last - 1)
    panel_do(0, "merge")
    settle(last)
    panel_do(0, "last")
    scatter.near(last - 2)
    scatter.near(last - 3)
    scatter.far(last - 2)
    panel_do(1, "second")
    scatter.far(last - 3)

    def settle_step(now, carry):
        settle(pick(now, (last - 2, last - 1, last - 3)))
        pl.when(now == 0)(lambda: panel_do(1, "merge"))
        return carry

    lax.fori_loop(0, 3, settle_step, 0)
    gain_box[d] = gain_mine[...]
    others(lambda at: gain_copy(at).start())
    totals.exchange()

    def close_up(step, carry):
        conclude(last - step)
        return carry

    lax.fori_loop(0, N_CHUNK, close_up, 0)
    others(lambda at: gain_arrival(at).wait_recv())
    gain_total = gain_box[0]
    for at in range(1, n_dp):
        gain_total = gain_total + gain_box[at]
    gain_sums[...] = gain_total
    stores = []
    where = len(copies)
    panel_do(1, "last")
    for n, panel in enumerate(panels):
        for m in range(1, n_sum) if n else range(1):
            stores += fetches([(sums[m], sums_out[m])], local.at[pl.ds(where + m, 1)])
    if not n_sum:
        stores += fetches([(triple, triple_out)], local.at[pl.ds(where, 1)])
    scatter.finish()
    totals.finish()
    for chunk in range(N_CHUNK):
        exchange(chunk).wait_send()
    others(lambda at: gain_copy(at).wait_send())
    for panel in panels:
        panel.finish()
    for copy in stores:
        copy.wait()
    flush.finish()


def attend_back(
    n_col, n_dp,
    q, k, v, grad_heads, seg_row, seg_col, inv_sum, cos_table, sin_table, x, r1, gain, grad_middle,
    gain_two, h1, wq, wk, wv, h2, grad_up,
):
    tok, width = x.shape
    half, heads = n_col * width, q.shape[1]
    rows = tok // N_CHUNK
    shape = jax.ShapeDtypeStruct
    triple = (tok, 6 * heads) if n_dp != 4 else (8, 128)
    outs = [shape((tok, width), F32), shape((2, 8, width), F32), shape(triple, BF16)]
    held = [q, k, v, grad_heads, seg_col, inv_sum, cos_table, sin_table, x, r1, grad_middle]
    held += [h1, h2, grad_up]
    scratch = [
        *[pltpu.VMEM(array.shape, array.dtype) for array in held],
        pltpu.VMEM((tok, width), F32),
        pltpu.VMEM((tok, 6 * heads), BF16),
        pltpu.VMEM((half, 6 * heads), BF16),
        pltpu.VMEM((tok, heads), F32),
        pltpu.VMEM((tok, heads), F32),
        pltpu.VMEM((rows, heads), F32),
        pltpu.VMEM((tok, width), F32),
        pltpu.VMEM((2, 8, width), F32),
        pltpu.VMEM((n_dp, 2, 8, width), F32),
        *Scatter.scratch(n_col, rows, width),
        *Totals.scratch(rows),
        pltpu.SemaphoreType.DMA((N_CHUNK,)),
        pltpu.SemaphoreType.DMA((N_CHUNK,)),
        pltpu.SemaphoreType.DMA((n_dp,)),
        pltpu.SemaphoreType.DMA((n_dp,)),
        pltpu.SemaphoreType.DMA((27,)),
        pltpu.SemaphoreType.DMA((1, N_CHUNK)),
    ]
    n_sum = 0
    if n_dp == 4:
        sizes = [(half // 4, grad_up.shape[1])] + [(half // 4, 2 * heads)] * 3
        n_sum = len(sizes)
        outs += [shape(size, F32) for size in sizes]
        scratch += [pltpu.VMEM(size, F32) for size in sizes]
        for size in sizes[:1] + [(half // 4, 6 * heads)]:
            scratch += Reduce.scratch(size[0], size[1] // 2)
    return kernel_call(
        functools.partial(attend_back_kernel, n_col, n_dp, n_sum), "attend_back", 5, outs,
        [True, False, True] + [True] * n_sum,
        [anywhere()] * 4 + [vmem()] + [anywhere()] * 6 + [vmem(), anywhere(), vmem()] + [anywhere()] * 6,
        scratch, 16 * tok * tok * heads,
    )(
        q, k, v, grad_heads, seg_row, seg_col, inv_sum, cos_table, sin_table, x, r1, gain, grad_middle,
        gain_two, h1, wq, wk, wv, h2, grad_up,
    )


def finish_kernel(groups, share, gain_sums, *refs):
    n_copy = sum(groups)
    sources, refs = refs[:n_copy], refs[n_copy:]
    gain_out, refs = refs[:2], refs[2:]
    results, refs = refs[: len(groups)], refs[len(groups) :]
    held, (get, put) = refs[:n_copy], refs[n_copy:]
    targets = []
    for result, parts in zip(results, groups):
        cols = result.shape[1] // parts
        targets += [result.at[:, pl.ds(part * cols, cols)] for part in range(parts)]
    pieces = 2
    inward, outward = [], []
    for n, (source, keep, target) in enumerate(zip(sources, held, targets)):
        rows = keep.shape[0] // pieces
        for piece in range(pieces):
            at = pl.ds(piece * rows, rows)
            inward.append(pltpu.make_async_copy(source.at[at, :], keep.at[at, :], get.at[n, piece]))
            outward.append(pltpu.make_async_copy(keep.at[at, :], target.at[at, :], put.at[n, piece]))
    for copy in inward:
        copy.start()
    d = lax.axis_index("dp")
    width = gain_sums.shape[-1]
    shift = lax.rem(width - d * share, width)
    for n in range(2):
        moved = pltpu.roll(gain_sums[n], shift, 1)
        gain_out[n][...] = jnp.sum(moved, axis=0, keepdims=True)[:, 0:share]
    for one, two in zip(inward, outward):
        one.wait()
        two.start()
    for copy in outward:
        copy.wait()


def finish(share, gain_sums, arrays):
    shape = jax.ShapeDtypeStruct
    groups = tuple(len(parts) for parts in arrays)
    flat = [part for parts in arrays for part in parts]
    outs = [shape((1, share), F32)] * 2
    outs += [shape((p[0].shape[0], sum(x.shape[1] for x in p)), p[0].dtype) for p in arrays]
    n_copy = len(flat)
    return pl.pallas_call(
        functools.partial(finish_kernel, groups, share),
        out_shape=outs,
        in_specs=[vmem()] + [anywhere()] * n_copy,
        out_specs=[vmem()] * 2 + [anywhere()] * len(arrays),
        scratch_shapes=[pltpu.VMEM(x.shape, x.dtype) for x in flat]
        + [pltpu.SemaphoreType.DMA((n_copy, 2)), pltpu.SemaphoreType.DMA((n_copy, 2))],
        compiler_params=pltpu.CompilerParams(vmem_limit_bytes=VMEM_LIMIT),
        name="finish",
    )(gain_sums, *flat)


def body(
    n_dp,
    n_col,
    tokens,
    gain_attn,
    gain_ffn,
    w_query,
    w_key,
    w_value,
    w_out,
    w_gate,
    w_up,
    w_down,
    grad_output,
    segments,
    positions,
):
    tok, width = tokens.shape
    heads = w_query.shape[1] // 2
    gain_one, gain_two = gain_attn.reshape(1, width), gain_ffn.reshape(1, width)
    (
        q, k, v, h1, r1, cos_table, sin_table, seg_col, dy_end, dy_mid, wo_other, wg_other, wu_other, wd_other,
    ) = project(
        n_col, tokens, gain_one, positions, segments, grad_output,
        w_query, w_key, w_value, w_out, w_gate, w_up, w_down,
    )
    (
        heads_all, inv_sum, middle, dy_full,
        h2, units, grad_gate, grad_up, grad_two, scale, gain_sum, held, down_one,
    ) = layer(
        n_col, n_dp, q, k, v, segments, seg_col, tokens, gain_two, w_out, grad_output, dy_end, dy_mid,
        w_gate, w_up, w_down, wg_other, wu_other, wd_other,
    )
    output, grad_heads, branch_half, grad_middle, *sums_one = branch_back(
        n_col, n_dp, grad_two, scale, held, gain_two, units, w_down, middle, dy_full, h2, grad_gate,
        w_out, wo_other, heads_all,
    )
    grad_tokens, gain_sums, triple, *sums_two = attend_back(
        n_col, n_dp, q, k, v, grad_heads, segments, seg_col, inv_sum, cos_table, sin_table, tokens, r1,
        gain_one, grad_middle, gain_sum, h1, w_query, w_key, w_value, h2, grad_up,
    )
    if n_dp == 4:
        down_two, grad_wg, grad_wo = sums_one
        grad_wd = (down_one, down_two)
        grad_wu, *grad_qkv = sums_two
    else:

        def summed(left, right):
            grad = jnp.einsum("ta,tb->ab", left, right, preferred_element_type=F32).astype(BF16)
            return lax.psum_scatter(grad, "dp", scatter_dimension=0, tiled=True).astype(F32)

        row = lax.axis_index("row")
        dy_half = lax.dynamic_slice(dy_full, (0, row * n_col * width), (tok, n_col * width))
        grad_wd, grad_wg = (summed(units, dy_half),), summed(h2, grad_gate)
        grad_wu, grad_wo = summed(h2, grad_up), summed(heads_all, branch_half)
        parts = summed(h1, triple).reshape(-1, 2, 3, heads)
        grad_qkv = [parts[:, :, n].reshape(-1, 2 * heads) for n in range(3)]
    gain_a, gain_b, *results = finish(
        width // n_dp, gain_sums,
        [(m,) for m in (output, grad_tokens, *grad_qkv, grad_wo, grad_wg, grad_wu)] + [grad_wd],
    )
    blocks = [m.reshape((1, 1) + m.shape) for m in results[2:]]
    return (*results[:2], gain_a.reshape(1, 1, -1), gain_b.reshape(1, 1, -1), *blocks)


def solution(mesh):
    return jax.shard_map(
        functools.partial(body, mesh.shape["dp"], mesh.shape["col"]),
        mesh=mesh,
        in_specs=(
            P("dp", ("row", "col")),
            P(("row", "col")),
            P(("row", "col")),
            P("row", "col"),
            P("row", "col"),
            P("row", "col"),
            P("col", "row"),
            P("row", "col"),
            P("row", "col"),
            P("col", "row"),
            P("dp", ("row", "col")),
            P("dp", None),
            P("dp", None),
        ),
        out_specs=(
            P("dp", ("row", "col")),
            P("dp", ("row", "col")),
            P(("row", "col"), "dp", None),
            P(("row", "col"), "dp", None),
            P("row", "dp", None, "col"),
            P("row", "dp", None, "col"),
            P("row", "dp", None, "col"),
            P("col", "dp", None, "row"),
            P("row", "dp", None, "col"),
            P("row", "dp", None, "col"),
            P("col", "dp", None, "row"),
        ),
        check_vma=False,
    )
```

```python
import functools

import jax
import jax.numpy as jnp
import numpy as np
from jax import lax
from jax.experimental import pallas as pl
from jax.experimental.pallas import tpu as pltpu
from jax.sharding import PartitionSpec as P

MESH = pl.DeviceIdType.MESH
F32 = jnp.float32
BF16 = jnp.bfloat16
HD = 64
N_CHUNK = 4
norm_eps = 1e-05
rope_base = 130000.0
masked_score = -1e30
VMEM_LIMIT = 64 * 1024 * 1024 - 65536


def dot_nn(left, right):
    return lax.dot_general(left, right, (((1,), (0,)), ((), ())), preferred_element_type=F32)


def dot_nt(left, right):
    return lax.dot_general(left, right, (((1,), (1,)), ((), ())), preferred_element_type=F32)


def dot_tn(left, right):
    return lax.dot_general(left, right, (((0,), (0,)), ((), ())), preferred_element_type=F32)


def span(start, size):
    return pl.ds(pl.multiple_of(start, size), size)


def remote(src, dst, send_sem, recv_sem, where):
    return pltpu.make_async_remote_copy(
        src_ref=src,
        dst_ref=dst,
        send_sem=send_sem,
        recv_sem=recv_sem,
        device_id=where,
        device_id_type=MESH,
    )


def greet(peers):
    barrier = pltpu.get_barrier_semaphore()
    count = jnp.int32(0)
    for present, where in peers:

        @pl.when(present)
        def _():
            pl.semaphore_signal(barrier, inc=1, device_id=where, device_id_type=MESH)

        count = count + present.astype(jnp.int32)
    pl.semaphore_wait(barrier, count)


def line_peers(r, c, n_col):
    always = c >= 0
    return [
        (c > 0, {"col": jnp.maximum(c - 1, 0)}),
        (c < n_col - 1, {"col": jnp.minimum(c + 1, n_col - 1)}),
        (always, {"row": 1 - r}),
    ]


def group_peers(r, c, n_col):
    return [
        ((c != at) | (r != half), {"row": jnp.int32(half), "col": jnp.int32(at)})
        for half in range(2)
        for at in range(n_col)
    ]


class Gather:
    def __init__(self, full, send, recv, r, c, n_col, width, n_chunk=N_CHUNK):
        self.full, self.send, self.recv = full, send, recv
        self.r, self.c, self.n_col, self.width = r, c, n_col, width
        self.n_chunk = n_chunk

    def piece(self, half, at, chunk):
        cols = span(half * (self.n_col * self.width) + at * self.width, self.width)
        return self.full.at[chunk, :, cols]

    def copy(self, way, at, chunk):
        piece = self.piece(self.r, at, chunk)
        where = (
            {"col": jnp.maximum(self.c - 1, 0)},
            {"col": jnp.minimum(self.c + 1, self.n_col - 1)},
            {"row": 1 - self.r},
        )[way]
        return remote(
            piece, piece, self.send.at[way, at, chunk], self.recv.at[self.r, at, chunk], where
        )

    def wait(self, half, at, chunk):
        piece = self.piece(half, at, chunk)
        remote(
            piece, piece, self.send.at[0, at, chunk], self.recv.at[half, at, chunk], {"row": 1 - self.r}
        ).wait_recv()

    def start(self, chunk):
        c = self.c

        @pl.when(c > 0)
        def _():
            self.copy(0, c, chunk).start()

        @pl.when(c < self.n_col - 1)
        def _():
            self.copy(1, c, chunk).start()

        self.copy(2, c, chunk).start()

    def relay(self, distance, chunk):
        c, last = self.c, self.n_col - 1

        @pl.when(c + distance <= last)
        def _():
            at = c + distance
            self.wait(self.r, at, chunk)

            @pl.when(c > 0)
            def _():
                self.copy(0, at, chunk).start()

            self.copy(2, at, chunk).start()

        @pl.when(c - distance >= 0)
        def _():
            at = c - distance
            self.wait(self.r, at, chunk)

            @pl.when(c < last)
            def _():
                self.copy(1, at, chunk).start()

            self.copy(2, at, chunk).start()

    def toward(self, way, at, chunk):
        piece = self.piece(self.r, at, chunk)
        where = {"col": jnp.clip(self.c - 1 + 2 * way, 0, self.n_col - 1)}
        return remote(piece, piece, self.send.at[way, at, chunk], self.recv.at[self.r, at, chunk], where)

    def hand(self, at, chunk, way=None):
        self.wait(self.r, at, chunk)
        if way is not None:
            self.toward(way, at, chunk).start()
        self.copy(2, at, chunk).start()

    def end_relay(self, distance, chunk):
        self.hand(jnp.where(self.c == 0, distance, 3 - distance), chunk)

    def middle_relay(self, kind, chunk):
        outward = (self.c == 2).astype(jnp.int32)
        near_end = 3 * outward
        at = {"a": 3 - self.c, "b": near_end, "c": 3 - near_end}[kind]
        self.hand(at, chunk, 1 - outward if kind == "b" else outward)

    def tick(self, now):
        for distance in range(self.n_col - 1, 0, -1):
            chunk = now + 1 - distance

            @pl.when((chunk >= 0) & (chunk < self.n_chunk))
            def _():
                self.relay(distance, chunk)

    def wait_other(self, chunk):
        def one(at, carry):
            self.wait(1 - self.r, at, chunk)
            return carry

        lax.fori_loop(0, self.n_col, one, 0)

    def finish(self):
        c, last = self.c, self.n_col - 1

        def one(step, carry):
            at, chunk = step // self.n_chunk, step % self.n_chunk

            @pl.when((c > 0) & (at >= c))
            def _():
                self.copy(0, at, chunk).wait_send()

            @pl.when((c < last) & (at <= c))
            def _():
                self.copy(1, at, chunk).wait_send()

            self.copy(2, at, chunk).wait_send()
            return carry

        lax.fori_loop(0, self.n_col * self.n_chunk, one, 0)


class Scatter:
    def __init__(self, part, stage, inbox, send, recv, c, n_col, n_chunk=N_CHUNK):
        self.part, self.stage, self.inbox = part, stage, inbox
        self.send, self.recv, self.c, self.n_col = send, recv, c, n_col
        self.n_chunk = n_chunk
        self.width = stage.shape[-1]
        self.middle = (c > 0) & (c < n_col - 1)

    def term(self, chunk, dest):
        return self.part[chunk, :, span(dest * self.width, self.width)]

    def staged(self, dest):
        return dest - (dest > self.c).astype(jnp.int32)

    def slot(self, way, dest, at):
        inner = ((at == 1) & (way == 1)) | ((at == 2) & (way == 0))
        return jnp.where((dest == at) & inner, 4, dest)

    def copy(self, way, chunk, dest):
        where = jnp.clip(self.c + 1 - 2 * way, 0, self.n_col - 1)
        slot = self.slot(way, dest, where)
        return remote(
            self.stage.at[chunk, self.staged(dest)],
            self.inbox.at[chunk, slot],
            self.send.at[chunk, dest],
            self.recv.at[chunk, slot],
            {"col": where},
        )

    def arrival(self, way, chunk, dest):
        slot = self.slot(way, dest, self.c)
        here = self.inbox.at[chunk, slot]
        remote(here, here, self.send.at[chunk, dest], self.recv.at[chunk, slot], {"col": self.c}).wait_recv()
        return self.inbox[chunk, slot].astype(F32)

    def open(self, chunk):
        @pl.when(jnp.logical_not(self.middle))
        def _():
            way = (self.c > 0).astype(jnp.int32)

            def ship(step, carry):
                dest = jnp.where(way == 0, self.n_col - 1 - step, step)
                self.stage[chunk, self.staged(dest)] = self.term(chunk, dest).astype(BF16)
                self.copy(way, chunk, dest).start()
                return carry

            lax.fori_loop(0, self.n_col - 1, ship, 0)

    def pass_on(self, way, chunk, dest):
        total = self.term(chunk, dest) + self.arrival(way, chunk, dest)
        self.stage[chunk, self.staged(dest)] = total.astype(BF16)
        self.copy(way, chunk, dest).start()

    def near(self, chunk):
        @pl.when(self.middle)
        def _():
            way = (self.c > 1).astype(jnp.int32)

            def step_on(step, carry):
                self.pass_on(way, chunk, jnp.where(way == 0, self.n_col - 1 - step, step))
                return carry

            lax.fori_loop(0, 2, step_on, 0)

    def far(self, chunk):
        @pl.when(self.middle)
        def _():
            way = (self.c == 1).astype(jnp.int32)
            self.pass_on(way, chunk, jnp.where(self.c == 1, 0, self.n_col - 1))

    def total(self, chunk, out, at):
        c = self.c
        way = (c == 0).astype(jnp.int32)
        out[at, :] = self.term(chunk, c) + self.arrival(way, chunk, c)

        @pl.when(self.middle)
        def _():
            out[at, :] += self.arrival(1, chunk, c)

    def finish(self):
        def one(step, carry):
            chunk, dest = step // self.n_col, step % self.n_col

            @pl.when(dest != self.c)
            def _():
                self.copy(0, chunk, dest).wait_send()

            return carry

        lax.fori_loop(0, self.n_chunk * self.n_col, one, 0)

    @staticmethod
    def scratch(n_col, rows, width, n_chunk=N_CHUNK):
        return [
            pltpu.VMEM((n_chunk, rows, n_col * width), F32),
            pltpu.VMEM((n_chunk, n_col - 1, rows, width), BF16),
            pltpu.VMEM((n_chunk, n_col + 1, rows, width), BF16),
            pltpu.SemaphoreType.DMA((n_chunk, n_col)),
            pltpu.SemaphoreType.DMA((n_chunk, n_col + 1)),
        ]


def gather_sems(n_col, n_chunk=N_CHUNK):
    return [
        pltpu.SemaphoreType.DMA((3, n_col, n_chunk)),
        pltpu.SemaphoreType.DMA((2, n_col, n_chunk)),
    ]


N_NOTE = 16


def put_notes(full, chunk, cols, values):
    rows = full.shape[1] - N_NOTE
    width = values[0].shape[1]
    at = lax.broadcasted_iota(jnp.int32, (N_NOTE, width), 0)
    notes = jnp.zeros((N_NOTE, width), F32)
    for n, value in enumerate(values):
        for piece in range(3):
            rounded = value.astype(BF16).astype(F32)
            notes = jnp.where(at == 3 * n + piece, rounded, notes)
            value = value - rounded
    full[chunk, rows:, cols] = notes.astype(BF16)


def get_note(full, chunk, cols, n):
    rows = full.shape[1] - N_NOTE
    notes = full[chunk, rows:, cols].astype(F32)
    return (notes[3 * n : 3 * n + 1, :] + notes[3 * n + 1 : 3 * n + 2, :]) + notes[3 * n + 2 : 3 * n + 3, :]


def as_row(column):
    return jnp.broadcast_to(column, (column.shape[0], 128)).T[0:1, :]


def as_column(row):
    return jnp.broadcast_to(row, (128, row.shape[1])).T[:, 0:1]


class Totals:
    def __init__(self, held, sent, inbox, send, recv, r, c):
        self.held, self.sent, self.inbox, self.send, self.recv = held, sent, inbox, send, recv
        self.partners = ({"row": 1 - r}, {"col": c + 1 - 2 * (c % 2)}, {"col": c + 2 - 4 * (c // 2)})

    def note(self, chunk, column):
        self.held[pl.ds(chunk, 1), :] = as_row(column)

    def copy(self, step):
        return remote(
            self.sent.at[step], self.inbox.at[step], self.send.at[step], self.recv.at[step], self.partners[step]
        )

    def step(self, n):
        if n > 0:
            self.copy(n - 1).wait_recv()
            self.held[...] += self.inbox[n - 1]
        if n < 3:
            self.sent[n] = self.held[...]
            self.copy(n).start()

    def exchange(self):
        for n in range(4):
            self.step(n)

    def column(self, chunk):
        return as_column(self.held[pl.ds(chunk, 1), :])

    def finish(self):
        for step in range(3):
            self.copy(step).wait_send()

    @staticmethod
    def scratch(rows):
        return [
            pltpu.VMEM((8, rows), F32),
            pltpu.VMEM((3, 8, rows), F32),
            pltpu.VMEM((3, 8, rows), F32),
            pltpu.SemaphoreType.DMA((3,)),
            pltpu.SemaphoreType.DMA((3,)),
        ]


def lanes(shape):
    return lax.broadcasted_iota(jnp.int32, shape, len(shape) - 1)


def swap_halves(values):
    half, width = HD // 2, values.shape[-1]
    low = (lanes(values.shape) & (HD - 1)) < half
    return jnp.where(
        low, pltpu.roll(values, width - half, 1), pltpu.roll(values, half, 1)
    )


def widen(table, width):
    return jnp.concatenate([table] * (width // table.shape[-1]), axis=-1)


class Flush:
    def __init__(self, pairs, sems, rows):
        self.pairs, self.sems, self.rows = pairs, sems, rows

    def copy(self, n, chunk):
        source, target = self.pairs[n]
        at = span(chunk * self.rows, self.rows)
        if isinstance(source, tuple):
            source = source[0].at[chunk, 0 : self.rows, source[1]]
        else:
            source = source.at[at, :]
        return pltpu.make_async_copy(source, target.at[at, :], self.sems.at[n, chunk])

    def start(self, chunk, which=None):
        for n in range(len(self.pairs)) if which is None else which:
            self.copy(n, chunk).start()

    def finish(self):
        def one(chunk, carry):
            for n in range(len(self.pairs)):
                self.copy(n, chunk).wait()
            return carry

        lax.fori_loop(0, N_CHUNK, one, 0)


def fetches(pairs, sems):
    copies = [pltpu.make_async_copy(source, target, sems.at[n]) for n, (source, target) in enumerate(pairs)]
    for copy in copies:
        copy.start()
    return copies


def vmem():
    return pl.BlockSpec(memory_space=pltpu.VMEM)


def anywhere():
    return pl.BlockSpec(memory_space=pl.ANY)


def kernel_call(body, name, ident, outs, out_any, in_specs, scratch, flops):
    return pl.pallas_call(
        body,
        out_shape=outs,
        in_specs=in_specs,
        out_specs=[anywhere() if flag else vmem() for flag in out_any],
        scratch_shapes=scratch,
        compiler_params=pltpu.CompilerParams(
            collective_id=ident, has_side_effects=True, vmem_limit_bytes=VMEM_LIMIT
        ),
        cost_estimate=pl.CostEstimate(flops=flops, bytes_accessed=1 << 24, transcendentals=0),
        name=name,
    )


def project_kernel(
    n_col,
    x, gain, positions, segments, rope, dy, wq, wk, wv, wo, wg, wu, wd,
    q_out, k_out, v_out, h1_out, r1, cos_table, sin_table, seg_col, dy_end, dy_mid,
    wo_other, wg_other, wu_other, wd_other,
    full, hidden, weights, q, k, v, h1, ag_send, ag_recv,
    w_send, w_recv, d_send, d_recv, local, flushed,
):
    r, c = lax.axis_index("row"), lax.axis_index("col")
    tok, width = x.shape
    half = n_col * width
    heads = wq.shape[1] // 2
    units = wg.shape[1] // 2
    me = r * n_col + c
    rows = tok // N_CHUNK
    held = fetches(
        [
            (
                w.at[:, span(r * heads, heads)],
                weights.at[span(r * half, half), pl.ds(n * heads, heads)],
            )
            for n, w in enumerate((wq, wk, wv))
        ],
        local,
    )
    mine = span(me * width, width)

    def prepare(chunk, carry):
        values = x[span(chunk * rows, rows), :]
        full[chunk, 0:rows, mine] = values
        values = values.astype(F32)
        square = as_row(jnp.sum(values * values, axis=1, keepdims=True))
        put_notes(full, chunk, mine, (square, gain[...]))
        return carry

    lax.fori_loop(0, N_CHUNK, prepare, 0)
    greet(group_peers(r, c, n_col))
    gather = Gather(full, ag_send, ag_recv, r, c, n_col, width)
    flush = Flush(((q, q_out), (k, k_out), (v, v_out), (h1, h1_out)), flushed, rows)

    def chunk_rows(chunk):
        return span(chunk * rows, rows)

    gather.start(0)
    gather.start(1)
    other = {"row": 1 - r}
    moved = [
        remote(
            w.at[:, span((1 - r) * heads, heads)],
            weights.at[span(r * half, half), pl.ds(n * heads, heads)],
            w_send.at[n], w_recv.at[n], other,
        )
        for n, w in enumerate((wq, wk, wv))
    ]
    moved.append(remote(wo.at[span((1 - r) * heads, heads), :], wo_other, w_send.at[3], w_recv.at[3], other))
    moved.append(remote(wg.at[:, span((1 - r) * units, units)], wg_other, w_send.at[4], w_recv.at[4], other))
    moved.append(remote(wu.at[:, span((1 - r) * units, units)], wu_other, w_send.at[5], w_recv.at[5], other))
    moved.append(remote(wd.at[span((1 - r) * units, units), :], wd_other, w_send.at[6], w_recv.at[6], other))
    inward = {"col": jnp.where(c == 0, 1, jnp.where(c == 1, 2, jnp.where(c == 2, 1, 2)))}
    at_end = (c == 0) | (c == 3)
    early_end = remote(dy, dy_end, d_send.at[0], d_recv.at[0], inward)
    early_mid = remote(dy, dy_mid, d_send.at[0], d_recv.at[1], inward)

    for copy in moved[:3]:
        copy.start()
    gather.tick(0)
    gather.start(2)
    for copy in moved[3:]:
        copy.start()

    def tables(chunk, carry):
        at = chunk_rows(chunk)
        place = jnp.broadcast_to(positions[:, at].astype(F32), (128, rows)).T
        angles = place * rope[0:1, :]
        cos_table[at, :] = jnp.cos(angles)
        sin_table[at, :] = jnp.sin(angles) * rope[1:2, :]
        seg_col[at, :] = jnp.broadcast_to(segments[:, at].astype(F32), (128, rows)).T
        return carry

    lax.fori_loop(0, N_CHUNK, tables, 0)
    gather.tick(1)
    gather.start(3)
    pl.when(at_end)(early_end.start)
    gather.tick(2)

    def compute(chunk):
        at = chunk_rows(chunk)
        square = jnp.zeros((1, rows), F32)
        for block in range(2 * n_col):
            square = square + get_note(full, chunk, pl.ds(block * width, width), 0)
        scale = lax.rsqrt(as_column(square) * (1.0 / (2 * half)) + norm_eps)
        r1[at, :] = jnp.broadcast_to(scale, (rows, r1.shape[1]))
        for block in range(2 * n_col):
            cols = pl.ds(block * width, width)
            values = full[chunk, 0:rows, cols].astype(F32)
            hidden[:, cols] = (values * scale * get_note(full, chunk, cols, 1)).astype(BF16)
        h1[at, :] = hidden[:, span(r * half, half)]
        values = dot_nn(hidden[...], weights[...])
        cos_rows = widen(cos_table[at, :], heads)
        sin_rows = widen(sin_table[at, :], heads)
        for n, out in enumerate((q, k)):
            part = values[:, n * heads : (n + 1) * heads]
            out[at, :] = (part * cos_rows + swap_halves(part) * sin_rows).astype(BF16)
        v[at, :] = values[:, 2 * heads :].astype(BF16)
        flush.start(chunk)

    for copy in held:
        copy.wait()
    for copy in moved[:3]:
        copy.wait_recv()

    def step(chunk, carry):
        gather.wait_other(chunk)
        compute(chunk)
        gather.tick(chunk + 3)
        pl.when((chunk == 0) & jnp.logical_not(at_end))(early_mid.start)
        return carry

    lax.fori_loop(0, N_CHUNK, step, 0)
    gather.finish()
    for copy in moved[3:]:
        copy.wait_recv()
    for copy in moved:
        copy.wait_send()
    early_end.wait_send()

    @pl.when(jnp.logical_not(at_end))
    def _():
        early_end.wait_recv()
        early_mid.wait_recv()

    flush.finish()


def project(n_col, x, gain, positions, segments, dy, wq, wk, wv, wo, wg, wu, wd):
    tok, width = x.shape
    full = 2 * n_col * width
    half = n_col * width
    heads, units = wq.shape[1] // 2, wg.shape[1] // 2
    lane = np.arange(128) % HD
    inv_freq = rope_base ** (-2.0 * (lane % (HD // 2)) / HD)
    rope = jnp.asarray(np.stack([inv_freq, np.where(lane < HD // 2, -1.0, 1.0)]), F32)
    shape = jax.ShapeDtypeStruct
    outs = [
        shape((tok, heads), BF16), shape((tok, heads), BF16), shape((tok, heads), BF16),
        shape((tok, half), BF16), shape((tok, 128), F32),
        shape((tok, 128), F32), shape((tok, 128), F32), shape((tok, 128), F32),
        shape((tok, width), BF16), shape((tok, width), BF16),
        shape((heads, wo.shape[1]), BF16), shape((half, units), BF16),
        shape((half, units), BF16), shape((units, wd.shape[1]), BF16),
    ]
    scratch = [
        pltpu.VMEM((N_CHUNK, tok // N_CHUNK + N_NOTE, full), BF16),
        pltpu.VMEM((tok // N_CHUNK, full), BF16),
        pltpu.VMEM((full, 3 * heads), BF16),
        *[pltpu.VMEM((tok, heads), BF16)] * 3,
        pltpu.VMEM((tok, half), BF16),
        *gather_sems(n_col),
        pltpu.SemaphoreType.DMA((7,)),
        pltpu.SemaphoreType.DMA((7,)),
        pltpu.SemaphoreType.DMA((1,)),
        pltpu.SemaphoreType.DMA((2,)),
        pltpu.SemaphoreType.DMA((3,)),
        pltpu.SemaphoreType.DMA((4, N_CHUNK)),
    ]
    return kernel_call(
        functools.partial(project_kernel, n_col), "project", 1, outs,
        [True] * 4 + [False] * 4 + [True] * 6,
        [vmem()] * 5 + [anywhere()] * 8, scratch, 6 * tok * full * heads,
    )(x, gain, positions, segments, rope, dy, wq, wk, wv, wo, wg, wu, wd)


def allowed_pairs(seg_col, seg_row, chunk, rows, keys):
    seg_row = seg_row.astype(F32)
    query_at = chunk * rows + lax.broadcasted_iota(jnp.int32, (rows, keys), 0)
    key_at = lanes((rows, keys))
    return (key_at <= query_at) & (seg_col[:, 0:1] == seg_row)


def of_head(values, head):
    return jnp.where((lanes(values.shape) // HD) == head, values, jnp.zeros_like(values))


class LateGather:
    def __init__(self, full, send, recv, r, c, n_col, width):
        self.inner = Gather(full, send, recv, r, c, n_col, width)
        self.c = c
        self.end = (c == 0) | (c == 3)
        self.near_end = jnp.where(c < 2, 0, 3)
        self.far_end = 3 - self.near_end
        self.other = 3 - c
        self.outward = (c >= 2).astype(jnp.int32)

    def copy(self, way, at, chunk):
        piece = self.inner.piece(self.inner.r, at, chunk)
        where = ({"col": self.near_end}, {"col": self.other}, {"row": 1 - self.inner.r})[way]
        return remote(
            piece, piece, self.inner.send.at[way, at, chunk], self.inner.recv.at[self.inner.r, at, chunk], where
        )

    def start(self, chunk):
        c = self.c
        self.copy(2, c, chunk).start()

        @pl.when(jnp.logical_not(self.end))
        def _():
            self.copy(0, c, chunk).start()
            self.copy(1, self.near_end, chunk).start()
            self.copy(0, self.other, chunk).start()
            self.copy(2, self.near_end, chunk).start()
            self.copy(2, self.other, chunk).start()

    def relay(self, chunk):
        @pl.when(jnp.logical_not(self.end))
        def _():
            self.inner.wait(self.inner.r, self.far_end, chunk)
            self.copy(0, self.far_end, chunk).start()
            self.copy(2, self.far_end, chunk).start()

    def collect(self, chunk):
        @pl.when(self.end)
        def _():
            for step in range(3):
                at = jnp.where(self.c == 0, 1 + step, 2 - step)
                self.inner.wait(self.inner.r, at, chunk)
                self.copy(2, at, chunk).start()

    def finish(self):
        def one(step, carry):
            at, chunk = step // 4, step % 4
            self.copy(2, at, chunk).wait_send()

            @pl.when(jnp.logical_not(self.end))
            def _():
                pl.when(at != self.near_end)(lambda: self.copy(0, at, chunk).wait_send())
                pl.when(at == self.near_end)(lambda: self.copy(1, at, chunk).wait_send())

            return carry

        lax.fori_loop(0, 4 * N_CHUNK, one, 0)


def layer_kernel(
    n_col, n_sum,
    q_in, k_in, v_in, seg_row, seg_col_in, x_in, gain, wo, dy, dy_end, dy_mid,
    wg, wu, wd, wg_other, wu_other, wd_other,
    heads_out, inv_sum, middle_out, dy_out,
    h2_out, units_out, gate_out, up_out, two_out, scale_out, gain_sum, held, sum_out,
    q, k, v, seg_col, x, heads_all, middle, dy_full, w_out,
    units, grad_gate, grad_up, grad_two,
    full, gate_own, up_own, down_own, gate_far, up_far,
    part, stage_z, inbox_z, z_send, z_recv, stage_f, inbox_f, f_send, f_recv,
    dy_send, dy_recv, ag_send, ag_recv,
    h_send, h_recv, x_send, x_recv, local, flushed, *refs,
):
    r, c = lax.axis_index("row"), lax.axis_index("col")
    tok, heads = q.shape
    width = x.shape[1]
    half = n_col * width
    n_unit = down_own.shape[0]
    rows = tok // N_CHUNK
    me = r * n_col + c
    row_base = r * n_col
    sums = refs[0:1]
    mine, far = span(r * n_unit, n_unit), span((1 - r) * n_unit, n_unit)
    near_rows, far_rows = span(r * half, half), span((1 - r) * half, half)
    block = span(me * width, width)
    everything = pl.ds(0, dy_full.shape[2])

    def chunk_rows(chunk):
        return span(chunk * rows, rows)

    scale_wide = seg_col
    late = LateGather(dy_full, dy_send, dy_recv, r, c, n_col, width)
    gather = Gather(full, ag_send, ag_recv, r, c, n_col, width)
    scatter_z = Scatter(part, stage_z, inbox_z, z_send, z_recv, c, n_col)
    scatter_f = Scatter(part, stage_f, inbox_f, f_send, f_recv, c, n_col)
    flush = Flush(
        (
            ((full, near_rows), h2_out), (grad_gate, gate_out), (grad_up, up_out), (units, units_out),
            (grad_two, two_out), (scale_wide, scale_out),
            (heads_all, heads_out), (middle, middle_out), ((dy_full, everything), dy_out),
        ),
        flushed, rows,
    )
    panels = []
    if n_sum:

        def tile(owner, side):
            cols = half // 4
            n_row = sums[0].shape[0]
            right = dy_full[:, :, span(r * half + side * cols, cols)].reshape(tok, cols)
            return dot_tn(units[:, span(owner * n_row, n_row)], right)

        panels.append(Reduce(tile, sums, *refs[1:]))

    def block_load(source, at):
        return source.reshape(N_CHUNK, rows, width), dy_full.at[:, :, span(at * width, width)]

    own, *first = fetches(
        [block_load(dy, me), (q_in, q), (k_in, k), (v_in, v), (seg_col_in, seg_col), (wo, w_out), (x_in, x)],
        local,
    )
    early = [
        pltpu.make_async_copy(*block_load(dy_end, row_base + late.near_end), local.at[7]),
        pltpu.make_async_copy(*block_load(dy_mid, row_base + late.other), local.at[8]),
    ]

    @pl.when(jnp.logical_not(late.end))
    def _():
        for copy in early:
            copy.start()

    greet(line_peers(r, c, n_col) + (square_peers() if n_sum else []))
    loads = fetches(
        [
            (wg.at[:, mine], gate_own.at[near_rows, :]),
            (wg_other, gate_own.at[far_rows, :]),
            (wu.at[:, mine], up_own.at[near_rows, :]),
            (wu_other, up_own.at[far_rows, :]),
            (wd.at[mine, :], down_own.at[:, near_rows]),
            (wd_other, down_own.at[:, far_rows]),
            (wg.at[:, far], gate_far),
            (wu.at[:, far], up_far),
        ],
        local.at[pl.ds(9, 8)],
    )
    own.wait()

    @pl.when(jnp.logical_not(late.end))
    def _():
        for copy in early:
            copy.wait()


    def heads_copy(chunk):
        piece = heads_all.at[pl.ds(chunk * rows, rows), span(r * heads, heads)]
        return remote(piece, piece, h_send.at[chunk], h_recv.at[chunk], {"row": 1 - r})

    def attend(chunk):
        at = pl.ds(chunk * rows, rows)
        keys = (chunk + 1) * rows
        allowed = allowed_pairs(seg_col[at, :], seg_row[:, 0:keys], chunk, rows, keys)

        def head_step(head, carry):
            total, inverse = carry
            scores = dot_nt(of_head(q[at, :], head), k[0:keys, :]) * HD**-0.5
            weights = jnp.exp(jnp.where(allowed, scores, masked_score))
            inv = 1.0 / jnp.sum(weights, axis=1, keepdims=True)
            probs = (weights * inv).astype(BF16)
            total = total + dot_nn(probs, of_head(v[0:keys, :], head))
            inverse = jnp.where(lanes((rows, 128)) == head, inv, inverse)
            return total, inverse

        total, inverse = lax.fori_loop(
            0, heads // HD, head_step, (jnp.zeros((rows, heads), F32), jnp.zeros((rows, 128), F32))
        )
        heads_all[at, span(r * heads, heads)] = total.astype(BF16)
        inv_sum[at, :] = inverse
        heads_copy(chunk).start()

    def contract(chunk):
        heads_copy(chunk).wait_recv()
        flush.start(chunk, (6,))
        part[chunk] = dot_nn(heads_all[span(chunk * rows, rows), :], w_out[...])
        scatter_z.open(chunk)

    def settle_z(chunk):
        at = chunk_rows(chunk)
        scatter_z.total(chunk, middle, at)
        values = middle[at, :] + x[at, :].astype(F32)
        middle[at, :] = values
        full[chunk, 0:rows, block] = (values * gain[...]).astype(BF16)
        put_notes(full, chunk, block, (as_row(jnp.sum(values * values, axis=1, keepdims=True)),))
        gather.start(chunk)
        flush.start(chunk, (7,))

    def exchange(n, chunk):
        piece = (grad_gate, grad_up, units)[n].at[chunk_rows(chunk), mine]
        return remote(piece, piece, x_send.at[n, chunk], x_recv.at[n, chunk], {"row": 1 - r})

    def norm(chunk):
        square = jnp.zeros((1, rows), F32)
        for at in range(2 * n_col):
            square = square + get_note(full, chunk, pl.ds(at * width, width), 0)
        scale = lax.rsqrt(as_column(square) * (1.0 / (2 * half)) + norm_eps)
        scale_wide[chunk_rows(chunk), :] = jnp.broadcast_to(scale, (rows, scale_wide.shape[1]))

    size = n_unit // 2

    def units_part(chunk, step):
        at = chunk_rows(chunk)
        scale = scale_wide[at, 0:1]
        cols = span(step * size, size)
        gate = dot_nn(full[chunk, 0:rows, :], gate_own[:, cols]) * scale
        up = dot_nn(full[chunk, 0:rows, :], up_own[:, cols]) * scale
        grad = dot_nt(dy_full[chunk], down_own[cols, :])
        sig = jax.nn.sigmoid(gate)
        act = gate * sig
        put = span(r * n_unit + step * size, size)
        units[at, put] = (act * up).astype(BF16)
        grad = grad * scale
        grad_gate[at, put] = (grad * up * sig * (1.0 + gate * (1.0 - sig))).astype(BF16)
        grad_up[at, put] = (grad * act).astype(BF16)

    def back(chunk):
        at = chunk_rows(chunk)
        part[chunk] = dot_nt(grad_gate[at, mine], gate_own[near_rows, :]) + dot_nt(
            grad_up[at, mine], up_own[near_rows, :]
        )
        for n in range(2):
            exchange(n, chunk).wait_recv()
        part[chunk] += dot_nt(grad_gate[at, far], gate_far[...]) + dot_nt(grad_up[at, far], up_far[...])
        scatter_f.open(chunk)
        exchange(2, chunk).wait_recv()
        flush.start(chunk, (0, 1, 2, 3, 5, 8))

    def settle_f(chunk):
        at = chunk_rows(chunk)
        scatter_f.total(chunk, grad_two, at)
        product = grad_two[at, :] * middle[at, :]
        held[pl.ds(chunk, 1), :] = as_row(jnp.sum(product * gain[...], axis=1, keepdims=True))
        gain_sum[...] += jnp.sum(product.reshape(rows // 8, 8, width), axis=0)
        flush.start(chunk, (4,))

    middle_role = scatter_z.middle

    def at_end(*acts):
        @pl.when(jnp.logical_not(middle_role))
        def _():
            for act, *what in acts:
                act(*what)

    def at_middle(*acts):
        @pl.when(middle_role)
        def _():
            for act, *what in acts:
                act(*what)

    near, far_sum = scatter_z.near, scatter_z.far
    near_f, far_f = scatter_f.near, scatter_f.far
    end_relay, middle_relay = gather.end_relay, gather.middle_relay
    gain_sum[...] = jnp.zeros_like(gain_sum)
    held[...] = jnp.zeros_like(held)
    at_end(*[(late.start, chunk) for chunk in range(N_CHUNK)])
    at_middle((late.start, 0), (late.start, 1), (late.start, 2))
    for copy in first:
        copy.wait()
    at_middle((late.relay, 0), (late.start, 3))
    attend(0)
    contract(0)
    at_middle((near, 0))
    attend(1)
    attend(2)
    at_middle((far_sum, 0))
    contract(1)
    at_middle((near, 1), (far_sum, 1))
    contract(2)
    at_middle((near, 2), (far_sum, 2))

    def settle_first(chunk, carry):
        settle_z(chunk)
        return carry

    lax.fori_loop(0, 2, settle_first, 0)
    attend(3)
    at_middle((middle_relay, "b", 0))
    at_end((late.collect, 0))
    at_middle((middle_relay, "a", 0), (middle_relay, "b", 1), (middle_relay, "c", 0))
    settle_z(2)
    at_middle((late.relay, 1), (middle_relay, "c", 1), (middle_relay, "a", 1), (middle_relay, "a", 2))
    at_end((end_relay, 1, 0))
    contract(3)
    at_middle((near, 3), (middle_relay, "b", 2))
    at_end((end_relay, 3, 0), (end_relay, 2, 0))
    for copy in loads:
        copy.wait()

    def step(now, carry):
        late.inner.wait_other(now)
        gather.wait_other(now)
        norm(now)

        def part_step(n, carry):
            units_part(now, n)
            return carry

        lax.fori_loop(0, 2, part_step, 0)
        for n in range(3):
            exchange(n, now).start()
        pl.when(now == 1)(lambda: at_middle((near_f, 0), (middle_relay, "a", 3)))
        pl.when(now == 3)(lambda: at_middle((far_f, 1), (near_f, 2), (far_f, 2)))
        back(now)

        @pl.when(now == 0)
        def _():
            at_end((end_relay, 2, 1), (end_relay, 1, 1))
            at_middle((far_sum, 3))
            settle_z(3)
            at_middle((middle_relay, "c", 2), (late.relay, 2))
            at_end((end_relay, 3, 1), (late.collect, 1))

        @pl.when(now == 1)
        def _():
            at_middle((middle_relay, "b", 3), (late.relay, 3))
            at_end((end_relay, 1, 2), (end_relay, 2, 2), (end_relay, 2, 3), (end_relay, 3, 2), (late.collect, 2))

        @pl.when(now == 2)
        def _():
            at_middle((middle_relay, "c", 3), (far_f, 0), (near_f, 1))
            at_end((end_relay, 3, 3), (end_relay, 1, 3), (late.collect, 3))

        return carry

    lax.fori_loop(0, N_CHUNK, step, 0)
    for panel in panels:
        panel.first()
    at_middle((near_f, 3), (far_f, 3))
    for panel in panels:
        panel.second()

    def drain(now, carry):
        settle_f(now)
        return carry

    lax.fori_loop(0, N_CHUNK, drain, 0)
    gather.finish()
    late.finish()
    scatter_z.finish()
    scatter_f.finish()
    stores = []
    for panel in panels:
        panel.merge()
        panel.last()
        stores += fetches([(sums[0], sum_out)], local.at[pl.ds(17, 1)])
        panel.finish()

    def close(chunk, carry):
        heads_copy(chunk).wait_send()
        for n in range(3):
            exchange(n, chunk).wait_send()
        return carry

    lax.fori_loop(0, N_CHUNK, close, 0)
    for copy in stores:
        copy.wait()
    flush.finish()


def layer(
    n_col, n_dp, q, k, v, seg_row, seg_col, x, gain, wo, dy, dy_end, dy_mid,
    wg, wu, wd, wg_other, wu_other, wd_other,
):
    tok, heads = q.shape
    width = x.shape[1]
    half, n_unit = n_col * width, wg.shape[1] // 2
    rows = tok // N_CHUNK
    shape = jax.ShapeDtypeStruct
    n_sum = int(n_dp == 4)
    size = (wd.shape[0] // 4, half // 2) if n_sum else (8, 128)
    outs = [
        shape((tok, 2 * heads), BF16), shape((tok, 128), F32), shape((tok, width), F32),
        shape((tok, 2 * half), BF16), shape((tok, half), BF16),
        shape((tok, 2 * n_unit), BF16), shape((tok, 2 * n_unit), BF16), shape((tok, 2 * n_unit), BF16),
        shape((tok, width), F32), shape((tok, 128), F32), shape((8, width), F32), shape((8, rows), F32),
        shape(size, F32),
    ]
    scatter = Scatter.scratch(n_col, rows, width)
    scratch = [
        *[pltpu.VMEM(array.shape, array.dtype) for array in (q, k, v, seg_col, x)],
        pltpu.VMEM((tok, 2 * heads), BF16),
        pltpu.VMEM((tok, width), F32),
        pltpu.VMEM((N_CHUNK, rows, 2 * half), BF16),
        pltpu.VMEM(wo.shape, BF16),
        *[pltpu.VMEM((tok, 2 * n_unit), BF16)] * 3,
        pltpu.VMEM((tok, width), F32),
        pltpu.VMEM((N_CHUNK, rows + N_NOTE, 2 * half), BF16),
        pltpu.VMEM((2 * half, n_unit), BF16),
        pltpu.VMEM((2 * half, n_unit), BF16),
        pltpu.VMEM((n_unit, 2 * half), BF16),
        pltpu.VMEM((half, n_unit), BF16),
        pltpu.VMEM((half, n_unit), BF16),
        *scatter,
        *scatter[1:],
        *gather_sems(n_col),
        *gather_sems(n_col),
        pltpu.SemaphoreType.DMA((N_CHUNK,)),
        pltpu.SemaphoreType.DMA((N_CHUNK,)),
        pltpu.SemaphoreType.DMA((3, N_CHUNK)),
        pltpu.SemaphoreType.DMA((3, N_CHUNK)),
        pltpu.SemaphoreType.DMA((18,)),
        pltpu.SemaphoreType.DMA((9, N_CHUNK)),
    ]
    if n_sum:
        scratch += [pltpu.VMEM(size, F32), *Reduce.scratch(size[0], size[1] // 2)]
    return kernel_call(
        functools.partial(layer_kernel, n_col, n_sum), "layer", 2, outs,
        [True, False, True, True] + [True] * 6 + [False, False, True],
        [anywhere()] * 3 + [vmem(), anywhere(), anywhere(), vmem()] + [anywhere()] * 10,
        scratch, 20 * tok * half * n_unit,
    )(
        q, k, v, seg_row, seg_col, x, gain, wo, dy, dy_end, dy_mid,
        wg, wu, wd, wg_other, wu_other, wd_other,
    )


class Reduce:
    def __init__(self, tile, outs, stage_one, inbox_one, stage_two, inbox_two, send, recv):
        d = lax.axis_index("dp")
        self.x, self.y = d % 2, d // 2
        self.tile, self.outs = tile, outs
        self.stage_one, self.inbox_one = stage_one, inbox_one
        self.stage_two, self.inbox_two = stage_two, inbox_two
        self.send, self.recv = send, recv
        self.along_x = {"dp": self.y * 2 + 1 - self.x}
        self.along_y = {"dp": (1 - self.y) * 2 + self.x}

    def along(self, side):
        return {"dp": jnp.where(side == 0, self.along_x["dp"], self.along_y["dp"])}

    def copy_one(self, side, n):
        return remote(
            self.stage_one.at[side, n], self.inbox_one.at[side, n],
            self.send.at[side, n], self.recv.at[side, n], self.along(side),
        )

    def copy_two(self, side):
        return remote(
            self.stage_two.at[side], self.inbox_two.at[side],
            self.send.at[side, 2], self.recv.at[side, 2], self.along(1 - side),
        )

    def first(self):
        def one(step, carry):
            side = step % 2
            near = jnp.where(side == 0, self.y, self.x)
            n = jnp.where(step < 2, 1 - near, near)
            owner = jnp.where(side == 0, n * 2 + 1 - self.x, (1 - self.y) * 2 + n)
            self.stage_one[side, n] = self.tile(owner, side).astype(BF16)
            self.copy_one(side, n).start()
            return carry

        lax.fori_loop(0, 4, one, 0)

    def second(self):
        def one(side, carry):
            n = jnp.where(side == 0, 1 - self.y, 1 - self.x)
            owner = jnp.where(side == 0, n * 2 + self.x, self.y * 2 + n)
            value = self.tile(owner, side)
            self.copy_one(side, n).wait_recv()
            self.stage_two[side] = (value + self.inbox_one[side, n].astype(F32)).astype(BF16)
            self.copy_two(side).start()
            return carry

        lax.fori_loop(0, 2, one, 0)

    def put(self, side, value, add):
        each = value.shape[1] // len(self.outs)
        cols = span(side * each, each)
        for n, out in enumerate(self.outs):
            term = value[:, n * each : (n + 1) * each]
            out[:, cols] = out[:, cols] + term if add else term

    def merge(self):
        def one(side, carry):
            n = jnp.where(side == 0, self.y, self.x)
            value = self.tile(self.y * 2 + self.x, side)
            self.copy_one(side, n).wait_recv()
            self.put(side, value + self.inbox_one[side, n].astype(F32), False)
            return carry

        lax.fori_loop(0, 2, one, 0)

    def last(self):
        def one(side, carry):
            self.copy_two(side).wait_recv()
            self.put(side, self.inbox_two[side].astype(F32), True)
            return carry

        lax.fori_loop(0, 2, one, 0)

    def finish(self):
        def one(side, carry):
            for n in range(2):
                self.copy_one(side, n).wait_send()
            self.copy_two(side).wait_send()
            return carry

        lax.fori_loop(0, 2, one, 0)

    @staticmethod
    def scratch(rows, cols):
        return [
            pltpu.VMEM((2, 2, rows, cols), BF16),
            pltpu.VMEM((2, 2, rows, cols), BF16),
            pltpu.VMEM((2, rows, cols), BF16),
            pltpu.VMEM((2, rows, cols), BF16),
            pltpu.SemaphoreType.DMA((2, 3)),
            pltpu.SemaphoreType.DMA((2, 3)),
        ]


def square_peers():
    d = lax.axis_index("dp")
    x, y = d % 2, d // 2
    always = d >= 0
    return [(always, {"dp": y * 2 + 1 - x}), (always, {"dp": (1 - y) * 2 + x})]


def pick(step, table):
    value = jnp.int32(table[0])
    for n in range(1, len(table)):
        value = jnp.where(step == n, table[n], value)
    return value


def tile_of(left, right, n_row, base=0, width=None):
    cols = (right.shape[1] if width is None else width) // 2

    def tile(owner, side):
        return dot_tn(left[:, span(owner * n_row, n_row)], right[:, span(base + side * cols, cols)])

    return tile


def far_peers(c):
    return [(c >= 0, {"col": c + 2 - 4 * (c // 2)})]


def branch_kernel(
    n_col, n_sum,
    two_in, scale_in, sums_in, gain, units_in, wd, middle_in, dy_full, h2_in, gate_in, wo, wo_other, heads_in,
    *refs,
):
    (output_out, heads_out, half_out, middle_grad_out), refs = refs[:4], refs[4:]
    sums_out, refs = refs[:n_sum], refs[n_sum:]
    (
        units, middle, h2, grad_gate, heads_all, branch_half, output, grad_heads, grad_middle, scale_wide,
        full, down, dy_half, w_out, part, stage, inbox, rs_send, rs_recv,
        held, sent, arrived, t_send, t_recv, ag_send, ag_recv, local, flushed,
    ), refs = refs[:28], refs[28:]
    sums, refs = refs[:n_sum], refs[n_sum:]
    r, c = lax.axis_index("row"), lax.axis_index("col")
    tok, width = middle.shape
    half = n_col * width
    heads = grad_heads.shape[1]
    rows = tok // N_CHUNK
    me = r * n_col + c
    mine, other, block = span(r * half, half), span((1 - r) * half, half), span(me * width, width)
    copies = fetches(
        [
            (dy_full.at[:, mine], dy_half), (units_in, units), (two_in, grad_middle), (middle_in, middle),
            (scale_in, scale_wide), (wd, down), (h2_in, h2), (gate_in, grad_gate),
            (wo.at[span(r * heads, heads), :], w_out.at[:, mine]), (wo_other, w_out.at[:, other]),
            (heads_in, heads_all),
        ],
        local,
    )
    totals = Totals(held, sent, arrived, t_send, t_recv, r, c)
    held[...] = sums_in[...]
    greet(line_peers(r, c, n_col) + far_peers(c) + (square_peers() if n_sum else []))
    totals.step(0)
    gather = Gather(full, ag_send, ag_recv, r, c, n_col, width)
    scatter = Scatter(part, stage, inbox, rs_send, rs_recv, c, n_col)
    flush = Flush(
        ((output, output_out), (grad_heads, heads_out), (branch_half, half_out), (grad_middle, middle_grad_out)),
        flushed, rows,
    )
    panels = []
    if n_sum:
        terms = ((units, dy_half, half // 2, half // 2), (h2, grad_gate, 0, None), (heads_all, branch_half, 0, None))
        for n, (left, right, base, cols) in enumerate(terms):
            tile = tile_of(left, right, sums[n].shape[0], base, cols)
            panels.append(Reduce(tile, (sums[n],), *refs[6 * n : 6 * n + 6]))

    def panel_do(n, *whats):
        if n_sum:
            for what in whats:
                getattr(panels[n], what)()

    def at_end(*acts):
        @pl.when(jnp.logical_not(scatter.middle))
        def _():
            for distance, chunk in acts:
                gather.end_relay(distance, chunk)

    def at_middle(*acts):
        @pl.when(scatter.middle)
        def _():
            for act, *what in acts:
                act(*what)

    def conclude(chunk):
        at = span(chunk * rows, rows)
        mean = totals.column(chunk) * (1.0 / (2 * half))
        scale = scale_wide[at, 0:1]
        grad = (
            dy_half[at, span(c * width, width)].astype(F32)
            + grad_middle[at, :] * gain[...]
            - middle[at, :] * (scale * scale * mean)
        )
        grad_middle[at, :] = grad
        full[chunk, :, block] = grad.astype(BF16)
        gather.start(chunk)
        flush.start(chunk, (3,))

    def outward(chunk):
        part[chunk] = dot_nn(units[span(chunk * rows, rows), :], down[...])
        scatter.open(chunk)

    def heads_back(chunk):
        at = span(chunk * rows, rows)
        gather.wait_other(chunk)
        branch_half[at, :] = full[chunk, :, mine]
        grad_heads[at, :] = dot_nt(full[chunk], w_out[...]).astype(BF16)
        flush.start(chunk, (1, 2))

    def settle(chunk):
        at = span(chunk * rows, rows)
        scatter.total(chunk, output, at)
        output[at, :] += middle[at, :]
        flush.start(chunk, (0,))

    relay, near, far = gather.middle_relay, scatter.near, scatter.far
    totals.step(1)
    for copy in copies[:2]:
        copy.wait()
    panel_do(0, "first")
    totals.step(2)
    for copy in copies[2:6]:
        copy.wait()
    def store(n):
        return pltpu.make_async_copy(sums[n], sums_out[n], local.at[11 + n])

    def stored(n):
        if n_sum:
            store(n).start()

    def after_first():
        for copy in copies[6:]:
            copy.wait()
        panel_do(1, "first")
        totals.step(3)

        def one(step, carry):
            conclude(pick(step, (1, 2, 0, 3)))
            return carry

        lax.fori_loop(0, N_CHUNK, one, 0)
        at_middle((relay, "a", 2), (relay, "a", 0), (relay, "b", 1), (relay, "b", 2), (relay, "c", 1))
        at_end((2, 2))
        at_middle((relay, "b", 3), (relay, "a", 1), (near, 3))

    def after_third():
        at_middle((relay, "c", 3), (relay, "b", 0), (far, 3))
        at_end((2, 1), (3, 1), (2, 0), (1, 2), (1, 1))
        panel_do(1, "second")

    def after_fifth():
        panel_do(1, "merge")
        panel_do(0, "second")
        at_end((3, 2))
        at_middle((near, 2), (far, 0))

    def after_sixth():
        panel_do(1, "last")
        stored(1)
        at_end((1, 0), (3, 3), (3, 0))
        at_middle((far, 2))

    def after_seventh():
        at_middle((near, 1))
        at_end((2, 3), (1, 3))

    def stage(now, carry):
        turn = pick(now, (0, 0, 0, 1, 0, 1, 1, 1))
        chunk = pick(now, (3, 0, 2, 1, 1, 2, 0, 3))
        pl.when(turn == 0)(lambda: outward(chunk))
        pl.when(turn == 1)(lambda: heads_back(chunk))
        pl.when(now == 0)(after_first)
        pl.when(now == 1)(lambda: at_middle((relay, "a", 3)))
        pl.when(now == 2)(after_third)
        pl.when(now == 3)(lambda: at_middle((relay, "c", 2), (near, 0), (relay, "c", 0)))
        pl.when(now == 4)(after_fifth)
        pl.when(now == 5)(after_sixth)
        pl.when(now == 6)(after_seventh)
        return carry

    lax.fori_loop(0, 8, stage, 0)
    panel_do(2, "first")

    def before_last():
        panel_do(2, "second")
        panel_do(0, "merge", "last")
        stored(0)

    def close_up(now, carry):
        pl.when(now == 1)(lambda: at_middle((far, 1)))
        pl.when(now == 3)(before_last)
        settle(pick(now, (2, 0, 3, 1)))
        return carry

    lax.fori_loop(0, N_CHUNK, close_up, 0)
    panel_do(2, "merge", "last")
    stored(2)
    gather.finish()
    scatter.finish()
    totals.finish()
    for n, panel in enumerate(panels):
        panel.finish()
        store(n).wait()
    flush.finish()


def branch_back(
    n_col, n_dp, two, scale, held, gain, units, wd, middle, dy_full, h2, grad_gate, wo, wo_other, heads_all
):
    tok, width = middle.shape
    half, heads = n_col * width, wo_other.shape[0]
    rows = tok // N_CHUNK
    shape = jax.ShapeDtypeStruct
    outs = [
        shape((tok, width), F32), shape((tok, heads), BF16), shape((tok, half), BF16), shape((tok, width), F32)
    ]
    scratch = [
        pltpu.VMEM(units.shape, BF16),
        pltpu.VMEM(middle.shape, F32),
        pltpu.VMEM(h2.shape, BF16),
        pltpu.VMEM(grad_gate.shape, BF16),
        pltpu.VMEM(heads_all.shape, BF16),
        pltpu.VMEM((tok, half), BF16),
        pltpu.VMEM((tok, width), F32),
        pltpu.VMEM((tok, heads), BF16),
        pltpu.VMEM((tok, width), F32),
        pltpu.VMEM(scale.shape, F32),
        pltpu.VMEM((N_CHUNK, rows, 2 * half), BF16),
        pltpu.VMEM(wd.shape, BF16),
        pltpu.VMEM((tok, half), BF16),
        pltpu.VMEM((heads, 2 * half), BF16),
        *Scatter.scratch(n_col, rows, width),
        *Totals.scratch(rows),
        *gather_sems(n_col),
        pltpu.SemaphoreType.DMA((14,)),
        pltpu.SemaphoreType.DMA((4, N_CHUNK)),
    ]
    n_sum = 0
    if n_dp == 4:
        n_sum = 3
        sizes = [(wd.shape[0] // 4, half // 2), (half // 4, grad_gate.shape[1]), (heads // 2, half)]
        outs += [shape(size, F32) for size in sizes]
        scratch += [pltpu.VMEM(size, F32) for size in sizes]
        for size in sizes:
            scratch += Reduce.scratch(size[0], size[1] // 2)
    return kernel_call(
        functools.partial(branch_kernel, n_col, n_sum), "branch", 4, outs, [True] * len(outs),
        [anywhere(), anywhere(), vmem(), vmem()] + [anywhere()] * 9, scratch, 12 * tok * half * half,
    )(two, scale, held, gain, units, wd, middle, dy_full, h2, grad_gate, wo, wo_other, heads_all)


def attend_back_kernel(
    n_col, n_dp, n_sum,
    q_in, k_in, v_in, heads_grad_in, seg_row, seg_col_in, inv_in, cos_in, sin_in, x_in, r1_in, gain, middle_in,
    gain_two, h1_in, wq, wk, wv, h2_in, up_in,
    *refs,
):
    (tokens_out, gain_sums, triple_out), refs = refs[:3], refs[3:]
    sums_out, refs = refs[:n_sum], refs[n_sum:]
    (
        q, k, v, grad_heads, seg_col, inv_sum, cos_table, sin_table, x, r1, grad_middle,
        h1, h2, grad_up, grad_tokens, triple,
        weights, grad_k, grad_v, grad_q, grad_one, gain_mine, gain_box, part, stage, inbox, rs_send, rs_recv,
        held, sent, arrived, st_send, st_recv, x_send, x_recv, g_send, g_recv, local, flushed,
    ), refs = refs[:39], refs[39:]
    sums, refs = refs[:n_sum], refs[n_sum:]
    r, c, d = lax.axis_index("row"), lax.axis_index("col"), lax.axis_index("dp")
    tok, width = x.shape
    half = n_col * width
    heads = q.shape[1]
    rows = tok // N_CHUNK
    me = r * n_col + c
    early = [(h2_in, h2), (up_in, grad_up)]
    first = [
        (q_in, q), (k_in, k), (v_in, v), (heads_grad_in, grad_heads), (seg_col_in, seg_col), (inv_in, inv_sum),
        (cos_in, cos_table), (sin_in, sin_table),
    ]
    later = [(h1_in, h1), (x_in, x), (r1_in, r1)]
    later.append((middle_in, grad_middle))
    for n, w in enumerate((wq, wk, wv)):
        for side in range(2):
            later.append(
                (w.at[:, pl.ds(side * heads, heads)], weights.at[:, pl.ds((side * 3 + n) * heads, heads)])
            )
    copies = fetches(early + first + later, local)
    early, first, later = copies[:2], copies[2:10], copies[10:]
    dp_peers = [(d != at, {"dp": jnp.int32(at)}) for at in range(n_dp)]
    greet(group_peers(r, c, n_col) + dp_peers)
    scatter = Scatter(part, stage, inbox, rs_send, rs_recv, c, n_col)
    totals = Totals(held, sent, arrived, st_send, st_recv, r, c)
    flush = Flush(((grad_tokens, tokens_out),), flushed, rows)
    panels = []
    if n_sum:
        for n, (left, right) in enumerate(((h2, grad_up), (h1, triple))):
            tile = tile_of(left, right, sums[n].shape[0])
            panels.append(Reduce(tile, sums[1:] if n else sums[:1], *refs[6 * n : 6 * n + 6]))

    def exchange(chunk):
        piece = triple.at[span(chunk * rows, rows), span(r * 3 * heads, 3 * heads)]
        return remote(piece, piece, x_send.at[chunk], x_recv.at[chunk], {"row": 1 - r})

    def attend(chunk):
        at = pl.ds(chunk * rows, rows)
        keys = (chunk + 1) * rows
        allowed = allowed_pairs(seg_col[at, :], seg_row[:, 0:keys], chunk, rows, keys)
        grad_q[...] = jnp.zeros_like(grad_q)

        def head_step(head, carry):
            query = of_head(q[at, :], head)
            grad = of_head(grad_heads[at, :], head)
            scores = dot_nt(query, k[0:keys, :]) * HD**-0.5
            inv = jnp.sum(jnp.where(lanes((rows, 128)) == head, inv_sum[at, :], 0.0), axis=1, keepdims=True)
            probs = jnp.exp(jnp.where(allowed, scores, masked_score)) * inv
            grad_probs = dot_nt(grad, v[0:keys, :])
            weighted = jnp.sum(probs * grad_probs, axis=1, keepdims=True)
            grad_scores = (probs * (grad_probs - weighted) * HD**-0.5).astype(BF16)
            grad_q[...] += dot_nn(grad_scores, of_head(k[0:keys, :], head))
            grad_k[0:keys, :] += dot_tn(grad_scores, query)
            grad_v[0:keys, :] += dot_tn(probs.astype(BF16), grad)
            return carry

        lax.fori_loop(0, heads // HD, head_step, 0)
        cos_rows = widen(cos_table[at, :], heads)
        sin_rows = widen(sin_table[at, :], heads)
        for n, value in enumerate((grad_q[...], grad_k[at, :])):
            value = value * cos_rows - swap_halves(value) * sin_rows
            triple[at, span((r * 3 + n) * heads, heads)] = value.astype(BF16)
        triple[at, span((r * 3 + 2) * heads, heads)] = grad_v[at, :].astype(BF16)
        exchange(chunk).start()

    def contract(chunk):
        at = span(chunk * rows, rows)
        exchange(chunk).wait_recv()
        part[chunk] = dot_nt(triple[at, :], weights[...])
        scatter.open(chunk)

    def settle(chunk):
        at = span(chunk * rows, rows)
        scatter.total(chunk, grad_one, at)
        product = grad_one[at, :] * (x[at, :].astype(F32) * r1[at, 0:1])
        totals.note(chunk, jnp.sum(product * gain[...], axis=1, keepdims=True))
        gain_mine[0] += jnp.sum(product.reshape(rows // 8, 8, width), axis=0)

    def conclude(chunk):
        at = span(chunk * rows, rows)
        mean = totals.column(chunk) * (1.0 / (2 * half))
        scale = r1[at, 0:1]
        grad_tokens[at, :] = grad_middle[at, :] + scale * (
            grad_one[at, :] * gain[...] - x[at, :].astype(F32) * (scale * mean)
        )
        flush.start(chunk)

    def gain_copy(at):
        return remote(gain_box.at[d], gain_box.at[d], g_send.at[at], g_recv.at[d], {"dp": at})

    def gain_arrival(at):
        return remote(gain_box.at[at], gain_box.at[at], g_send.at[at], g_recv.at[at], {"dp": at})

    def others(act):
        def one(at, carry):
            pl.when(at != d)(lambda: act(at))
            return carry

        lax.fori_loop(0, n_dp, one, 0)

    def panel_do(n, what):
        if n_sum:
            getattr(panels[n], what)()

    gain_mine[0] = jnp.zeros(gain_mine.shape[1:], F32)
    gain_mine[1] = gain_two[...]
    grad_k[...] = jnp.zeros_like(grad_k)
    grad_v[...] = jnp.zeros_like(grad_v)
    last = N_CHUNK - 1
    for copy in early:
        copy.wait()
    panel_do(0, "first")
    for copy in first:
        copy.wait()
    attend(last)
    for copy in later:
        copy.wait()
    contract(last)
    attend(last - 1)
    panel_do(0, "second")
    contract(last - 1)
    scatter.near(last)
    attend(last - 2)
    attend(last - 3)
    contract(last - 2)
    scatter.near(last - 1)
    scatter.far(last)
    contract(last - 3)
    panel_do(1, "first")
    scatter.far(last - 1)
    panel_do(0, "merge")
    settle(last)
    panel_do(0, "last")
    scatter.near(last - 2)
    scatter.near(last - 3)
    scatter.far(last - 2)
    panel_do(1, "second")
    scatter.far(last - 3)

    def settle_step(now, carry):
        settle(pick(now, (last - 2, last - 1, last - 3)))
        pl.when(now == 0)(lambda: panel_do(1, "merge"))
        return carry

    lax.fori_loop(0, 3, settle_step, 0)
    gain_box[d] = gain_mine[...]
    others(lambda at: gain_copy(at).start())
    totals.exchange()

    def close_up(step, carry):
        conclude(last - step)
        return carry

    lax.fori_loop(0, N_CHUNK, close_up, 0)
    others(lambda at: gain_arrival(at).wait_recv())
    gain_total = gain_box[0]
    for at in range(1, n_dp):
        gain_total = gain_total + gain_box[at]
    gain_sums[...] = gain_total
    stores = []
    where = len(copies)
    panel_do(1, "last")
    for n, panel in enumerate(panels):
        for m in range(1, n_sum) if n else range(1):
            stores += fetches([(sums[m], sums_out[m])], local.at[pl.ds(where + m, 1)])
    if not n_sum:
        stores += fetches([(triple, triple_out)], local.at[pl.ds(where, 1)])
    scatter.finish()
    totals.finish()
    for chunk in range(N_CHUNK):
        exchange(chunk).wait_send()
    others(lambda at: gain_copy(at).wait_send())
    for panel in panels:
        panel.finish()
    for copy in stores:
        copy.wait()
    flush.finish()


def attend_back(
    n_col, n_dp,
    q, k, v, grad_heads, seg_row, seg_col, inv_sum, cos_table, sin_table, x, r1, gain, grad_middle,
    gain_two, h1, wq, wk, wv, h2, grad_up,
):
    tok, width = x.shape
    half, heads = n_col * width, q.shape[1]
    rows = tok // N_CHUNK
    shape = jax.ShapeDtypeStruct
    triple = (tok, 6 * heads) if n_dp != 4 else (8, 128)
    outs = [shape((tok, width), F32), shape((2, 8, width), F32), shape(triple, BF16)]
    held = [q, k, v, grad_heads, seg_col, inv_sum, cos_table, sin_table, x, r1, grad_middle]
    held += [h1, h2, grad_up]
    scratch = [
        *[pltpu.VMEM(array.shape, array.dtype) for array in held],
        pltpu.VMEM((tok, width), F32),
        pltpu.VMEM((tok, 6 * heads), BF16),
        pltpu.VMEM((half, 6 * heads), BF16),
        pltpu.VMEM((tok, heads), F32),
        pltpu.VMEM((tok, heads), F32),
        pltpu.VMEM((rows, heads), F32),
        pltpu.VMEM((tok, width), F32),
        pltpu.VMEM((2, 8, width), F32),
        pltpu.VMEM((n_dp, 2, 8, width), F32),
        *Scatter.scratch(n_col, rows, width),
        *Totals.scratch(rows),
        pltpu.SemaphoreType.DMA((N_CHUNK,)),
        pltpu.SemaphoreType.DMA((N_CHUNK,)),
        pltpu.SemaphoreType.DMA((n_dp,)),
        pltpu.SemaphoreType.DMA((n_dp,)),
        pltpu.SemaphoreType.DMA((27,)),
        pltpu.SemaphoreType.DMA((1, N_CHUNK)),
    ]
    n_sum = 0
    if n_dp == 4:
        sizes = [(half // 4, grad_up.shape[1])] + [(half // 4, 2 * heads)] * 3
        n_sum = len(sizes)
        outs += [shape(size, F32) for size in sizes]
        scratch += [pltpu.VMEM(size, F32) for size in sizes]
        for size in sizes[:1] + [(half // 4, 6 * heads)]:
            scratch += Reduce.scratch(size[0], size[1] // 2)
    return kernel_call(
        functools.partial(attend_back_kernel, n_col, n_dp, n_sum), "attend_back", 5, outs,
        [True, False, True] + [True] * n_sum,
        [anywhere()] * 4 + [vmem()] + [anywhere()] * 6 + [vmem(), anywhere(), vmem()] + [anywhere()] * 6,
        scratch, 16 * tok * tok * heads,
    )(
        q, k, v, grad_heads, seg_row, seg_col, inv_sum, cos_table, sin_table, x, r1, gain, grad_middle,
        gain_two, h1, wq, wk, wv, h2, grad_up,
    )


def finish_kernel(groups, share, gain_sums, *refs):
    n_copy = sum(groups)
    sources, refs = refs[:n_copy], refs[n_copy:]
    gain_out, refs = refs[:2], refs[2:]
    results, refs = refs[: len(groups)], refs[len(groups) :]
    held, (get, put) = refs[:n_copy], refs[n_copy:]
    targets = []
    for result, parts in zip(results, groups):
        cols = result.shape[1] // parts
        targets += [result.at[:, pl.ds(part * cols, cols)] for part in range(parts)]
    inward, outward = [], []
    for n, (source, keep, target) in enumerate(zip(sources, held, targets)):
        inward.append(pltpu.make_async_copy(source, keep, get.at[n]))
        outward.append(pltpu.make_async_copy(keep, target, put.at[n]))
    for copy in inward:
        copy.start()
    d = lax.axis_index("dp")
    width = gain_sums.shape[-1]
    shift = lax.rem(width - d * share, width)
    for n in range(2):
        moved = pltpu.roll(gain_sums[n], shift, 1)
        gain_out[n][...] = jnp.sum(moved, axis=0, keepdims=True)[:, 0:share]
    for one, two in zip(inward, outward):
        one.wait()
        two.start()
    for copy in outward:
        copy.wait()


def finish(share, gain_sums, arrays):
    shape = jax.ShapeDtypeStruct
    groups = tuple(len(parts) for parts in arrays)
    flat = [part for parts in arrays for part in parts]
    outs = [shape((1, share), F32)] * 2
    outs += [shape((p[0].shape[0], sum(x.shape[1] for x in p)), p[0].dtype) for p in arrays]
    n_copy = len(flat)
    return pl.pallas_call(
        functools.partial(finish_kernel, groups, share),
        out_shape=outs,
        in_specs=[vmem()] + [anywhere()] * n_copy,
        out_specs=[vmem()] * 2 + [anywhere()] * len(arrays),
        scratch_shapes=[pltpu.VMEM(x.shape, x.dtype) for x in flat]
        + [pltpu.SemaphoreType.DMA((n_copy,)), pltpu.SemaphoreType.DMA((n_copy,))],
        compiler_params=pltpu.CompilerParams(vmem_limit_bytes=VMEM_LIMIT),
        name="finish",
    )(gain_sums, *flat)


def body(
    n_dp,
    n_col,
    tokens,
    gain_attn,
    gain_ffn,
    w_query,
    w_key,
    w_value,
    w_out,
    w_gate,
    w_up,
    w_down,
    grad_output,
    segments,
    positions,
):
    tok, width = tokens.shape
    heads = w_query.shape[1] // 2
    gain_one, gain_two = gain_attn.reshape(1, width), gain_ffn.reshape(1, width)
    (
        q, k, v, h1, r1, cos_table, sin_table, seg_col, dy_end, dy_mid, wo_other, wg_other, wu_other, wd_other,
    ) = project(
        n_col, tokens, gain_one, positions, segments, grad_output,
        w_query, w_key, w_value, w_out, w_gate, w_up, w_down,
    )
    (
        heads_all, inv_sum, middle, dy_full,
        h2, units, grad_gate, grad_up, grad_two, scale, gain_sum, held, down_one,
    ) = layer(
        n_col, n_dp, q, k, v, segments, seg_col, tokens, gain_two, w_out, grad_output, dy_end, dy_mid,
        w_gate, w_up, w_down, wg_other, wu_other, wd_other,
    )
    output, grad_heads, branch_half, grad_middle, *sums_one = branch_back(
        n_col, n_dp, grad_two, scale, held, gain_two, units, w_down, middle, dy_full, h2, grad_gate,
        w_out, wo_other, heads_all,
    )
    grad_tokens, gain_sums, triple, *sums_two = attend_back(
        n_col, n_dp, q, k, v, grad_heads, segments, seg_col, inv_sum, cos_table, sin_table, tokens, r1,
        gain_one, grad_middle, gain_sum, h1, w_query, w_key, w_value, h2, grad_up,
    )
    if n_dp == 4:
        down_two, grad_wg, grad_wo = sums_one
        grad_wd = (down_one, down_two)
        grad_wu, *grad_qkv = sums_two
    else:

        def summed(left, right):
            grad = jnp.einsum("ta,tb->ab", left, right, preferred_element_type=F32).astype(BF16)
            return lax.psum_scatter(grad, "dp", scatter_dimension=0, tiled=True).astype(F32)

        row = lax.axis_index("row")
        dy_half = lax.dynamic_slice(dy_full, (0, row * n_col * width), (tok, n_col * width))
        grad_wd, grad_wg = (summed(units, dy_half),), summed(h2, grad_gate)
        grad_wu, grad_wo = summed(h2, grad_up), summed(heads_all, branch_half)
        parts = summed(h1, triple).reshape(-1, 2, 3, heads)
        grad_qkv = [parts[:, :, n].reshape(-1, 2 * heads) for n in range(3)]
    gain_a, gain_b, *results = finish(
        width // n_dp, gain_sums,
        [(m,) for m in (output, grad_tokens, *grad_qkv, grad_wo, grad_wg, grad_wu)] + [grad_wd],
    )
    blocks = [m.reshape((1, 1) + m.shape) for m in results[2:]]
    return (*results[:2], gain_a.reshape(1, 1, -1), gain_b.reshape(1, 1, -1), *blocks)


def solution(mesh):
    return jax.shard_map(
        functools.partial(body, mesh.shape["dp"], mesh.shape["col"]),
        mesh=mesh,
        in_specs=(
            P("dp", ("row", "col")),
            P(("row", "col")),
            P(("row", "col")),
            P("row", "col"),
            P("row", "col"),
            P("row", "col"),
            P("col", "row"),
            P("row", "col"),
            P("row", "col"),
            P("col", "row"),
            P("dp", ("row", "col")),
            P("dp", None),
            P("dp", None),
        ),
        out_specs=(
            P("dp", ("row", "col")),
            P("dp", ("row", "col")),
            P(("row", "col"), "dp", None),
            P(("row", "col"), "dp", None),
            P("row", "dp", None, "col"),
            P("row", "dp", None, "col"),
            P("row", "dp", None, "col"),
            P("col", "dp", None, "row"),
            P("row", "dp", None, "col"),
            P("row", "dp", None, "col"),
            P("col", "dp", None, "row"),
        ),
        check_vma=False,
    )
```
